32 devices in a mesh: block: 4 (over y, core), patch: 8 (over z, x).
Axes of the slice: x: 2, y: 2, z: 4, core: 2. Of those that a mesh axis runs over, the one named last changes fastest.
Arguments:
- samples_in: bfloat16 [8, 16, 512, 128], P('block', None, 'patch'), may hold values from -6 to 6
- block_order: int32 [8, 8], P('patch'), may hold values from 0 to 7, each once within a row
- seam_link: int32 [8], P('patch'), may hold values from 0 to 1, as said below
- w_in: bfloat16 [8, 32, 256], P('block'), may hold values from -1.5 to 1.5
- w_mid: bfloat16 [8, 2, 256, 256], P('block'), may hold values from -0.5 to 0.5
- w_feat: bfloat16 [8, 256, 64], P('block'), may hold values from -0.375 to 0.375
- w_density: bfloat16 [8, 256], P('block'), may hold values from -0.375 to 0.375
- w_conv: bfloat16 [4, 3, 3, 64, 64], replicated, may hold values from -0.375 to 0.375
- w_color: bfloat16 [3, 64], replicated, may hold values from -0.75 to 0.75
Outputs:
- pixels: float32 [3, 64, 2048], P(None, 'block', 'patch')
The draws below stay inside these ranges and needn't reach their ends.
Inputs may be any that keep to these rules, and one draw needn't show every extreme that they name: Each row of block_order names every one of the 8 blocks once, in the order in which that patch's rays pass them, nearest first. seam_link[p] is 1 where patch p + 1 continues patch p to the right in one image; the entry before last is always 1; the last entry is not read.
All inputs are finite; a program needn't handle non-finite values.
Results may differ from the reference program's by a relative error of at most 0.015.
Values may be sent and summed in bfloat16 or wider, within the bound.
No kernel may reach another device: no remote copies, remote signals or barrier semaphores. Data moves between devices by JAX's collectives and lax.ppermute only.
A program may use at most 64 MiB of HBM per device.

```python
import jax
import jax.numpy as jnp
from jax import lax

WIDTH = 256
ENC = 32
FEAT = 64
SAMP = 4
COLS_LO = 64
NB = 8
IMG_ROWS = 16
PATCHES = 8
TOTAL_COLS = 512
N_PATCH = 8


def draw_seam_link(key, part):
    levels = jax.random.randint(jax.random.fold_in(key, 17), (PATCHES,), 0, 4)
    links = (levels < 3).astype(jnp.int32)
    return links.at[PATCHES - 2].set(1)


def steps_of(own_key, extent, cuts, low, top_value):
    level, own = 1.0, jax.random.fold_in(own_key, 6)
    for dim, shards_of in cuts:
        heights = jnp.exp(jax.random.uniform(jax.random.fold_in(own, dim), (shards_of,), jnp.float32, low / len(cuts), top_value / len(cuts)))
        level = level * jnp.repeat(heights, extent[dim] // shards_of).reshape([-1 if axis == dim else 1 for axis in range(len(extent))])
    return level


def noise(key, dims, spread, bound, split=(), kind=jnp.bfloat16):
    array = jax.random.normal(key, dims, jnp.float32) * spread
    if len(split) > 0:
        array = steps_of(key, dims, split, -0.22, 0.18) * array
    return jnp.clip(array, min=-bound, max=bound).astype(kind)


def setup_inputs(seed: int = 0) -> dict:
    splits = jax.random.split(jax.random.key(seed), 10)
    return {
        "samples_in": noise(splits[0], (NB, IMG_ROWS, TOTAL_COLS, SAMP * ENC), 1.0, 6.0, ((0, 4), (2, 8))),
        "block_order": jax.vmap(lambda own: jax.random.permutation(own, NB))(jax.random.split(splits[1], PATCHES)).reshape((PATCHES, NB)).astype(jnp.int32),
        "seam_link": draw_seam_link(jax.random.fold_in(splits[9], 71), 0),
        "w_in": noise(splits[3], (NB, ENC, WIDTH), (ENC // 2) ** -0.5, 1.5, ((0, 4),)),
        "w_mid": noise(splits[4], (NB, 2, WIDTH, WIDTH), (WIDTH // 2) ** -0.5, 0.5, ((0, 4),)),
        "w_feat": noise(splits[5], (NB, WIDTH, FEAT), WIDTH ** -0.5, 0.375, ((0, 4),)),
        "w_density": noise(splits[6], (NB, WIDTH), WIDTH ** -0.5, 0.375, ((0, 4),)),
        "w_conv": noise(splits[7], (4, 3, 3, FEAT, FEAT), (9 * FEAT // 2) ** -0.5, 0.375),
        "w_color": noise(splits[8], (3, FEAT), FEAT ** -0.5, 0.75),
    }


step_length = 0.03
highest = lax.Precision.HIGHEST


def block_field(samples, w_first, w_hidden, w_head, w_dens):
    count = samples.shape[0]
    flat = samples.reshape(count * SAMP, ENC)
    hidden = jax.nn.relu(jnp.dot(flat, w_first, preferred_element_type=jnp.float32)).astype(jnp.bfloat16)
    hidden = jax.nn.relu(jnp.dot(hidden, w_hidden[0], preferred_element_type=jnp.float32)).astype(jnp.bfloat16)
    hidden = jax.nn.relu(jnp.dot(hidden, w_hidden[1], preferred_element_type=jnp.float32)).astype(jnp.bfloat16)
    feature = lax.dot_general(w_head, hidden, (((0,), (1,)), ((), ())), preferred_element_type=jnp.float32)
    density = jax.nn.softplus(jnp.dot(hidden, w_dens, preferred_element_type=jnp.float32))
    optical = step_length * density.reshape(count, SAMP)
    earlier = jnp.cumsum(optical, axis=1) - optical
    weights = jnp.exp(-earlier) * (-jnp.expm1(-optical))
    colour = jnp.sum(feature.reshape(feature.shape[0], count, SAMP) * weights[None], axis=2)
    return jnp.sum(optical, axis=1), colour


def ranks_of(order_row):
    blocks = order_row.shape[0]
    places = jnp.arange(blocks, dtype=jnp.int32)
    hits = (order_row[None, :] == places[:, None]).astype(jnp.int32)
    return jnp.sum(places[None, :] * hits, axis=1)


def column_masks(seam_link, width):
    total = width * N_PATCH
    column = jnp.arange(total, dtype=jnp.int32)
    owner = column // width
    prior = jnp.concatenate([jnp.zeros((1,), jnp.int32), seam_link[:-1]])
    left_open = jnp.where(column % width == 0, prior[owner], 1)
    right_open = jnp.where(column % width == width - 1, seam_link[owner], 1)
    return left_open.astype(jnp.bfloat16), right_open.astype(jnp.bfloat16)


def convolve(image, kernel, seam_link):
    rows = image.shape[1]
    total = image.shape[2]
    left_open, right_open = column_masks(seam_link, total // N_PATCH)
    padded = jnp.pad(image, ((0, 0), (1, 1), (1, 1)))
    result = jnp.zeros((kernel.shape[2], rows, total), jnp.float32)
    for down in range(3):
        for across in range(3):
            window = padded[:, down:down + rows, across:across + total]
            if across == 0:
                window = window * left_open[None, None, :]
            if across == 2:
                window = window * right_open[None, None, :]
            result = result + lax.dot_general(kernel[down, across], window, (((1,), (0,)), ((), ())), preferred_element_type=jnp.float32)
    return result


def enlarge(image):
    return jnp.repeat(jnp.repeat(image, 2, axis=1), 2, axis=2)


def reference(samples_in, block_order, seam_link, w_in, w_mid, w_feat, w_density, w_conv, w_color):
    def render_patch(patch):
        columns = lax.dynamic_slice_in_dim(samples_in, patch * COLS_LO, COLS_LO, 2)
        rays = columns.reshape(NB, IMG_ROWS * COLS_LO, SAMP * ENC)
        depth_all, colour_all = lax.map(lambda parts: block_field(parts[0], parts[1], parts[2], parts[3], parts[4]), (rays, w_in, w_mid, w_feat, w_density))
        rank = ranks_of(block_order[patch])
        earlier = (rank[:, None] < rank[None, :]).astype(jnp.float32)
        prefix = jnp.dot(earlier.T, depth_all, precision=highest)
        mixed = jnp.einsum("br,bfr->fr", jnp.exp(-prefix), colour_all, precision=highest)
        return mixed.astype(jnp.bfloat16)

    images = lax.map(render_patch, jnp.arange(N_PATCH, dtype=jnp.int32))
    composite = images.reshape(N_PATCH, FEAT, IMG_ROWS, COLS_LO).transpose(1, 2, 0, 3).reshape(FEAT, IMG_ROWS, N_PATCH * COLS_LO)
    decoded = jax.nn.relu(convolve(enlarge(composite), w_conv[0], seam_link)).astype(jnp.bfloat16)
    decoded = jax.nn.relu(convolve(decoded, w_conv[1], seam_link)).astype(jnp.bfloat16)
    decoded = jax.nn.relu(convolve(enlarge(decoded), w_conv[2], seam_link)).astype(jnp.bfloat16)
    final = convolve(decoded, w_conv[3], seam_link)
    return lax.dot_general(w_color.astype(jnp.float32), final, (((1,), (0,)), ((), ())), precision=highest)
```

```python
import functools

import numpy as np

import jax
import jax.numpy as jnp
from jax import lax
from jax.experimental import pallas as pl
from jax.experimental.pallas import tpu as pltpu
from jax.sharding import PartitionSpec as P

STEP = 0.03
LANES = 128
EDGE = 2
LEAD = 8
F32 = jnp.float32
BF16 = jnp.bfloat16


def dot(a, b):
    return jnp.dot(a, b, preferred_element_type=F32)


def dot_t(a, b):
    return lax.dot_general(a, b, (((1,), (1,)), ((), ())), preferred_element_type=F32)


def relu16(x):
    return jnp.maximum(x, 0.0).astype(BF16)


def softplus(v):
    e = jnp.exp(-jnp.abs(v))
    tail = jnp.where(e < 1e-3, e * (1.0 - e * (0.5 - e * (1.0 / 3.0))), jnp.log(1.0 + e))
    return jnp.maximum(v, 0.0) + tail


def fade(optical):
    through = jnp.exp(-optical)
    small = optical * (1.0 - optical * (0.5 - optical * (1.0 / 6.0 - optical * (1.0 / 24.0))))
    return through, jnp.where(optical < 0.0625, small, 1.0 - through)


def field_rays(xs, win, wmid, whead, samples, enc):
    rays = xs[0].shape[0]
    lane = lax.broadcasted_iota(jnp.int32, xs[0].shape, 1)
    total = None
    for b, x in enumerate(xs):
        zero = jnp.zeros_like(x)
        parts = [
            jnp.where((lane >= s * enc) & (lane < (s + 1) * enc), x, zero) for s in range(samples)
        ]
        hidden = relu16(dot(jnp.concatenate(parts, axis=0), win[b]))
        hidden = relu16(dot(hidden, wmid[b, 0]))
        hidden = relu16(dot(hidden, wmid[b, 1]))
        head = dot(hidden, whead[b])
        total = head if total is None else total + head
    left = jnp.ones((rays, LANES), F32)
    colour = jnp.zeros((rays, LANES), F32)
    depth = jnp.zeros((rays, LANES), F32)
    for s in range(samples):
        own = total[s * rays : (s + 1) * rays]
        optical = STEP * softplus(own[:, LANES:])
        through, stop = fade(optical)
        colour = colour + (left * stop) * own[:, :LANES]
        left = left * through
        depth = depth + optical
    return colour, depth


def split16(x):
    high = x.astype(BF16).astype(F32)
    return high, x - high


def depth_rows(depth):
    turned = depth.T
    pair = jnp.concatenate([turned[0:1], turned[LANES // 2 : LANES // 2 + 1]], axis=0)
    high, low = split16(pair)
    return jnp.concatenate([high, low], axis=0)


def field_kernel(cfg, place_ref, own_ref, halo_ref, win_ref, wmid_ref, whead_ref, *rest):
    groups, samples, enc = cfg["groups"], cfg["samples"], cfg["enc"]
    outs = rest[:groups]
    col_own, col_halo, dep_own, dep_halo, tiled = rest[groups:]
    cols, rows_all, rows_dev = cfg["cols"], cfg["rows_all"], cfg["rows_dev"]
    blocks = own_ref.shape[0]
    pad = EDGE * cols
    count = rows_all * cols
    col_own[0:pad, :] = jnp.zeros((pad, LANES), BF16)
    col_own[pad + count :, :] = jnp.zeros((pad, LANES), BF16)
    dep_own[...] = jnp.zeros(dep_own.shape, F32)
    dep_halo[...] = jnp.zeros(dep_halo.shape, F32)
    for b in range(blocks):
        for s in range(samples):
            tiled[b, s * enc : (s + 1) * enc, :] = win_ref[b]
    step = cfg["chunk"]
    for first in range(0, count, step):
        xs = [own_ref[b, first : first + step, :] for b in range(blocks)]
        colour, depth = field_rays(xs, tiled, wmid_ref, whead_ref, samples, enc)
        col_own[pad + first : pad + first + step, :] = colour.astype(BF16)
        for k in range(step // LANES):
            at = 4 * ((pad + first) // LANES + k)
            dep_own[at : at + 4, :] = depth_rows(depth[k * LANES : (k + 1) * LANES])
    xs = [halo_ref[b] for b in range(blocks)]
    colour, depth = field_rays(xs, tiled, wmid_ref, whead_ref, samples, enc)
    col_halo[...] = colour.astype(BF16)
    hrays = depth.shape[0]
    for k in range(cfg["hchunks"]):
        part = depth[k * LANES : min((k + 1) * LANES, hrays)]
        if part.shape[0] < LANES:
            part = jnp.concatenate([part, jnp.zeros((LANES - part.shape[0], LANES), F32)], axis=0)
        dep_halo[4 * k : 4 * k + 4, :] = depth_rows(part)
    n_own, n_halo, n_dep = cfg["n_own"], cfg["n_halo"], cfg["n_dep"]
    place = place_ref[0]
    for s in range(groups):
        dest = cfg["dest"](place, s)
        out = outs[s]
        start = pl.multiple_of(dest * (rows_dev * cols), LANES)
        out[0:n_own, :] = col_own[pl.ds(start, n_own), :]
        start = pl.multiple_of(dest * (rows_dev * 2 * EDGE), 16)
        out[n_own : n_own + n_halo, :] = col_halo[pl.ds(start, n_halo), :]
        start = pl.multiple_of(dest * (4 * rows_dev * cols // LANES), 8)
        at = n_own + n_halo
        out[at : at + n_dep, :] = dep_own[pl.ds(start, n_dep), :].astype(BF16)
        out[at + n_dep :, :] = dep_halo[...].astype(BF16)


def decoder_kernel(cfg, info_ref, w0_ref, w1_ref, w2_ref, w3_ref, *rest):
    groups, nb = cfg["groups"], cfg["nb"]
    bufs = rest[:groups]
    out_ref = rest[groups]
    comp, x0, sa, xa, xc, rep = rest[groups + 1 : groups + 7]
    rank_ref = rest[groups + 7]
    cols, rows_dev, pitch = cfg["cols"], cfg["rows_dev"], cfg["pitch"]
    n_own, n_halo, n_dep = cfg["n_own"], cfg["n_halo"], cfg["n_dep"]
    rows_in = rows_dev + 2 * EDGE
    rows_mid = rows_dev + 2
    mid = rows_mid * pitch
    half = LANES // 2
    per_dev = nb // groups
    place = info_ref[0]
    left_open, right_open = info_ref[1].astype(F32), info_ref[2].astype(F32)
    top_open, bottom_open = info_ref[3].astype(F32), info_ref[4].astype(F32)

    earlier = []
    for side in range(3):
        for k in range(nb):
            rank_ref[info_ref[8 + side * nb + k]] = k
        wide = 2 * per_dev * groups
        row = jnp.zeros((nb, wide), jnp.int32)
        column = jnp.zeros((nb, wide), jnp.int32)
        lane = lax.broadcasted_iota(jnp.int32, (nb, wide), 1)
        sub = lax.broadcasted_iota(jnp.int32, (nb, wide), 0)
        for s in range(groups):
            source = cfg["source"](place, s)
            for i in range(per_dev):
                rank = rank_ref[source * per_dev + i]
                at = s * 2 * per_dev + i
                row = jnp.where((lane == at) | (lane == at + per_dev), rank, row)
                column = jnp.where(sub == s * per_dev + i, rank, column)
        earlier.append(jnp.where(row < column, 1.0, 0.0).astype(BF16))

    at = n_own + n_halo
    own_rows = [bufs[s][at : at + n_dep, :].astype(F32) for s in range(groups)]
    halo_rows = [bufs[s][at + n_dep :, :].astype(F32) for s in range(groups)]
    chunks = n_own // LANES
    factors = []
    for k in range(chunks):
        stack = jnp.concatenate([own_rows[s][4 * k : 4 * k + 4] for s in range(groups)], axis=0)
        factors.append(jnp.exp(-dot(earlier[0], stack.astype(BF16))))
    lane = lax.broadcasted_iota(jnp.int32, (nb, LANES), 1)
    on_left = (lane & (2 * EDGE - 1)) < EDGE
    for k in range(cfg["hchunks"]):
        stack = jnp.concatenate(
            [halo_rows[s][4 * k : 4 * k + 4] for s in range(groups)], axis=0
        ).astype(BF16)
        from_left = jnp.exp(-dot(earlier[1], stack)) * left_open
        from_right = jnp.exp(-dot(earlier[2], stack)) * right_open
        factors.append(jnp.where(on_left, from_left, from_right))
    used = len(factors) * nb
    factors.append(jnp.zeros((LANES - used, LANES), F32))
    turned = jnp.concatenate(factors, axis=0).T
    high, low = split16(turned)
    high, low = high.astype(BF16), low.astype(BF16)

    def spread(k):
        r = lax.broadcasted_iota(jnp.int32, (LANES, groups * LANES), 0)
        c = lax.broadcasted_iota(jnp.int32, (LANES, groups * LANES), 1)
        pick = jnp.where(r - k * nb == c // half, 1.0, 0.0).astype(BF16)
        return dot(high, pick) + dot(low, pick)

    def mix(weights, lo, n):
        acc = None
        for s in range(groups):
            term = weights[:, s * LANES : (s + 1) * LANES] * bufs[s][lo : lo + n, :].astype(F32)
            acc = term if acc is None else acc + term
        return acc + pltpu.roll(acc, half, 1)

    comp[...] = jnp.zeros(comp.shape, F32)
    base = pitch
    per_chunk = LANES // cols
    for k in range(chunks):
        mixed = mix(spread(k), k * LANES, LANES)
        for t in range(per_chunk):
            q = base + (k * per_chunk + t) * pitch + LEAD
            comp[q : q + cols, :] = mixed[t * cols : (t + 1) * cols]
    for k in range(cfg["hchunks"]):
        rep[k * LANES : (k + 1) * LANES, :] = spread(chunks + k)
    start = pl.multiple_of(place * (rows_dev * 2 * EDGE), 16)
    mixed = mix(rep[pl.ds(start, n_halo), :], n_own, n_halo)
    for r in range(rows_in):
        q = base + r * pitch + LEAD
        comp[q - EDGE : q, :] = mixed[r * 2 * EDGE : r * 2 * EDGE + EDGE]
        comp[q + cols : q + cols + EDGE, :] = mixed[r * 2 * EDGE + EDGE : (r + 1) * 2 * EDGE]

    n_in = rows_in * pitch
    lane = lax.broadcasted_iota(jnp.int32, (n_in, LANES), 1)
    here = jnp.where(lane < half, comp[base - 1 : base - 1 + n_in, :], comp[base : base + n_in, :])
    x0[:, 0:LANES] = here.astype(BF16)
    x0[:, LANES : 2 * LANES] = comp[base + 1 : base + 1 + n_in, :].astype(BF16)

    q = lax.broadcasted_iota(jnp.int32, (mid, 2 * LANES), 0)
    pos = q
    for r in range(1, rows_mid):
        pos = pos - jnp.where(q >= r * pitch, pitch, 0)
    mask = jnp.where(pos < LEAD, left_open, jnp.where(pos >= LEAD + cols, right_open, 1.0))
    mask = mask * jnp.where(q < pitch, top_open, jnp.where(q >= mid - pitch, bottom_open, 1.0))

    def windows(ref, pieces):
        return jnp.concatenate(
            [ref[r * pitch : r * pitch + n, a:b] for r, n, a, b in pieces], axis=1
        )

    wide = 2 * LANES
    lhs = windows(x0, [(d, mid, 0, wide) for d in range(3)])
    value = jnp.maximum(dot_t(lhs, w0_ref[...]), 0.0) * mask

    sa[0:8, :] = jnp.zeros((8, wide), F32)
    sa[8 + mid :, :] = jnp.zeros((8, wide), F32)
    three = 3 * LANES
    xa[0:pitch, :] = jnp.zeros((pitch, 2 * three), BF16)
    xa[pitch + mid :, :] = jnp.zeros((pitch, 2 * three), BF16)

    def lay_out(value):
        sa[8 : 8 + mid, :] = value
        for pr in range(2):
            for d in range(3):
                c = pr * three + d * LANES
                xa[pitch : pitch + mid, c : c + LANES] = sa[
                    7 + d : 7 + d + mid, pr * LANES : (pr + 1) * LANES
                ].astype(BF16)

    lay_out(value)
    lhs = windows(
        xa, [(0, mid, three, 2 * three), (1, mid, 0, 2 * three), (2, mid, 0, three)]
    )
    value = jnp.maximum(dot_t(lhs, w1_ref[...]), 0.0) * mask
    lay_out(value)
    for pr in range(2):
        for pc in range(2):
            where = [(0, 1), (1, 0), (1, 1)] if pr == 0 else [(1, 0), (1, 1), (2, 0)]
            lhs = windows(
                xa,
                [(d, mid, p * three + pc * LANES, p * three + pc * LANES + wide) for d, p in where],
            )
            value = jnp.maximum(dot_t(lhs, w2_ref[pc]), 0.0) * mask
            sa[8 : 8 + mid, :] = value
            for rr in range(2):
                at = (2 * pr + rr) * 4 * LANES
                tile = value[:, rr * LANES : (rr + 1) * LANES]
                xc[:, at + (1 + pc) * LANES : at + (2 + pc) * LANES] = tile.astype(BF16)
                slot, move = (3, 9) if pc == 0 else (0, 7)
                xc[:, at + slot * LANES : at + (slot + 1) * LANES] = sa[
                    move : move + mid, rr * LANES : (rr + 1) * LANES
                ].astype(BF16)
    n_out = rows_dev * pitch
    four = 4 * LANES
    lhs = windows(
        xc, [(0, n_out, 3 * four, 4 * four), (1, n_out, 0, 4 * four), (2, n_out, 0, four)]
    )
    final = dot_t(lhs, w3_ref[...])
    final = final + pltpu.roll(final, half, 1)
    rays = jnp.concatenate(
        [final[r * pitch + LEAD : r * pitch + LEAD + cols] for r in range(rows_dev)], axis=0
    )
    turned = rays.T
    stack = jnp.concatenate(
        [
            jnp.concatenate(
                [turned[16 * v : 16 * v + 16, r * cols : (r + 1) * cols] for v in range(4)], axis=1
            )
            for r in range(rows_dev)
        ],
        axis=0,
    )
    r = lax.broadcasted_iota(jnp.int32, (4 * cols, 4 * cols), 0)
    c = lax.broadcasted_iota(jnp.int32, (4 * cols, 4 * cols), 1)
    place_of = (c & 3) * cols + (c >> 2)
    pick = jnp.where(r == place_of, 1.0, 0.0).astype(BF16)
    high, low = split16(stack)
    image = dot(high.astype(BF16), pick) + dot(low.astype(BF16), pick)
    colours = out_ref.shape[0]
    for r in range(rows_dev):
        for u in range(4):
            for p in range(colours):
                at = r * 16 + u * colours + p
                out_ref[p, 4 * r + u : 4 * r + u + 1, :] = image[at : at + 1, :]


def phase_taps():
    t = np.zeros((2, 3, 3), np.float32)
    for p in range(2):
        for a in range(3):
            t[p, (p + a - 1) // 2 + 1, a] = 1
    return t


def decoder_weights(w_conv, w_color):
    feat = w_conv.shape[-1]
    w = w_conv.reshape(w_conv.shape[0], 9, feat, feat)
    t = phase_taps()

    def build(table, kernel):
        n, k = table.shape[:2]
        made = jnp.einsum(
            "nkt,toc->nokc", jnp.asarray(table, BF16), kernel, preferred_element_type=F32
        )
        return made.astype(BF16).reshape(n * feat, k * feat)

    t0 = np.zeros((2, 2, 3, 4, 3, 3), np.float32)
    t0[:, :, :, :3] = np.einsum("pda,qfe->pqdfae", t, t)
    w0 = build(t0.reshape(4, 12, 9), w[0])
    t1 = np.zeros((2, 2, 4, 6, 3, 3), np.float32)
    for p in range(2):
        for q in range(2):
            for a in range(3):
                for e in range(3):
                    t1[p, q, p + a, q + e + 1, a, e] = 1
    w1 = build(t1.reshape(4, 24, 9), w[1])
    both = []
    for pc in range(2):
        t2 = np.zeros((2, 2, 3, 4, 3, 3), np.float32)
        t2[:, :, :, 1 - pc : 4 - pc] = np.einsum("pda,qfe->pqdfae", t, t)
        both.append(build(t2.reshape(4, 12, 9), w[2]))
    w2 = jnp.stack(both)
    colours = w_color.shape[0]
    mixed = jnp.einsum(
        "po,aeoc->paec",
        w_color.astype(F32),
        w_conv[3].astype(F32),
        precision=lax.Precision.HIGHEST,
    )
    rows = []
    for v in range(4):
        for u in range(4):
            own = jnp.pad(mixed, ((0, 0), (u, 3 - u), (v + 1, 4 - v), (0, 0)))
            rows.append(own)
        rows.append(jnp.zeros((16 - 4 * colours,) + rows[-1].shape[1:], F32))
    w3 = jnp.concatenate(rows, axis=0)
    w3 = w3.reshape(w3.shape[0], -1)
    high = w3.astype(BF16)
    low = (w3 - high.astype(F32)).astype(BF16)
    return w0, w1, w2, jnp.concatenate([high, low], axis=0)


def body(samples_in, block_order, seam_link, w_in, w_mid, w_feat, w_density, w_conv, w_color):
    blk_dev, rows_all, cols, width = samples_in.shape
    groups, place = lax.axis_size("block"), lax.axis_index("block")
    patches, patch = lax.axis_size("patch"), lax.axis_index("patch")
    nb = block_order.shape[1]
    enc = w_in.shape[1]
    feat = w_feat.shape[2]
    rows_dev = rows_all // groups
    count = rows_all * cols
    power = groups & (groups - 1) == 0
    hrays = (rows_all + 2 * EDGE) * 2 * EDGE
    hchunks = -(-hrays // LANES)
    n_own = (rows_dev + 2 * EDGE) * cols
    n_halo = (rows_dev + 2 * EDGE) * 2 * EDGE
    n_dep = 4 * n_own // LANES
    n_tail = 16
    cfg = dict(
        groups=groups,
        nb=nb,
        samples=width // enc,
        enc=enc,
        cols=cols,
        rows_all=rows_all,
        rows_dev=rows_dev,
        pitch=cols + 16,
        chunk=2 * LANES,
        n_own=n_own,
        n_halo=n_halo,
        n_dep=n_dep,
        hchunks=hchunks,
        dest=(lambda p, s: p ^ s) if power else (lambda p, s: lax.rem(p + s, groups)),
        source=(lambda p, s: p ^ s) if power else (lambda p, s: lax.rem(p + groups - s, groups)),
    )

    odd = (patch & 1) == 1
    edge_l = samples_in[:, :, :EDGE].reshape(-1, width)
    edge_r = samples_in[:, :, cols - EDGE :].reshape(-1, width)
    meta = jnp.concatenate([block_order[0], seam_link]).astype(BF16)
    meta = jnp.pad(meta[None, :], ((0, 15), (0, width - nb - 1)))
    near = jnp.concatenate([jnp.where(odd, edge_l, edge_r), meta], axis=0)
    far = jnp.concatenate([jnp.where(odd, edge_r, edge_l), meta], axis=0)
    swap_near = [(i, i ^ 1) for i in range(patches) if i ^ 1 < patches]
    swap_far = []
    for i in range(1, patches - 1, 2):
        swap_far += [(i, i + 1), (i + 1, i)]
    far = lax.ppermute(far, "patch", swap_far)
    near = lax.ppermute(near, "patch", swap_near)
    from_left = jnp.where(odd, near, far)
    from_right = jnp.where(odd, far, near)
    edges = blk_dev * rows_all * EDGE
    halo = jnp.concatenate(
        [
            from_left[:edges].reshape(blk_dev, rows_all, EDGE, width),
            from_right[:edges].reshape(blk_dev, rows_all, EDGE, width),
        ],
        axis=2,
    )
    halo = jnp.pad(halo, ((0, 0), (EDGE, EDGE), (0, 0), (0, 0))).reshape(blk_dev, hrays, width)
    order_l = from_left[edges, : nb + 1].astype(jnp.int32)
    order_r = from_right[edges, : nb + 1].astype(jnp.int32)
    flags = jnp.stack(
        [
            place,
            order_l[nb] * (patch > 0),
            seam_link[0] * (patch < patches - 1),
            place > 0,
            place < groups - 1,
            place * 0,
            place * 0,
            place * 0,
        ]
    ).astype(jnp.int32)
    info = jnp.concatenate([flags, block_order[0], order_l[:nb], order_r[:nb]])

    heads = []
    for b in range(blk_dev):
        dens = jnp.broadcast_to(w_density[b][:, None], (w_density.shape[1], feat))
        blank = jnp.zeros_like(dens)
        parts = [blank] * (2 * blk_dev)
        parts[b] = w_feat[b]
        parts[blk_dev + b] = dens
        heads.append(jnp.concatenate(parts, axis=1))
    whead = jnp.stack(heads)

    size = n_own + n_halo + n_dep + n_tail
    smem = pl.BlockSpec(memory_space=pltpu.SMEM)
    vmem = pl.BlockSpec(memory_space=pltpu.VMEM)
    bufs = pl.pallas_call(
        functools.partial(field_kernel, cfg),
        out_shape=[jax.ShapeDtypeStruct((size, LANES), BF16)] * groups,
        in_specs=[smem] + [vmem] * 5,
        out_specs=[vmem] * groups,
        scratch_shapes=[
            pltpu.VMEM((count + 2 * EDGE * cols, LANES), BF16),
            pltpu.VMEM((hrays, LANES), BF16),
            pltpu.VMEM((4 * (count + 2 * EDGE * cols) // LANES, LANES), F32),
            pltpu.VMEM((n_tail, LANES), F32),
            pltpu.VMEM((blk_dev, width, w_in.shape[2]), BF16),
        ],
        name="field",
    )(jnp.reshape(place, (1,)), samples_in.reshape(blk_dev, count, width), halo, w_in, w_mid, whead)

    got = [bufs[0]]
    for s in range(1, groups):
        if power:
            route = [(i, i ^ s) for i in range(groups)]
        else:
            route = [(i, (i + s) % groups) for i in range(groups)]
        got.append(lax.ppermute(bufs[s], "block", route))

    w0, w1, w2, w3 = decoder_weights(w_conv, w_color)
    pitch = cfg["pitch"]
    rows_in, rows_mid = rows_dev + 2 * EDGE, rows_dev + 2
    return pl.pallas_call(
        functools.partial(decoder_kernel, cfg),
        out_shape=jax.ShapeDtypeStruct((w_color.shape[0], 4 * rows_dev, 4 * cols), F32),
        in_specs=[smem] + [vmem] * (4 + groups),
        out_specs=vmem,
        scratch_shapes=[
            pltpu.VMEM(((rows_in + 2) * pitch, LANES), F32),
            pltpu.VMEM((rows_in * pitch, 2 * LANES), BF16),
            pltpu.VMEM((rows_mid * pitch + 16, 2 * LANES), F32),
            pltpu.VMEM(((rows_mid + 2) * pitch, 6 * LANES), BF16),
            pltpu.VMEM((rows_mid * pitch, 16 * LANES), BF16),
            pltpu.VMEM((hchunks * LANES, groups * LANES), F32),
            pltpu.SMEM((nb,), jnp.int32),
        ],
        name="decoder",
    )(info, w0, w1, w2, w3, *got)


def solution(mesh):
    return jax.shard_map(
        body,
        mesh=mesh,
        in_specs=(
            P("block", None, "patch", None),
            P("patch", None),
            P("patch"),
            P("block", None, None),
            P("block", None, None, None),
            P("block", None, None),
            P("block", None),
            P(),
            P(),
        ),
        out_specs=P(None, "block", "patch"),
        check_vma=False,
    )
```

```python
import functools

import jax
import jax.numpy as jnp
from jax import lax
from jax.experimental import pallas as pl
from jax.experimental.pallas import tpu as pltpu
from jax.sharding import PartitionSpec as P

STEP = 0.03
LANES = 128
EDGE = 2
LEAD = 8
F32 = jnp.float32
BF16 = jnp.bfloat16


def dot(a, b):
    return jnp.dot(a, b, preferred_element_type=F32)


def dot_t(a, b):
    return lax.dot_general(a, b, (((1,), (1,)), ((), ())), preferred_element_type=F32)


def relu16(x):
    return jnp.maximum(x, 0.0).astype(BF16)


def softplus(v):
    e = jnp.exp(-jnp.abs(v))
    tail = jnp.where(e < 1e-3, e * (1.0 - e * (0.5 - e * (1.0 / 3.0))), jnp.log(1.0 + e))
    return jnp.maximum(v, 0.0) + tail


def fade(optical):
    through = jnp.exp(-optical)
    small = optical * (1.0 - optical * (0.5 - optical * (1.0 / 6.0 - optical * (1.0 / 24.0))))
    return through, jnp.where(optical < 0.0625, small, 1.0 - through)


def field_rays(xs, win, wmid, whead, samples, enc):
    rays = xs[0].shape[0]
    lane = lax.broadcasted_iota(jnp.int32, xs[0].shape, 1)
    total = None
    for b, x in enumerate(xs):
        zero = jnp.zeros_like(x)
        parts = [
            jnp.where((lane >= s * enc) & (lane < (s + 1) * enc), x, zero) for s in range(samples)
        ]
        hidden = relu16(dot(jnp.concatenate(parts, axis=0), win[b]))
        hidden = relu16(dot(hidden, wmid[b, 0]))
        hidden = relu16(dot(hidden, wmid[b, 1]))
        head = dot(hidden, whead[b])
        total = head if total is None else total + head
    left = jnp.ones((rays, LANES), F32)
    colour = jnp.zeros((rays, LANES), F32)
    depth = jnp.zeros((rays, LANES), F32)
    for s in range(samples):
        own = total[s * rays : (s + 1) * rays]
        optical = STEP * softplus(own[:, LANES:])
        through, stop = fade(optical)
        colour = colour + (left * stop) * own[:, :LANES]
        left = left * through
        depth = depth + optical
    return colour, depth


def split16(x):
    high = x.astype(BF16).astype(F32)
    return high, x - high


def depth_rows(depth):
    turned = depth.T
    pair = jnp.concatenate([turned[0:1], turned[LANES // 2 : LANES // 2 + 1]], axis=0)
    high, low = split16(pair)
    return jnp.concatenate([high, low], axis=0)


def field_kernel(cfg, at_ref, own_ref, near_ref, far_ref, win_ref, wmid_ref, wf_ref, wd_ref, *rest):
    groups, samples, enc = cfg["groups"], cfg["samples"], cfg["enc"]
    outs = rest[:groups]
    col_own, col_halo, dep_own, dep_halo, tiled, whead_ref, halo_ref = rest[groups:]
    cols, rows_all, rows_dev = cfg["cols"], cfg["rows_all"], cfg["rows_dev"]
    blocks = own_ref.shape[0]
    pad = EDGE * cols
    count = rows_all * cols
    col_own[0:pad, :] = jnp.zeros((pad, LANES), BF16)
    col_own[pad + count :, :] = jnp.zeros((pad, LANES), BF16)
    dep_own[...] = jnp.zeros(dep_own.shape, F32)
    dep_halo[...] = jnp.zeros(dep_halo.shape, F32)
    for b in range(blocks):
        for s in range(samples):
            tiled[b, s * enc : (s + 1) * enc, :] = win_ref[b]
    feat, width = wf_ref.shape[2], wf_ref.shape[1]
    dens = wd_ref[...].astype(F32)
    for b in range(blocks):
        r = lax.broadcasted_iota(jnp.int32, (feat, 2 * LANES), 0)
        c = lax.broadcasted_iota(jnp.int32, (feat, 2 * LANES), 1)
        lift = jnp.where(c - b * feat == r, 1.0, 0.0).astype(BF16)
        r = lax.broadcasted_iota(jnp.int32, (width, width), 0)
        c = lax.broadcasted_iota(jnp.int32, (width, width), 1)
        diag = jnp.where(r == c, dens[b : b + 1], 0.0).astype(BF16)
        c = lax.broadcasted_iota(jnp.int32, (width, 2 * LANES), 1)
        repeat = jnp.where((c - LANES) // feat == b, 1.0, 0.0).astype(BF16)
        whead_ref[b] = (dot(wf_ref[b], lift) + dot(diag, repeat)).astype(BF16)
    odd = at_ref[1] == 1
    near, far = near_ref[...].astype(F32), far_ref[...].astype(F32)
    sides = [jnp.where(odd, near, far), jnp.where(odd, far, near)]
    side_rays = rows_all * EDGE
    side_pitch = side_rays + 2 * EDGE * EDGE
    halo_ref[...] = jnp.zeros(halo_ref.shape, F32)
    for b in range(blocks):
        for i, side in enumerate(sides):
            q = i * side_pitch + EDGE * EDGE
            halo_ref[b, q : q + side_rays, :] = side[b * side_rays : (b + 1) * side_rays]
    step = cfg["chunk"]
    for first in range(0, count, step):
        xs = [own_ref[b, first : first + step, :] for b in range(blocks)]
        colour, depth = field_rays(xs, tiled, wmid_ref, whead_ref, samples, enc)
        col_own[pad + first : pad + first + step, :] = colour.astype(BF16)
        for k in range(step // LANES):
            at = 4 * ((pad + first) // LANES + k)
            dep_own[at : at + 4, :] = depth_rows(depth[k * LANES : (k + 1) * LANES])
    xs = [halo_ref[b].astype(BF16) for b in range(blocks)]
    colour, depth = field_rays(xs, tiled, wmid_ref, whead_ref, samples, enc)
    col_halo[...] = colour
    hrays = depth.shape[0]
    for k in range(cfg["hchunks"]):
        part = depth[k * LANES : min((k + 1) * LANES, hrays)]
        if part.shape[0] < LANES:
            part = jnp.concatenate([part, jnp.zeros((LANES - part.shape[0], LANES), F32)], axis=0)
        dep_halo[4 * k : 4 * k + 4, :] = depth_rows(part)
    n_own, n_halo, n_dep = cfg["n_own"], cfg["n_halo"], cfg["n_dep"]
    place = at_ref[0]
    half = n_halo // 2
    for s in range(groups):
        dest = cfg["dest"](place, s)
        out = outs[s]
        start = pl.multiple_of(dest * (rows_dev * cols), LANES)
        out[0:n_own, :] = col_own[pl.ds(start, n_own), :]
        for i in range(2):
            start = pl.multiple_of(i * side_pitch + dest * (rows_dev * EDGE), 8)
            q = n_own + i * half
            out[q : q + half, :] = col_halo[pl.ds(start, half), :].astype(BF16)
        start = pl.multiple_of(dest * (4 * rows_dev * cols // LANES), 8)
        at = n_own + n_halo
        out[at : at + n_dep, :] = dep_own[pl.ds(start, n_dep), :].astype(BF16)
        out[at + n_dep :, :] = dep_halo[...].astype(BF16)


def decoder_kernel(cfg, info_ref, w0_ref, w1_ref, w2_ref, w3_ref, *rest):
    groups, nb = cfg["groups"], cfg["nb"]
    bufs = rest[:groups]
    out_ref = rest[groups]
    comp, x0, sa, xa, xc, rep = rest[groups + 1 : groups + 7]
    rank_ref = rest[groups + 7]
    cols, rows_dev, pitch = cfg["cols"], cfg["rows_dev"], cfg["pitch"]
    n_own, n_halo, n_dep = cfg["n_own"], cfg["n_halo"], cfg["n_dep"]
    rows_in = rows_dev + 2 * EDGE
    rows_mid = rows_dev + 2
    mid = rows_mid * pitch
    half = LANES // 2
    per_dev = nb // groups
    place = info_ref[0]
    left_open, right_open = info_ref[1].astype(F32), info_ref[2].astype(F32)
    top_open, bottom_open = info_ref[3].astype(F32), info_ref[4].astype(F32)

    earlier = []
    for side in range(3):
        for k in range(nb):
            rank_ref[info_ref[8 + side * nb + k]] = k
        wide = 2 * per_dev * groups
        row = jnp.zeros((nb, wide), jnp.int32)
        column = jnp.zeros((nb, wide), jnp.int32)
        lane = lax.broadcasted_iota(jnp.int32, (nb, wide), 1)
        sub = lax.broadcasted_iota(jnp.int32, (nb, wide), 0)
        for s in range(groups):
            source = cfg["source"](place, s)
            for i in range(per_dev):
                rank = rank_ref[source * per_dev + i]
                at = s * 2 * per_dev + i
                row = jnp.where((lane == at) | (lane == at + per_dev), rank, row)
                column = jnp.where(sub == s * per_dev + i, rank, column)
        earlier.append(jnp.where(row < column, 1.0, 0.0).astype(BF16))

    at = n_own + n_halo
    own_rows = [bufs[s][at : at + n_dep, :].astype(F32) for s in range(groups)]
    halo_rows = [bufs[s][at + n_dep :, :].astype(F32) for s in range(groups)]
    chunks = n_own // LANES
    factors = []
    for k in range(chunks):
        stack = jnp.concatenate([own_rows[s][4 * k : 4 * k + 4] for s in range(groups)], axis=0)
        factors.append(jnp.exp(-dot(earlier[0], stack.astype(BF16))))
    lane = lax.broadcasted_iota(jnp.int32, (nb, LANES), 1)
    side_pitch = (cfg["rows_all"] + 2 * EDGE) * EDGE
    for k in range(cfg["hchunks"]):
        on_left = lane + k * LANES < side_pitch
        stack = jnp.concatenate(
            [halo_rows[s][4 * k : 4 * k + 4] for s in range(groups)], axis=0
        ).astype(BF16)
        from_left = jnp.exp(-dot(earlier[1], stack)) * left_open
        from_right = jnp.exp(-dot(earlier[2], stack)) * right_open
        factors.append(jnp.where(on_left, from_left, from_right))
    used = len(factors) * nb
    factors.append(jnp.zeros((LANES - used, LANES), F32))
    turned = jnp.concatenate(factors, axis=0).T
    high, low = split16(turned)
    high, low = high.astype(BF16), low.astype(BF16)

    def spread(k):
        r = lax.broadcasted_iota(jnp.int32, (LANES, groups * LANES), 0)
        c = lax.broadcasted_iota(jnp.int32, (LANES, groups * LANES), 1)
        pick = jnp.where(r - k * nb == c // half, 1.0, 0.0).astype(BF16)
        return dot(high, pick) + dot(low, pick)

    def mix(weights, lo, n):
        acc = None
        for s in range(groups):
            term = weights[:, s * LANES : (s + 1) * LANES] * bufs[s][lo : lo + n, :].astype(F32)
            acc = term if acc is None else acc + term
        return acc + pltpu.roll(acc, half, 1)

    comp[...] = jnp.zeros(comp.shape, F32)
    base = pitch
    per_chunk = LANES // cols
    for k in range(chunks):
        mixed = mix(spread(k), k * LANES, LANES)
        for t in range(per_chunk):
            q = base + (k * per_chunk + t) * pitch + LEAD
            comp[q : q + cols, :] = mixed[t * cols : (t + 1) * cols]
    for k in range(cfg["hchunks"]):
        rep[k * LANES : (k + 1) * LANES, :] = spread(chunks + k)
    size = n_halo // 2
    for i in range(2):
        start = pl.multiple_of(i * side_pitch + place * (rows_dev * EDGE), 8)
        mixed = mix(rep[pl.ds(start, size), :], n_own + i * size, size)
        for r in range(rows_in):
            q = base + r * pitch + LEAD + (cols if i else -EDGE)
            comp[q : q + EDGE, :] = mixed[r * EDGE : (r + 1) * EDGE]

    n_in = rows_in * pitch
    lane = lax.broadcasted_iota(jnp.int32, (n_in, LANES), 1)
    here = jnp.where(lane < half, comp[base - 1 : base - 1 + n_in, :], comp[base : base + n_in, :])
    x0[:, 0:LANES] = here.astype(BF16)
    x0[:, LANES : 2 * LANES] = comp[base + 1 : base + 1 + n_in, :].astype(BF16)

    q = lax.broadcasted_iota(jnp.int32, (mid, 2 * LANES), 0)
    pos = q
    for r in range(1, rows_mid):
        pos = pos - jnp.where(q >= r * pitch, pitch, 0)
    mask = jnp.where(pos < LEAD, left_open, jnp.where(pos >= LEAD + cols, right_open, 1.0))
    mask = mask * jnp.where(q < pitch, top_open, jnp.where(q >= mid - pitch, bottom_open, 1.0))

    def windows(ref, pieces):
        return jnp.concatenate(
            [ref[r * pitch : r * pitch + n, a:b] for r, n, a, b in pieces], axis=1
        )

    wide = 2 * LANES
    lhs = windows(x0, [(d, mid, 0, wide) for d in range(3)])
    value = jnp.maximum(dot_t(lhs, w0_ref[...]), 0.0) * mask

    sa[0:8, :] = jnp.zeros((8, wide), F32)
    sa[8 + mid :, :] = jnp.zeros((8, wide), F32)
    three = 3 * LANES
    xa[0:pitch, :] = jnp.zeros((pitch, 2 * three), BF16)
    xa[pitch + mid :, :] = jnp.zeros((pitch, 2 * three), BF16)

    def lay_out(value):
        sa[8 : 8 + mid, :] = value
        for pr in range(2):
            for d in range(3):
                c = pr * three + d * LANES
                xa[pitch : pitch + mid, c : c + LANES] = sa[
                    7 + d : 7 + d + mid, pr * LANES : (pr + 1) * LANES
                ].astype(BF16)

    lay_out(value)
    lhs = windows(
        xa, [(0, mid, three, 2 * three), (1, mid, 0, 2 * three), (2, mid, 0, three)]
    )
    value = jnp.maximum(dot_t(lhs, w1_ref[...]), 0.0) * mask
    lay_out(value)
    for pr in range(2):
        for pc in range(2):
            where = [(0, 1), (1, 0), (1, 1)] if pr == 0 else [(1, 0), (1, 1), (2, 0)]
            lhs = windows(
                xa,
                [(d, mid, p * three + pc * LANES, p * three + pc * LANES + wide) for d, p in where],
            )
            value = jnp.maximum(dot_t(lhs, w2_ref[pc]), 0.0) * mask
            sa[8 : 8 + mid, :] = value
            for rr in range(2):
                at = (2 * pr + rr) * 4 * LANES
                tile = value[:, rr * LANES : (rr + 1) * LANES]
                xc[:, at + (1 + pc) * LANES : at + (2 + pc) * LANES] = tile.astype(BF16)
                slot, move = (3, 9) if pc == 0 else (0, 7)
                xc[:, at + slot * LANES : at + (slot + 1) * LANES] = sa[
                    move : move + mid, rr * LANES : (rr + 1) * LANES
                ].astype(BF16)
    n_out = rows_dev * pitch
    four = 4 * LANES
    lhs = windows(
        xc, [(0, n_out, 3 * four, 4 * four), (1, n_out, 0, 4 * four), (2, n_out, 0, four)]
    )
    final = dot_t(lhs, w3_ref[...])
    final = final + pltpu.roll(final, half, 1)
    rays = jnp.concatenate(
        [final[r * pitch + LEAD : r * pitch + LEAD + cols] for r in range(rows_dev)], axis=0
    )
    turned = rays.T
    stack = jnp.concatenate(
        [
            jnp.concatenate(
                [turned[16 * v : 16 * v + 16, r * cols : (r + 1) * cols] for v in range(4)], axis=1
            )
            for r in range(rows_dev)
        ],
        axis=0,
    )
    r = lax.broadcasted_iota(jnp.int32, (4 * cols, 4 * cols), 0)
    c = lax.broadcasted_iota(jnp.int32, (4 * cols, 4 * cols), 1)
    place_of = (c & 3) * cols + (c >> 2)
    pick = jnp.where(r == place_of, 1.0, 0.0).astype(BF16)
    high, low = split16(stack)
    image = dot(high.astype(BF16), pick) + dot(low.astype(BF16), pick)
    colours = out_ref.shape[0]
    for r in range(rows_dev):
        for u in range(4):
            for p in range(colours):
                at = r * 16 + u * 4 + p
                out_ref[p, 4 * r + u : 4 * r + u + 1, :] = image[at : at + 1, :]


def phase_taps(p, d):
    return [a for a in range(3) if (p + a - 1) // 2 + 1 == d]


def weights_kernel(conv_ref, colour_ref, after_ref, w0_ref, w1_ref, w2_ref, w3_ref):
    feat = conv_ref.shape[1]
    r = lax.broadcasted_iota(jnp.int32, (feat, LANES), 0)
    lane = lax.broadcasted_iota(jnp.int32, (feat, LANES), 1)
    twice = jnp.where((lane == r) | (lane == r + feat), 1.0, 0.0).astype(BF16)
    low = lane < feat
    zero = jnp.zeros((feat, LANES), F32)
    taps = [
        dot(conv_ref[k * 9 * feat : (k + 1) * 9 * feat, :], twice) for k in range(4)
    ]

    def tap(k, a, e):
        at = (a * 3 + e) * feat
        return taps[k][at : at + feat]

    def pair(left, right):
        if left is None and right is None:
            return zero
        if left is right:
            return left
        return jnp.where(low, zero if left is None else left, zero if right is None else right)

    def put(ref, n, j, tile):
        ref[n * feat : (n + 1) * feat, j * LANES : (j + 1) * LANES] = tile.astype(BF16)

    for k in (0, 2):
        sums = {}
        for p in range(2):
            for q in range(2):
                for d in range(3):
                    for f in range(3):
                        parts = [tap(k, a, e) for a in phase_taps(p, d) for e in phase_taps(q, f)]
                        sums[p, q, d, f] = functools.reduce(jnp.add, parts) if parts else None
        for p in range(2):
            for q in range(2):
                n = 2 * p + q
                for d in range(3):
                    row = [sums[p, q, d, f] for f in range(3)]
                    layouts = [[None] + row, row + [None]]
                    refs = [w2_ref.at[0], w2_ref.at[1]] if k == 2 else [None, w0_ref]
                    for ref, blocks in zip(refs, layouts):
                        if ref is not None:
                            put(ref, n, 2 * d, pair(blocks[0], blocks[1]))
                            put(ref, n, 2 * d + 1, pair(blocks[2], blocks[3]))

    def pick(table, a, e):
        return table(a, e) if 0 <= a < 3 and 0 <= e < 3 else None

    for p in range(2):
        for q in range(2):
            for row in range(4):
                for j in range(3):
                    blocks = [
                        pick(lambda a, e: tap(1, a, e), row - p, c - 1 - q)
                        for c in (2 * j, 2 * j + 1)
                    ]
                    put(w1_ref, 2 * p + q, row * 3 + j, pair(*blocks))

    colours = colour_ref.shape[0]
    given = colour_ref[...].astype(F32)
    sub = lax.broadcasted_iota(jnp.int32, (8, feat), 0)
    mixer = jnp.zeros((8, feat), F32)
    for p in range(colours):
        mixer = jnp.where((sub & 3) == p, given[p : p + 1], mixer)
    mixer = mixer.astype(BF16)
    mixed = {
        (a, e): dot(mixer, tap(3, a, e).astype(BF16)) for a in range(3) for e in range(3)
    }
    lane = lax.broadcasted_iota(jnp.int32, (8, LANES), 1) < feat
    upper = lax.broadcasted_iota(jnp.int32, (8, LANES), 0) < 4
    blank = jnp.zeros((8, LANES), F32)

    def choose(mask, x, y):
        if x is None and y is None:
            return None
        return jnp.where(mask, blank if x is None else x, blank if y is None else y)

    for row in range(6):
        for j in range(4):
            pieces = []
            for v in range(4):
                for u in (0, 2):
                    halves = [
                        choose(
                            lane,
                            pick(lambda a, e: mixed[a, e], row - w, 2 * j - 1 - v),
                            pick(lambda a, e: mixed[a, e], row - w, 2 * j - v),
                        )
                        for w in (u, u + 1)
                    ]
                    made = choose(upper, *halves)
                    pieces.append(blank if made is None else made)
            tile = jnp.concatenate(pieces, axis=0)
            high, low16 = split16(tile)
            at = (row * 4 + j) * LANES
            w3_ref[:, at : at + LANES] = jnp.concatenate([high, low16], axis=0).astype(BF16)


def body(samples_in, block_order, seam_link, w_in, w_mid, w_feat, w_density, w_conv, w_color):
    blk_dev, rows_all, cols, width = samples_in.shape
    groups, place = lax.axis_size("block"), lax.axis_index("block")
    patches, patch = lax.axis_size("patch"), lax.axis_index("patch")
    nb = block_order.shape[1]
    enc = w_in.shape[1]
    feat = w_feat.shape[2]
    rows_dev = rows_all // groups
    count = rows_all * cols
    power = groups & (groups - 1) == 0
    hrays = (rows_all + 2 * EDGE) * 2 * EDGE
    hchunks = -(-hrays // LANES)
    n_own = (rows_dev + 2 * EDGE) * cols
    n_halo = (rows_dev + 2 * EDGE) * 2 * EDGE
    n_dep = 4 * n_own // LANES
    n_tail = 16
    cfg = dict(
        groups=groups,
        nb=nb,
        samples=width // enc,
        enc=enc,
        cols=cols,
        rows_all=rows_all,
        rows_dev=rows_dev,
        pitch=cols + 16,
        chunk=2 * LANES,
        n_own=n_own,
        n_halo=n_halo,
        n_dep=n_dep,
        hchunks=hchunks,
        dest=(lambda p, s: p ^ s) if power else (lambda p, s: lax.rem(p + s, groups)),
        source=(lambda p, s: p ^ s) if power else (lambda p, s: lax.rem(p + groups - s, groups)),
    )

    odd = (patch & 1) == 1
    edge_l = samples_in[:, :, :EDGE].reshape(-1, width)
    edge_r = samples_in[:, :, cols - EDGE :].reshape(-1, width)
    meta = jnp.concatenate([block_order[0], seam_link]).astype(BF16)
    meta = jnp.pad(meta[None, :], ((0, 15), (0, width - nb - 1)))
    near = jnp.concatenate([jnp.where(odd, edge_l, edge_r), meta], axis=0)
    far = jnp.concatenate([jnp.where(odd, edge_r, edge_l), meta], axis=0)
    swap_near = [(i, i ^ 1) for i in range(patches) if i ^ 1 < patches]
    swap_far = []
    for i in range(1, patches - 1, 2):
        swap_far += [(i, i + 1), (i + 1, i)]
    far = lax.ppermute(far, "patch", swap_far)
    near = lax.ppermute(near, "patch", swap_near)
    edges = blk_dev * rows_all * EDGE
    from_left = jnp.where(odd, near[edges], far[edges])
    from_right = jnp.where(odd, far[edges], near[edges])
    order_l = from_left[: nb + 1].astype(jnp.int32)
    order_r = from_right[: nb + 1].astype(jnp.int32)
    flags = jnp.stack(
        [
            place,
            order_l[nb] * (patch > 0),
            seam_link[0] * (patch < patches - 1),
            place > 0,
            place < groups - 1,
            place * 0,
            place * 0,
            place * 0,
        ]
    ).astype(jnp.int32)
    info = jnp.concatenate([flags, block_order[0], order_l[:nb], order_r[:nb]])

    size = n_own + n_halo + n_dep + n_tail
    params = pltpu.CompilerParams(vmem_limit_bytes=32 * 1024 * 1024)
    smem = pl.BlockSpec(memory_space=pltpu.SMEM)
    vmem = pl.BlockSpec(memory_space=pltpu.VMEM)
    bufs = pl.pallas_call(
        functools.partial(field_kernel, cfg),
        out_shape=[pltpu.VMEM((size, LANES), BF16)] * groups,
        in_specs=[smem] + [vmem] * 7,
        out_specs=[vmem] * groups,
        scratch_shapes=[
            pltpu.VMEM((count + 2 * EDGE * cols, LANES), BF16),
            pltpu.VMEM((hrays, LANES), F32),
            pltpu.VMEM((4 * (count + 2 * EDGE * cols) // LANES, LANES), F32),
            pltpu.VMEM((n_tail, LANES), F32),
            pltpu.VMEM((blk_dev, width, w_in.shape[2]), BF16),
            pltpu.VMEM((blk_dev, w_feat.shape[1], 2 * LANES), BF16),
            pltpu.VMEM((blk_dev, hrays, width), F32),
        ],
        compiler_params=params,
        name="field",
    )(
        jnp.stack([place, patch & 1]),
        samples_in.reshape(blk_dev, count, width),
        near,
        far,
        w_in,
        w_mid,
        w_feat,
        w_density,
    )

    got = [bufs[0]]
    for s in range(1, groups):
        if power:
            route = [(i, i ^ s) for i in range(groups)]
        else:
            route = [(i, (i + s) % groups) for i in range(groups)]
        got.append(lax.ppermute(bufs[s], "block", route))

    w0, w1, w2, w3 = pl.pallas_call(
        weights_kernel,
        out_shape=[
            pltpu.VMEM((4 * feat, 12 * feat), BF16),
            pltpu.VMEM((4 * feat, 24 * feat), BF16),
            pltpu.VMEM((2, 4 * feat, 12 * feat), BF16),
            pltpu.VMEM((2 * feat, 48 * feat), BF16),
        ],
        in_specs=[vmem, vmem, pl.BlockSpec(memory_space=pl.ANY)],
        out_specs=[vmem] * 4,
        compiler_params=params,
        cost_estimate=pl.CostEstimate(flops=10**8, bytes_accessed=10**6, transcendentals=0),
        name="weights",
    )(w_conv.reshape(-1, feat), w_color, bufs[0])
    pitch = cfg["pitch"]
    rows_in, rows_mid = rows_dev + 2 * EDGE, rows_dev + 2
    return pl.pallas_call(
        functools.partial(decoder_kernel, cfg),
        out_shape=jax.ShapeDtypeStruct((w_color.shape[0], 4 * rows_dev, 4 * cols), F32),
        in_specs=[smem] + [vmem] * (4 + groups),
        out_specs=vmem,
        scratch_shapes=[
            pltpu.VMEM(((rows_in + 2) * pitch, LANES), F32),
            pltpu.VMEM((rows_in * pitch, 2 * LANES), BF16),
            pltpu.VMEM((rows_mid * pitch + 16, 2 * LANES), F32),
            pltpu.VMEM(((rows_mid + 2) * pitch, 6 * LANES), BF16),
            pltpu.VMEM((rows_mid * pitch, 16 * LANES), BF16),
            pltpu.VMEM((hchunks * LANES, groups * LANES), F32),
            pltpu.SMEM((nb,), jnp.int32),
        ],
        compiler_params=params,
        name="decoder",
    )(info, w0, w1, w2, w3, *got)


def solution(mesh):
    return jax.shard_map(
        body,
        mesh=mesh,
        in_specs=(
            P("block", None, "patch", None),
            P("patch", None),
            P("patch"),
            P("block", None, None),
            P("block", None, None, None),
            P("block", None, None),
            P("block", None),
            P(),
            P(),
        ),
        out_specs=P(None, "block", "patch"),
        check_vma=False,
    )
```

```python
import functools

import jax
import jax.numpy as jnp
from jax import lax
from jax.experimental import pallas as pl
from jax.experimental.pallas import tpu as pltpu
from jax.sharding import PartitionSpec as P


STEP = 0.03
LANES = 128
EDGE = 2
LEAD = 8
F32 = jnp.float32
BF16 = jnp.bfloat16


def dot(a, b):
    return jnp.dot(a, b, preferred_element_type=F32)


def dot_t(a, b):
    return lax.dot_general(a, b, (((1,), (1,)), ((), ())), preferred_element_type=F32)


def relu16(x):
    return jnp.maximum(x.astype(BF16), jnp.zeros((), BF16))


def softplus(v):
    e = jnp.exp(-jnp.abs(v))
    tail = jnp.where(e < 1e-3, e * (1.0 - e * (0.5 - e * (1.0 / 3.0))), jnp.log(1.0 + e))
    return jnp.maximum(v, 0.0) + tail


def stopped(optical):
    small = optical * (1.0 - optical * (0.5 - optical * (1.0 / 6.0 - optical * (1.0 / 24.0))))
    return jnp.where(optical < 0.0625, small, 1.0 - jnp.exp(-optical))


def split16(x):
    high = x.astype(BF16).astype(F32)
    return high, x - high


def one_hot(shape, test):
    r = lax.broadcasted_iota(jnp.int32, shape, 0)
    c = lax.broadcasted_iota(jnp.int32, shape, 1)
    return jnp.where(test(r, c), 1.0, 0.0).astype(BF16)


def field_heads(xs, tiled, wmid, whead, spread, samples, enc):
    rays = xs[0].shape[0]
    lane = lax.broadcasted_iota(jnp.int32, xs[0].shape, 1)
    heads = [None] * samples
    for b, x in enumerate(xs):
        zero = jnp.zeros_like(x)
        parts = [
            jnp.where((lane >= s * enc) & (lane < (s + 1) * enc), x, zero) for s in range(samples)
        ]
        hidden = relu16(dot(jnp.concatenate(parts, axis=0), tiled[b]))
        hidden = relu16(dot(hidden, wmid[b, 0]))
        hidden = relu16(dot(hidden, wmid[b, 1]))
        for s in range(samples):
            made = dot(hidden[s * rays : (s + 1) * rays], whead[b, s])
            heads[s] = made if b == 0 else heads[s] + made
    return heads


def field_mix(heads, spread):
    samples, rays = len(heads), heads[0].shape[0]
    logit = heads[0][:, LANES:]
    for s in range(1, samples):
        logit = logit + heads[s][:, LANES:]
    optical = STEP * softplus(logit)
    group = LANES // samples
    lane = lax.broadcasted_iota(jnp.int32, (rays, LANES), 1)
    depth, before = optical, jnp.zeros((rays, LANES), F32)
    for s in range(1, samples):
        moved = pltpu.roll(optical, s * group, 1)
        depth = depth + moved
        before = before + jnp.where(lane >= s * group, moved, 0.0)
    weight = jnp.exp(-before) * stopped(optical)
    high, low = split16(weight)
    wide = dot(jnp.concatenate([high.astype(BF16), low.astype(BF16)], axis=1), spread[...])
    colour = None
    for s in range(samples):
        term = wide[:, s * LANES : (s + 1) * LANES] * heads[s][:, :LANES]
        colour = term if colour is None else colour + term
    return colour, depth


def depth_rows(depth, step):
    turned = depth.T
    pair = jnp.concatenate([turned[0:1], turned[step : step + 1]], axis=0)
    high, low = split16(pair)
    return jnp.concatenate([high, low], axis=0)


def edges_kernel(
    cfg, at_ref, order_hbm, seam_hbm, own_hbm, win_hbm, wd_hbm,
    own_ref, win_ref, wd_ref, near_ref, far_ref,
    left, right, order_ref, seam_ref, sems,
):
    cols, rows_all = cfg["cols"], cfg["rows_all"]
    blocks = own_ref.shape[0]
    small = [
        pltpu.make_async_copy(order_hbm, order_ref, sems.at[2]),
        pltpu.make_async_copy(seam_hbm, seam_ref, sems.at[3]),
    ]
    for copy in small:
        copy.start()
    load = pltpu.make_async_copy(own_hbm, own_ref, sems.at[0])
    load.start()
    more = [
        pltpu.make_async_copy(win_hbm, win_ref, sems.at[1]),
        pltpu.make_async_copy(wd_hbm, wd_ref, sems.at[4]),
    ]
    for copy in more:
        copy.start()
    nb = cfg["nb"]
    lane = lax.broadcasted_iota(jnp.int32, (16, LANES), 1)
    for copy in small:
        copy.wait()
    meta = jnp.where(lane == nb, seam_ref[0], 0)
    for k in range(nb):
        meta = jnp.where(lane == k, order_ref[0, k], meta)
    meta = meta.astype(F32).astype(BF16)
    load.wait()
    size = blocks * rows_all * EDGE
    for b in range(blocks):
        for r in range(rows_all):
            q = (b * rows_all + r) * EDGE
            left[q : q + EDGE, :] = own_ref[b, r * cols : r * cols + 16, :].astype(F32)[:EDGE]
            last = own_ref[b, (r + 1) * cols - 16 : (r + 1) * cols, :].astype(F32)
            right[q : q + EDGE, :] = last[16 - EDGE :]
    odd = at_ref[1] == 1
    near_ref[:size, :] = jnp.where(odd, left[...], right[...]).astype(BF16)
    far_ref[:size, :] = jnp.where(odd, right[...], left[...]).astype(BF16)
    near_ref[size:, :] = meta
    far_ref[size:, :] = meta
    for copy in more:
        copy.wait()


def field_chunks(cfg, own_ref, nets, col_own, dep_own, pieces):
    pad = EDGE * cfg["cols"]
    blocks = own_ref.shape[0]

    def start(chunk):
        xs = [
            jnp.concatenate([own_ref[b, pl.ds(at, LANES), :] for at in chunk], axis=0)
            for b in range(blocks)
        ]
        return field_heads(xs, *nets, cfg["samples"], cfg["enc"])

    def finish(chunk, heads):
        colour, depth = field_mix(heads, nets[3])
        for k, at in enumerate(chunk):
            rows = slice(k * LANES, (k + 1) * LANES)
            col_own[pl.ds(pl.multiple_of(at + pad, LANES), LANES), :] = colour[rows].astype(BF16)
            q = pl.multiple_of((at + pad) // LANES * 8, 8)
            dep_own[pl.ds(q, 4), :] = depth_rows(depth[rows], cfg["repeat"])

    waiting = None
    for chunk in pieces:
        heads = start(chunk)
        if waiting is not None:
            finish(*waiting)
        waiting = (chunk, heads)
    finish(*waiting)


def grouped(items, n):
    return [items[i : i + n] for i in range(0, len(items), n)]


def row_pieces(cfg, place, near):
    per = LANES // cfg["cols"]
    chip = place >> 1
    if cfg["groups"] == 4:
        first = jnp.where(chip == 0, 0, cfg["rows_all"] - cfg["n_near"])
    else:
        first = chip * (2 * cfg["rows_dev"]) + EDGE
    n = cfg["n_near"] if near else cfg["rows_all"] - cfg["n_near"]
    first = first if near else first + cfg["n_near"]
    starts = []
    for k in range(n // per):
        row = lax.rem(first + k * per, cfg["rows_all"])
        starts.append(pl.multiple_of(row * cfg["cols"], LANES))
    return starts


def field_kernel(
    cfg, at_ref, own_ref, win_ref, wmid_hbm, wf_ref, wd_ref,
    col_own, dep_own, tiled, whead, spread, wmid_ref, sem,
):
    load = pltpu.make_async_copy(wmid_hbm, wmid_ref, sem)
    load.start()
    samples, enc = cfg["samples"], cfg["enc"]
    blocks = own_ref.shape[0]
    pad = EDGE * cfg["cols"]
    count = cfg["rows_all"] * cfg["cols"]
    col_own[0:pad, :] = jnp.zeros((pad, LANES), BF16)
    col_own[pad + count :, :] = jnp.zeros((pad, LANES), BF16)
    ends = 8 * pad // LANES
    dep_own[0:ends, :] = jnp.zeros((ends, LANES), F32)
    dep_own[dep_own.shape[0] - ends :, :] = jnp.zeros((ends, LANES), F32)
    for b in range(blocks):
        for s in range(samples):
            tiled[b, s * enc : (s + 1) * enc, :] = win_ref[b]
    feat, width = wf_ref.shape[2], wf_ref.shape[1]
    repeat = cfg["repeat"]
    dens = wd_ref[...].astype(F32)
    group = lax.broadcasted_iota(jnp.int32, (width, LANES), 1) // repeat
    for b in range(blocks):
        lift = one_hot((feat, LANES), lambda r, c: c - b * feat == r)
        r = lax.broadcasted_iota(jnp.int32, (width, width), 0)
        c = lax.broadcasted_iota(jnp.int32, (width, width), 1)
        diag = jnp.where(r == c, dens[b : b + 1], 0.0).astype(BF16)
        features = dot(wf_ref[b], lift).astype(BF16)
        column = dot(diag, jnp.ones((width, LANES), BF16))
        for s in range(samples):
            whead[b, s, :, :LANES] = features
            whead[b, s, :, LANES:] = jnp.where(group == s * blocks + b, column, 0.0).astype(BF16)
    spread[...] = one_hot(
        spread.shape, lambda r, c: (r & (LANES - 1)) == c // (LANES // blocks) * repeat
    )
    load.wait()
    nets = (tiled, wmid_ref, whead, spread)
    pieces = row_pieces(cfg, at_ref[0], False)
    field_chunks(cfg, own_ref, nets, col_own, dep_own, grouped(pieces, cfg["chunk"]))


def pack(cfg, place, s, out, col_own, dep_own, col_halo, dep_halo):
    n_own, n_halo, n_dep = cfg["n_own"], cfg["n_halo"], cfg["n_dep"]
    cols, rows_dev = cfg["cols"], cfg["rows_dev"]
    half = n_halo // 2
    dest = place ^ s
    start = pl.multiple_of(dest * (rows_dev * cols), LANES)
    out[0:n_own, :] = col_own[pl.ds(start, n_own), :]
    for i in range(2):
        start = pl.multiple_of(i * cfg["side_pitch"] + dest * (rows_dev * EDGE), 8)
        q = n_own + i * half
        out[q : q + half, :] = col_halo[pl.ds(start, half), :].astype(BF16)
    start = pl.multiple_of(dest * (8 * rows_dev * cols // LANES), 8)
    at = n_own + n_halo
    groups = n_dep // 4
    rows = dep_own[pl.ds(start, 8 * groups), :]
    rows = jnp.concatenate([rows[8 * k : 8 * k + 4] for k in range(groups)], axis=0)
    out[at : at + n_dep, :] = rows.astype(BF16)
    out[at + n_dep :, :] = dep_halo[...].astype(BF16)


def halo_kernel(
    cfg, at_ref, near_ref, far_ref, tiled, wmid_ref, whead, spread, col_own, dep_own, *rest
):
    outs = rest[: cfg["groups"] - 2]
    col_halo, dep_halo, meta, halo_ref = rest[cfg["groups"] - 2 :]
    samples, enc, rows_all = cfg["samples"], cfg["enc"], cfg["rows_all"]
    blocks = halo_ref.shape[0]
    odd = at_ref[1] == 1
    near, far = near_ref[...].astype(F32), far_ref[...].astype(F32)
    sides = [jnp.where(odd, near, far), jnp.where(odd, far, near)]
    side_rays = rows_all * EDGE
    halo_ref[...] = jnp.zeros(halo_ref.shape, F32)
    for b in range(blocks):
        for i, side in enumerate(sides):
            q = i * cfg["side_pitch"] + EDGE * EDGE
            halo_ref[b, q : q + side_rays, :] = side[b * side_rays : (b + 1) * side_rays]
    for i, side in enumerate(sides):
        meta[8 * i : 8 * i + 8, :] = side[blocks * side_rays : blocks * side_rays + 8]
    xs = [halo_ref[b].astype(BF16) for b in range(blocks)]
    heads = field_heads(xs, tiled, wmid_ref, whead, spread, samples, enc)
    colour, depth = field_mix(heads, spread)
    col_halo[...] = colour
    dep_halo[...] = jnp.zeros(dep_halo.shape, F32)
    hrays = depth.shape[0]
    for k in range(cfg["hchunks"]):
        part = depth[k * LANES : min((k + 1) * LANES, hrays)]
        if part.shape[0] < LANES:
            part = jnp.concatenate([part, jnp.zeros((LANES - part.shape[0], LANES), F32)], axis=0)
        dep_halo[4 * k : 4 * k + 4, :] = depth_rows(part, cfg["repeat"])
    for s in range(2, cfg["groups"]):
        pack(cfg, at_ref[0], s, outs[s - 2], col_own, dep_own, col_halo, dep_halo)


def near_kernel(
    cfg, at_ref, own_ref, tiled, wmid_ref, whead, spread, col_in, dep_in, col_halo, dep_halo,
    meta_in, out_own, out_mate, meta, col_own, dep_own,
):
    meta[...] = meta_in[...]
    col_own[...] = col_in[...]
    dep_own[...] = dep_in[...]
    nets = (tiled, wmid_ref, whead, spread)
    pieces = row_pieces(cfg, at_ref[0], True)
    field_chunks(cfg, own_ref, nets, col_own, dep_own, grouped(pieces, cfg["chunk"]))
    pack(cfg, at_ref[0], 0, out_own, col_own, dep_own, col_halo, dep_halo)
    pack(cfg, at_ref[0], 1, out_mate, col_own, dep_own, col_halo, dep_halo)


def decoder_kernel(cfg, info_ref, w0_ref, w1_ref, w2_ref, w3_ref, *rest):
    groups, nb = cfg["groups"], cfg["nb"]
    bufs = rest[:groups]
    out_ref = rest[groups]
    comp, x0, sa, xa, sc, xc, rep, rank_ref = rest[groups + 1 :]
    cols, rows_dev, pitch = cfg["cols"], cfg["rows_dev"], cfg["pitch"]
    n_own, n_halo, n_dep = cfg["n_own"], cfg["n_halo"], cfg["n_dep"]
    rows_in = rows_dev + 2 * EDGE
    rows_mid = rows_dev + 2
    mid = rows_mid * pitch
    half = LANES // 2
    per_dev = nb // groups
    place = info_ref[0]
    left_open, right_open = info_ref[1].astype(F32), info_ref[2].astype(F32)
    top_open, bottom_open = info_ref[3].astype(F32), info_ref[4].astype(F32)

    earlier = []
    for side in range(3):
        for k in range(nb):
            rank_ref[info_ref[8 + side * nb + k]] = k
        wide = 2 * per_dev * groups
        row = jnp.zeros((nb, wide), jnp.int32)
        column = jnp.zeros((nb, wide), jnp.int32)
        lane = lax.broadcasted_iota(jnp.int32, (nb, wide), 1)
        sub = lax.broadcasted_iota(jnp.int32, (nb, wide), 0)
        for s in range(groups):
            source = place ^ s
            for i in range(per_dev):
                rank = rank_ref[source * per_dev + i]
                at = s * 2 * per_dev + i
                row = jnp.where((lane == at) | (lane == at + per_dev), rank, row)
                column = jnp.where(sub == s * per_dev + i, rank, column)
        earlier.append(jnp.where(row < column, 1.0, 0.0).astype(BF16))

    at = n_own + n_halo
    own_rows = [bufs[s][at : at + n_dep, :].astype(F32) for s in range(groups)]
    halo_rows = [bufs[s][at + n_dep :, :].astype(F32) for s in range(groups)]
    chunks = n_own // LANES
    factors = []
    for k in range(chunks):
        stack = jnp.concatenate([own_rows[s][4 * k : 4 * k + 4] for s in range(groups)], axis=0)
        factors.append(jnp.exp(-dot(earlier[0], stack.astype(BF16))))
    lane = lax.broadcasted_iota(jnp.int32, (nb, LANES), 1)
    side_pitch = (cfg["rows_all"] + 2 * EDGE) * EDGE
    for k in range(cfg["hchunks"]):
        on_left = lane + k * LANES < side_pitch
        stack = jnp.concatenate(
            [halo_rows[s][4 * k : 4 * k + 4] for s in range(groups)], axis=0
        ).astype(BF16)
        from_left = jnp.exp(-dot(earlier[1], stack)) * left_open
        from_right = jnp.exp(-dot(earlier[2], stack)) * right_open
        factors.append(jnp.where(on_left, from_left, from_right))
    used = len(factors) * nb
    factors.append(jnp.zeros((LANES - used, LANES), F32))
    turned = jnp.concatenate(factors, axis=0).T
    high, low = split16(turned)
    high, low = high.astype(BF16), low.astype(BF16)

    def spread(k):
        r = lax.broadcasted_iota(jnp.int32, (LANES, groups * LANES), 0)
        c = lax.broadcasted_iota(jnp.int32, (LANES, groups * LANES), 1)
        pick = jnp.where(r - k * nb == c // half, 1.0, 0.0).astype(BF16)
        return dot(high, pick) + dot(low, pick)

    def mix(weights, lo, n):
        acc = None
        for s in range(groups):
            term = weights[:, s * LANES : (s + 1) * LANES] * bufs[s][lo : lo + n, :].astype(F32)
            acc = term if acc is None else acc + term
        return acc + pltpu.roll(acc, half, 1)

    comp[...] = jnp.zeros(comp.shape, F32)
    base = pitch
    per_chunk = LANES // cols
    for k in range(chunks):
        mixed = mix(spread(k), k * LANES, LANES)
        for t in range(per_chunk):
            q = base + (k * per_chunk + t) * pitch + LEAD
            comp[q : q + cols, :] = mixed[t * cols : (t + 1) * cols]
    for k in range(cfg["hchunks"]):
        rep[k * LANES : (k + 1) * LANES, :] = spread(chunks + k)
    size = n_halo // 2
    for i in range(2):
        start = pl.multiple_of(i * side_pitch + place * (rows_dev * EDGE), 8)
        mixed = mix(rep[pl.ds(start, size), :], n_own + i * size, size)
        for r in range(rows_in):
            q = base + r * pitch + LEAD + (cols if i else -EDGE)
            comp[q : q + EDGE, :] = mixed[r * EDGE : (r + 1) * EDGE]

    n_in = rows_in * pitch
    lane = lax.broadcasted_iota(jnp.int32, (n_in, LANES), 1)
    here = jnp.where(lane < half, comp[base - 1 : base - 1 + n_in, :], comp[base : base + n_in, :])
    x0[:, 0:LANES] = here.astype(BF16)
    x0[:, LANES : 2 * LANES] = comp[base + 1 : base + 1 + n_in, :].astype(BF16)

    q = lax.broadcasted_iota(jnp.int32, (mid, 2 * LANES), 0)
    pos = q
    for r in range(1, rows_mid):
        pos = pos - jnp.where(q >= r * pitch, pitch, 0)
    mask = jnp.where(pos < LEAD, left_open, jnp.where(pos >= LEAD + cols, right_open, 1.0))
    mask = mask * jnp.where(q < pitch, top_open, jnp.where(q >= mid - pitch, bottom_open, 1.0))

    def convolve(ref, pieces, n, weights):
        made = []
        for h in range(2):
            lhs = jnp.concatenate(
                [ref[r * pitch + h * n // 2 : r * pitch + (h + 1) * n // 2, a:b] for r, a, b in pieces],
                axis=1,
            )
            made.append(dot_t(lhs, weights))
        return jnp.concatenate(made, axis=0)

    wide = 2 * LANES
    value = convolve(x0, [(d, 0, wide) for d in range(3)], mid, w0_ref[...])
    value = jnp.maximum(value, 0.0) * mask

    sa[0:8, :] = jnp.zeros((8, wide), F32)
    sa[8 + mid :, :] = jnp.zeros((8, wide), F32)
    three = 3 * LANES
    xa[0:pitch, :] = jnp.zeros((pitch, 2 * three), BF16)
    xa[pitch + mid :, :] = jnp.zeros((pitch, 2 * three), BF16)

    def lay_out(value):
        sa[8 : 8 + mid, :] = value
        for pr in range(2):
            for d in range(3):
                c = pr * three + d * LANES
                xa[pitch : pitch + mid, c : c + LANES] = sa[
                    7 + d : 7 + d + mid, pr * LANES : (pr + 1) * LANES
                ].astype(BF16)

    lay_out(value)
    value = convolve(
        xa, [(0, three, 2 * three), (1, 0, 2 * three), (2, 0, three)], mid, w1_ref[...]
    )
    value = jnp.maximum(value, 0.0) * mask
    lay_out(value)
    for pr in range(2):
        for pc in range(2):
            where = [(0, 1), (1, 0), (1, 1)] if pr == 0 else [(1, 0), (1, 1), (2, 0)]
            at = [p * three + pc * LANES for _, p in where]
            value = convolve(
                xa, [(d, c, c + wide) for (d, _), c in zip(where, at)], mid, w2_ref[pc]
            )
            value = jnp.maximum(value, 0.0) * mask
            own = sc.at[2 * pr + pc]
            own[8 : 8 + mid, :] = value
            for rr in range(2):
                at = (2 * pr + rr) * 4 * LANES
                tile = value[:, rr * LANES : (rr + 1) * LANES]
                xc[:, at + (1 + pc) * LANES : at + (2 + pc) * LANES] = tile.astype(BF16)
                slot, move = (3, 9) if pc == 0 else (0, 7)
                xc[:, at + slot * LANES : at + (slot + 1) * LANES] = own[
                    move : move + mid, rr * LANES : (rr + 1) * LANES
                ].astype(BF16)
    n_out = rows_dev * pitch
    four = 4 * LANES
    final = convolve(
        xc, [(0, 3 * four, 4 * four), (1, 0, 4 * four), (2, 0, four)], n_out, w3_ref[...]
    )
    final = final + pltpu.roll(final, half, 1)
    rays = jnp.concatenate(
        [final[r * pitch + LEAD : r * pitch + LEAD + cols] for r in range(rows_dev)], axis=0
    )
    turned = rays.T
    stack = jnp.concatenate(
        [
            jnp.concatenate(
                [turned[16 * v : 16 * v + 16, r * cols : (r + 1) * cols] for v in range(4)], axis=1
            )
            for r in range(rows_dev)
        ],
        axis=0,
    )
    r = lax.broadcasted_iota(jnp.int32, (4 * cols, 4 * cols), 0)
    c = lax.broadcasted_iota(jnp.int32, (4 * cols, 4 * cols), 1)
    place_of = (c & 3) * cols + (c >> 2)
    pick = jnp.where(r == place_of, 1.0, 0.0).astype(BF16)
    high, low = split16(stack)
    image = dot(high.astype(BF16), pick) + dot(low.astype(BF16), pick)
    colours = out_ref.shape[0]
    for r in range(rows_dev):
        for u in range(4):
            for p in range(colours):
                at = r * 16 + u * 4 + p
                out_ref[p, 4 * r + u : 4 * r + u + 1, :] = image[at : at + 1, :]


def phase_taps(p, d):
    return [a for a in range(3) if (p + a - 1) // 2 + 1 == d]


def weights_kernel(conv_ref, colour_ref, after_ref, w0_ref, w1_ref, w2_ref, w3_ref):
    feat = conv_ref.shape[1]
    r = lax.broadcasted_iota(jnp.int32, (feat, LANES), 0)
    lane = lax.broadcasted_iota(jnp.int32, (feat, LANES), 1)
    twice = jnp.where((lane == r) | (lane == r + feat), 1.0, 0.0).astype(BF16)
    low = lane < feat
    zero = jnp.zeros((feat, LANES), F32)
    taps = [
        dot(conv_ref[k * 9 * feat : (k + 1) * 9 * feat, :], twice) for k in range(4)
    ]

    def tap(k, a, e):
        at = (a * 3 + e) * feat
        return taps[k][at : at + feat]

    def pair(left, right):
        if left is None and right is None:
            return zero
        if left is right:
            return left
        return jnp.where(low, zero if left is None else left, zero if right is None else right)

    def put(ref, n, j, tile):
        ref[n * feat : (n + 1) * feat, j * LANES : (j + 1) * LANES] = tile.astype(BF16)

    for k in (0, 2):
        sums = {}
        for p in range(2):
            for q in range(2):
                for d in range(3):
                    for f in range(3):
                        parts = [tap(k, a, e) for a in phase_taps(p, d) for e in phase_taps(q, f)]
                        sums[p, q, d, f] = functools.reduce(jnp.add, parts) if parts else None
        for p in range(2):
            for q in range(2):
                n = 2 * p + q
                for d in range(3):
                    row = [sums[p, q, d, f] for f in range(3)]
                    layouts = [[None] + row, row + [None]]
                    refs = [w2_ref.at[0], w2_ref.at[1]] if k == 2 else [None, w0_ref]
                    for ref, blocks in zip(refs, layouts):
                        if ref is not None:
                            put(ref, n, 2 * d, pair(blocks[0], blocks[1]))
                            put(ref, n, 2 * d + 1, pair(blocks[2], blocks[3]))

    def pick(table, a, e):
        return table(a, e) if 0 <= a < 3 and 0 <= e < 3 else None

    for p in range(2):
        for q in range(2):
            for row in range(4):
                for j in range(3):
                    blocks = [
                        pick(lambda a, e: tap(1, a, e), row - p, c - 1 - q)
                        for c in (2 * j, 2 * j + 1)
                    ]
                    put(w1_ref, 2 * p + q, row * 3 + j, pair(*blocks))

    colours = colour_ref.shape[0]
    given = colour_ref[...].astype(F32)
    sub = lax.broadcasted_iota(jnp.int32, (8, feat), 0)
    mixer = jnp.zeros((8, feat), F32)
    for p in range(colours):
        mixer = jnp.where((sub & 3) == p, given[p : p + 1], mixer)
    mixer = mixer.astype(BF16)
    mixed = {
        (a, e): dot(mixer, tap(3, a, e).astype(BF16)) for a in range(3) for e in range(3)
    }
    lane = lax.broadcasted_iota(jnp.int32, (8, LANES), 1) < feat
    upper = lax.broadcasted_iota(jnp.int32, (8, LANES), 0) < 4
    blank = jnp.zeros((8, LANES), F32)

    def choose(mask, x, y):
        if x is None and y is None:
            return None
        return jnp.where(mask, blank if x is None else x, blank if y is None else y)

    for row in range(6):
        for j in range(4):
            pieces = []
            for v in range(4):
                for u in (0, 2):
                    halves = [
                        choose(
                            lane,
                            pick(lambda a, e: mixed[a, e], row - w, 2 * j - 1 - v),
                            pick(lambda a, e: mixed[a, e], row - w, 2 * j - v),
                        )
                        for w in (u, u + 1)
                    ]
                    made = choose(upper, *halves)
                    pieces.append(blank if made is None else made)
            tile = jnp.concatenate(pieces, axis=0)
            high, low16 = split16(tile)
            at = (row * 4 + j) * LANES
            w3_ref[:, at : at + LANES] = jnp.concatenate([high, low16], axis=0).astype(BF16)


def body(samples_in, block_order, seam_link, w_in, w_mid, w_feat, w_density, w_conv, w_color):
    blk_dev, rows_all, cols, width = samples_in.shape
    groups, place = lax.axis_size("block"), lax.axis_index("block")
    patches, patch = lax.axis_size("patch"), lax.axis_index("patch")
    nb = block_order.shape[1]
    enc = w_in.shape[1]
    feat = w_feat.shape[2]
    rows_dev = rows_all // groups
    count = rows_all * cols
    hrays = (rows_all + 2 * EDGE) * 2 * EDGE
    hchunks = -(-hrays // LANES)
    n_own = (rows_dev + 2 * EDGE) * cols
    n_halo = (rows_dev + 2 * EDGE) * 2 * EDGE
    n_dep = 4 * n_own // LANES
    n_tail = 16
    samples = width // enc
    cfg = dict(
        groups=groups,
        nb=nb,
        samples=samples,
        enc=enc,
        repeat=LANES // (samples * blk_dev),
        cols=cols,
        rows_all=rows_all,
        rows_dev=rows_dev,
        n_near=2 * rows_dev - (EDGE if groups == 4 else 2 * EDGE),
        side_pitch=hrays // 2,
        pitch=cols + 16,
        chunk=2,
        n_own=n_own,
        n_halo=n_halo,
        n_dep=n_dep,
        hchunks=hchunks,
    )
    smem = pl.BlockSpec(memory_space=pltpu.SMEM)
    vmem = pl.BlockSpec(memory_space=pltpu.VMEM)
    hbm = pl.BlockSpec(memory_space=pltpu.HBM)
    params = pltpu.CompilerParams(vmem_limit_bytes=24 * 1024 * 1024)
    here = jnp.stack([place, patch & 1])

    def far_off(x):
        return pltpu.with_memory_space_constraint(x, pltpu.HBM)


    edges = blk_dev * rows_all * EDGE
    own, win, dens, near, far = pl.pallas_call(
        functools.partial(edges_kernel, cfg),
        out_shape=[
            pltpu.VMEM((blk_dev, count, width), BF16),
            pltpu.VMEM(w_in.shape, BF16),
            pltpu.VMEM(w_density.shape, BF16),
            pltpu.VMEM((edges + 16, width), BF16),
            pltpu.VMEM((edges + 16, width), BF16),
        ],
        in_specs=[smem] + [hbm] * 5,
        out_specs=[vmem] * 5,
        scratch_shapes=[
            pltpu.VMEM((edges, width), F32),
            pltpu.VMEM((edges, width), F32),
            pltpu.SMEM(block_order.shape, jnp.int32),
            pltpu.SMEM(seam_link.shape, jnp.int32),
            pltpu.SemaphoreType.DMA((5,)),
        ],
        compiler_params=params,
        name="edges",
    )(
        here,
        far_off(block_order),
        seam_link,
        far_off(samples_in.reshape(blk_dev, count, width)),
        far_off(w_in),
        far_off(w_density),
    )
    swap_near = [(i, i ^ 1) for i in range(patches) if i ^ 1 < patches]
    swap_far = []
    for i in range(1, patches - 1, 2):
        swap_far += [(i, i + 1), (i + 1, i)]
    far = lax.ppermute(far, "patch", swap_far)
    near = lax.ppermute(near, "patch", swap_near)

    rays_flops = 2 * 2 * blk_dev * samples * w_mid.shape[2] * (3 * w_mid.shape[2])
    far_rays = (rows_all - cfg["n_near"]) * cols
    col_own, dep_own, tiled, whead, spread, wmid = pl.pallas_call(
        functools.partial(field_kernel, cfg),
        out_shape=[
            pltpu.VMEM((count + 2 * EDGE * cols, LANES), BF16),
            pltpu.VMEM((8 * (count + 2 * EDGE * cols) // LANES, LANES), F32),
            pltpu.VMEM((blk_dev, width, w_in.shape[2]), BF16),
            pltpu.VMEM((blk_dev, samples, w_feat.shape[1], 2 * LANES), BF16),
            pltpu.VMEM((2 * LANES, samples * LANES), BF16),
            pltpu.VMEM(w_mid.shape, BF16),
        ],
        in_specs=[smem, vmem, vmem, hbm, vmem, vmem],
        out_specs=[vmem] * 6,
        scratch_shapes=[pltpu.SemaphoreType.DMA],
        compiler_params=params,
        cost_estimate=pl.CostEstimate(
            flops=far_rays * rays_flops, bytes_accessed=10**6, transcendentals=0
        ),
        name="field",
    )(here, own, win, far_off(w_mid), w_feat, dens)

    size = n_own + n_halo + n_dep + n_tail
    shape = pltpu.VMEM((size, LANES), BF16)
    *bufs, col_halo, dep_halo, meta = pl.pallas_call(
        functools.partial(halo_kernel, cfg),
        out_shape=[shape] * (groups - 2)
        + [
            pltpu.VMEM((hrays, LANES), F32),
            pltpu.VMEM((n_tail, LANES), F32),
            pltpu.VMEM((16, LANES), F32),
        ],
        in_specs=[smem] + [vmem] * 8,
        out_specs=[vmem] * (groups + 1),
        scratch_shapes=[pltpu.VMEM((blk_dev, hrays, width), F32)],
        compiler_params=params,
        name="halo",
    )(here, near, far, tiled, wmid, whead, spread, col_own, dep_own)
    got = []
    for s in range(2, groups):
        got.append(lax.ppermute(bufs[s - 2], "block", [(i, i ^ s) for i in range(groups)]))

    near_rows = pl.pallas_call(
        functools.partial(near_kernel, cfg),
        out_shape=[shape] * 2 + [pltpu.VMEM((16, LANES), F32)],
        in_specs=[smem] + [vmem] * 10,
        out_specs=[vmem] * 3,
        scratch_shapes=[
            pltpu.VMEM(col_own.shape, BF16),
            pltpu.VMEM(dep_own.shape, F32),
        ],
        compiler_params=params,
        cost_estimate=pl.CostEstimate(
            flops=cfg["n_near"] * cols * rays_flops, bytes_accessed=10**6, transcendentals=0
        ),
        name="near",
    )
    mine, mate, meta = near_rows(
        here, own, tiled, wmid, whead, spread, col_own, dep_own, col_halo, dep_halo, meta
    )
    got = [mine, lax.ppermute(mate, "block", [(i, i ^ 1) for i in range(groups)])] + got

    order_l = meta[0, : nb + 1].astype(jnp.int32)
    order_r = meta[8, : nb + 1].astype(jnp.int32)
    flags = jnp.stack(
        [
            place,
            order_l[nb] * (patch > 0),
            seam_link[0] * (patch < patches - 1),
            place > 0,
            place < groups - 1,
            place * 0,
            place * 0,
            place * 0,
        ]
    ).astype(jnp.int32)
    info = jnp.concatenate([flags, block_order[0], order_l[:nb], order_r[:nb]])

    w0, w1, w2, w3 = pl.pallas_call(
        weights_kernel,
        out_shape=[
            pltpu.VMEM((4 * feat, 12 * feat), BF16),
            pltpu.VMEM((4 * feat, 24 * feat), BF16),
            pltpu.VMEM((2, 4 * feat, 12 * feat), BF16),
            pltpu.VMEM((2 * feat, 48 * feat), BF16),
        ],
        in_specs=[vmem, vmem, pl.BlockSpec(memory_space=pl.ANY)],
        out_specs=[vmem] * 4,
        compiler_params=params,
        cost_estimate=pl.CostEstimate(flops=10**8, bytes_accessed=10**6, transcendentals=0),
        name="weights",
    )(w_conv.reshape(-1, feat), w_color, mine)
    pitch = cfg["pitch"]
    rows_in, rows_mid = rows_dev + 2 * EDGE, rows_dev + 2
    return pl.pallas_call(
        functools.partial(decoder_kernel, cfg),
        out_shape=jax.ShapeDtypeStruct((w_color.shape[0], 4 * rows_dev, 4 * cols), F32),
        in_specs=[smem] + [vmem] * (4 + groups),
        out_specs=vmem,
        scratch_shapes=[
            pltpu.VMEM(((rows_in + 2) * pitch, LANES), F32),
            pltpu.VMEM((rows_in * pitch, 2 * LANES), BF16),
            pltpu.VMEM((rows_mid * pitch + 16, 2 * LANES), F32),
            pltpu.VMEM(((rows_mid + 2) * pitch, 6 * LANES), BF16),
            pltpu.VMEM((4, rows_mid * pitch + 16, 2 * LANES), F32),
            pltpu.VMEM((rows_mid * pitch, 16 * LANES), BF16),
            pltpu.VMEM((hchunks * LANES, groups * LANES), F32),
            pltpu.SMEM((nb,), jnp.int32),
        ],
        compiler_params=params,
        name="decoder",
    )(info, w0, w1, w2, w3, *got)


def solution(mesh):
    return jax.shard_map(
        body,
        mesh=mesh,
        in_specs=(
            P("block", None, "patch", None),
            P("patch", None),
            P("patch"),
            P("block", None, None),
            P("block", None, None, None),
            P("block", None, None),
            P("block", None),
            P(),
            P(),
        ),
        out_specs=P(None, "block", "patch"),
        check_vma=False,
    )
```

```python
import functools

import jax
import jax.numpy as jnp
from jax import lax
from jax.experimental import pallas as pl
from jax.experimental.pallas import tpu as pltpu
from jax.sharding import PartitionSpec as P


STEP = 0.03
LANES = 128
EDGE = 2
LEAD = 8
F32 = jnp.float32
BF16 = jnp.bfloat16


def dot(a, b):
    return jnp.dot(a, b, preferred_element_type=F32)


def dot_t(a, b):
    return lax.dot_general(a, b, (((1,), (1,)), ((), ())), preferred_element_type=F32)


def relu16(x):
    return jnp.maximum(x.astype(BF16), jnp.zeros((), BF16))


def softplus(v):
    e = jnp.exp(-jnp.abs(v))
    tail = jnp.where(e < 1e-3, e * (1.0 - e * (0.5 - e * (1.0 / 3.0))), jnp.log(1.0 + e))
    return jnp.maximum(v, 0.0) + tail


def stopped(optical):
    small = optical * (1.0 - optical * (0.5 - optical * (1.0 / 6.0 - optical * (1.0 / 24.0))))
    return jnp.where(optical < 0.0625, small, 1.0 - jnp.exp(-optical))


def split16(x):
    high = x.astype(BF16).astype(F32)
    return high, x - high


def one_hot(shape, test):
    r = lax.broadcasted_iota(jnp.int32, shape, 0)
    c = lax.broadcasted_iota(jnp.int32, shape, 1)
    return jnp.where(test(r, c), 1.0, 0.0).astype(BF16)


def field_heads(xs, tiled, wmid, whead, spread, samples, enc):
    rays = xs[0].shape[0]
    lane = lax.broadcasted_iota(jnp.int32, xs[0].shape, 1)
    heads = [None] * samples
    for b, x in enumerate(xs):
        zero = jnp.zeros_like(x)
        parts = [
            jnp.where((lane >= s * enc) & (lane < (s + 1) * enc), x, zero) for s in range(samples)
        ]
        hidden = relu16(dot(jnp.concatenate(parts, axis=0), tiled[b]))
        hidden = relu16(dot(hidden, wmid[b, 0]))
        hidden = relu16(dot(hidden, wmid[b, 1]))
        for s in range(samples):
            made = dot(hidden[s * rays : (s + 1) * rays], whead[b, s])
            heads[s] = made if b == 0 else heads[s] + made
    return heads


def field_mix(heads, spread):
    samples, rays = len(heads), heads[0].shape[0]
    logit = heads[0][:, LANES:]
    for s in range(1, samples):
        logit = logit + heads[s][:, LANES:]
    optical = STEP * softplus(logit)
    group = LANES // samples
    lane = lax.broadcasted_iota(jnp.int32, (rays, LANES), 1)
    depth, before = optical, jnp.zeros((rays, LANES), F32)
    for s in range(1, samples):
        moved = pltpu.roll(optical, s * group, 1)
        depth = depth + moved
        before = before + jnp.where(lane >= s * group, moved, 0.0)
    weight = jnp.exp(-before) * stopped(optical)
    high, low = split16(weight)
    wide = dot(jnp.concatenate([high.astype(BF16), low.astype(BF16)], axis=1), spread[...])
    colour = None
    for s in range(samples):
        term = wide[:, s * LANES : (s + 1) * LANES] * heads[s][:, :LANES]
        colour = term if colour is None else colour + term
    return colour, depth


def depth_rows(depth, step):
    turned = depth.T
    pair = jnp.concatenate([turned[0:1], turned[step : step + 1]], axis=0)
    high, low = split16(pair)
    return jnp.concatenate([high, low], axis=0)


def edges_kernel(
    cfg, order_hbm, seam_hbm, own_hbm, *rest
):
    n = (len(rest) - 8) // 2
    sources, targets = rest[:n], rest[n + 1 : 2 * n + 1]
    own_ref = rest[n]
    meta_ref, near_ref, far_ref, left, right, order_ref, seam_ref, sems = rest[2 * n + 1 :]
    cols, rows_all = cfg["cols"], cfg["rows_all"]
    blocks = own_ref.shape[0]
    small = [
        pltpu.make_async_copy(order_hbm, order_ref, sems.at[n + 1]),
        pltpu.make_async_copy(seam_hbm, seam_ref, sems.at[n + 2]),
    ]
    for copy in small:
        copy.start()
    load = pltpu.make_async_copy(own_hbm, own_ref, sems.at[0])
    load.start()
    more = [
        pltpu.make_async_copy(source, target, sems.at[1 + i])
        for i, (source, target) in enumerate(zip(sources, targets))
    ]
    for copy in more:
        copy.start()
    nb = cfg["nb"]
    lane = lax.broadcasted_iota(jnp.int32, (16, LANES), 1)
    for copy in small:
        copy.wait()
    meta = jnp.where(lane == nb, seam_ref[0], 0)
    for k in range(nb):
        meta = jnp.where(lane == k, order_ref[0, k], meta)
    meta = meta.astype(F32).astype(BF16)
    load.wait()
    size = blocks * rows_all * EDGE
    for b in range(blocks):
        for r in range(rows_all):
            q = (b * rows_all + r) * EDGE
            left[q : q + EDGE, :] = own_ref[b, r * cols : r * cols + 16, :].astype(F32)[:EDGE]
            last = own_ref[b, (r + 1) * cols - 16 : (r + 1) * cols, :].astype(F32)
            right[q : q + EDGE, :] = last[16 - EDGE :]
    meta_ref[...] = meta
    odd = (lax.axis_index("patch") & 1) == 1
    near_ref[:size, :] = jnp.where(odd, left[...], right[...]).astype(BF16)
    far_ref[:size, :] = jnp.where(odd, right[...], left[...]).astype(BF16)
    near_ref[size:, :] = meta
    far_ref[size:, :] = meta
    for copy in more:
        copy.wait()


def field_chunks(cfg, own_ref, nets, col_own, dep_own, pieces):
    pad = EDGE * cfg["cols"]
    blocks = own_ref.shape[0]

    def start(chunk):
        xs = [
            jnp.concatenate([own_ref[b, pl.ds(at, LANES), :] for at in chunk], axis=0)
            for b in range(blocks)
        ]
        return field_heads(xs, *nets, cfg["samples"], cfg["enc"])

    def finish(chunk, heads):
        colour, depth = field_mix(heads, nets[3])
        for k, at in enumerate(chunk):
            rows = slice(k * LANES, (k + 1) * LANES)
            col_own[pl.ds(pl.multiple_of(at + pad, LANES), LANES), :] = colour[rows].astype(BF16)
            q = pl.multiple_of((at + pad) // LANES * 8, 8)
            dep_own[pl.ds(q, 4), :] = depth_rows(depth[rows], cfg["repeat"])

    waiting = None
    for chunk in pieces:
        heads = start(chunk)
        if waiting is not None:
            finish(*waiting)
        waiting = (chunk, heads)
    finish(*waiting)


def grouped(items, n):
    return [items[i : i + n] for i in range(0, len(items), n)]


def row_pieces(cfg, place, near):
    per = LANES // cfg["cols"]
    chip = place >> 1
    if cfg["groups"] == 4:
        first = jnp.where(chip == 0, 0, cfg["rows_all"] - cfg["n_near"])
    else:
        first = chip * (2 * cfg["rows_dev"]) + EDGE
    n = cfg["n_near"] if near else cfg["rows_all"] - cfg["n_near"]
    first = first if near else first + cfg["n_near"]
    starts = []
    for k in range(n // per):
        row = lax.rem(first + k * per, cfg["rows_all"])
        starts.append(pl.multiple_of(row * cfg["cols"], LANES))
    return starts


def field_kernel(
    cfg, own_ref, win_ref, wmid_ref, wf_ref, wd_ref, col_own, dep_own, tiled, whead, spread
):
    samples, enc = cfg["samples"], cfg["enc"]
    blocks = own_ref.shape[0]
    pad = EDGE * cfg["cols"]
    count = cfg["rows_all"] * cfg["cols"]
    col_own[0:pad, :] = jnp.zeros((pad, LANES), BF16)
    col_own[pad + count :, :] = jnp.zeros((pad, LANES), BF16)
    ends = 8 * pad // LANES
    dep_own[0:ends, :] = jnp.zeros((ends, LANES), F32)
    dep_own[dep_own.shape[0] - ends :, :] = jnp.zeros((ends, LANES), F32)
    for b in range(blocks):
        for s in range(samples):
            tiled[b, s * enc : (s + 1) * enc, :] = win_ref[b]
    feat, width = wf_ref.shape[2], wf_ref.shape[1]
    repeat = cfg["repeat"]
    dens = wd_ref[...].astype(F32)
    group = lax.broadcasted_iota(jnp.int32, (width, LANES), 1) // repeat
    for b in range(blocks):
        lift = one_hot((feat, LANES), lambda r, c: c - b * feat == r)
        r = lax.broadcasted_iota(jnp.int32, (width, width), 0)
        c = lax.broadcasted_iota(jnp.int32, (width, width), 1)
        diag = jnp.where(r == c, dens[b : b + 1], 0.0).astype(BF16)
        features = dot(wf_ref[b], lift).astype(BF16)
        column = dot(diag, jnp.ones((width, LANES), BF16))
        for s in range(samples):
            whead[b, s, :, :LANES] = features
            whead[b, s, :, LANES:] = jnp.where(group == s * blocks + b, column, 0.0).astype(BF16)
    spread[...] = one_hot(
        spread.shape, lambda r, c: (r & (LANES - 1)) == c // (LANES // blocks) * repeat
    )
    nets = (tiled, wmid_ref, whead, spread)
    pieces = row_pieces(cfg, lax.axis_index("block"), False)
    field_chunks(cfg, own_ref, nets, col_own, dep_own, grouped(pieces, cfg["chunk"]))


def pack(cfg, place, s, out, col_own, dep_own, col_halo, dep_halo):
    n_own, n_halo, n_dep = cfg["n_own"], cfg["n_halo"], cfg["n_dep"]
    cols, rows_dev = cfg["cols"], cfg["rows_dev"]
    half = n_halo // 2
    dest = place ^ s
    start = pl.multiple_of(dest * (rows_dev * cols), LANES)
    out[0:n_own, :] = col_own[pl.ds(start, n_own), :]
    for i in range(2):
        start = pl.multiple_of(i * cfg["side_pitch"] + dest * (rows_dev * EDGE), 8)
        q = n_own + i * half
        out[q : q + half, :] = col_halo[pl.ds(start, half), :].astype(BF16)
    start = pl.multiple_of(dest * (8 * rows_dev * cols // LANES), 8)
    at = n_own + n_halo
    groups = n_dep // 4
    rows = dep_own[pl.ds(start, 8 * groups), :]
    rows = jnp.concatenate([rows[8 * k : 8 * k + 4] for k in range(groups)], axis=0)
    out[at : at + n_dep, :] = rows.astype(BF16)
    out[at + n_dep :, :] = dep_halo[...].astype(BF16)


def halo_kernel(
    cfg, near_ref, far_ref, tiled, wmid_ref, whead, spread, col_own, dep_own, *rest
):
    outs = rest[: cfg["groups"] - 2]
    col_halo, dep_halo, meta, halo_ref = rest[cfg["groups"] - 2 :]
    samples, enc, rows_all = cfg["samples"], cfg["enc"], cfg["rows_all"]
    blocks = halo_ref.shape[0]
    odd = (lax.axis_index("patch") & 1) == 1
    near, far = near_ref[...].astype(F32), far_ref[...].astype(F32)
    sides = [jnp.where(odd, near, far), jnp.where(odd, far, near)]
    side_rays = rows_all * EDGE
    halo_ref[...] = jnp.zeros(halo_ref.shape, F32)
    for b in range(blocks):
        for i, side in enumerate(sides):
            q = i * cfg["side_pitch"] + EDGE * EDGE
            halo_ref[b, q : q + side_rays, :] = side[b * side_rays : (b + 1) * side_rays]
    for i, side in enumerate(sides):
        meta[8 * i : 8 * i + 8, :] = side[blocks * side_rays : blocks * side_rays + 8]
    xs = [halo_ref[b].astype(BF16) for b in range(blocks)]
    heads = field_heads(xs, tiled, wmid_ref, whead, spread, samples, enc)
    colour, depth = field_mix(heads, spread)
    col_halo[...] = colour
    dep_halo[...] = jnp.zeros(dep_halo.shape, F32)
    hrays = depth.shape[0]
    for k in range(cfg["hchunks"]):
        part = depth[k * LANES : min((k + 1) * LANES, hrays)]
        if part.shape[0] < LANES:
            part = jnp.concatenate([part, jnp.zeros((LANES - part.shape[0], LANES), F32)], axis=0)
        dep_halo[4 * k : 4 * k + 4, :] = depth_rows(part, cfg["repeat"])
    for s in range(2, cfg["groups"]):
        pack(cfg, lax.axis_index("block"), s, outs[s - 2], col_own, dep_own, col_halo, dep_halo)


def earlier_blocks(cfg, place, order, rows):
    groups, nb = cfg["groups"], cfg["nb"]
    per = nb // groups
    sub = lax.broadcasted_iota(jnp.int32, (rows, LANES), 0)
    lane = lax.broadcasted_iota(jnp.int32, (rows, LANES), 1)
    hit = (jnp.broadcast_to(order, (rows, LANES)) == sub.astype(F32)) & (lane < nb)
    rank = jnp.sum(jnp.where(hit, lane.astype(F32), 0.0), axis=1, keepdims=True)
    rank = jnp.broadcast_to(rank, (rows, LANES))
    block = ((lane // (2 * per)) ^ place) * per + lane % per
    other = jnp.sum(jnp.where(sub == block, rank, 0.0), axis=0, keepdims=True)
    return jnp.where(other < rank, 1.0, 0.0)


def near_kernel(
    cfg, own_ref, tiled, wmid_ref, whead, spread, col_in, dep_in, col_halo, dep_halo,
    meta_sides, meta_own, out_own, out_mate, earlier, flags, col_own, dep_own,
):
    nb, patch = cfg["nb"], lax.axis_index("patch")
    mine = meta_own[...].astype(F32)[0:1]
    sides = [mine, meta_sides[0:1, :], meta_sides[8:9, :]]
    rows = earlier.shape[0] // 3
    for i, order in enumerate(sides):
        made = earlier_blocks(cfg, lax.axis_index("block"), order, rows)
        earlier[i * rows : (i + 1) * rows, :] = made.astype(BF16)
    lane = lax.broadcasted_iota(jnp.int32, (1, LANES), 1)
    for i, (order, there) in enumerate([(sides[1], patch > 0), (mine, patch < cfg["patches"] - 1)]):
        seam = jnp.sum(jnp.where(lane == nb, order, 0.0), axis=1, keepdims=True)
        seam = jnp.where(there, seam, 0.0)
        flags[8 * i : 8 * i + 8, :] = jnp.broadcast_to(seam, (8, LANES))
    col_own[...] = col_in[...]
    dep_own[...] = dep_in[...]
    nets = (tiled, wmid_ref, whead, spread)
    pieces = row_pieces(cfg, lax.axis_index("block"), True)
    field_chunks(cfg, own_ref, nets, col_own, dep_own, grouped(pieces, cfg["chunk"]))
    pack(cfg, lax.axis_index("block"), 0, out_own, col_own, dep_own, col_halo, dep_halo)
    pack(cfg, lax.axis_index("block"), 1, out_mate, col_own, dep_own, col_halo, dep_halo)


def decoder_kernel(cfg, earlier_ref, flags_ref, w0_ref, w1_ref, w2_ref, w3_ref, *rest):
    groups, nb = cfg["groups"], cfg["nb"]
    bufs = rest[:groups]
    out_ref = rest[groups]
    comp, x0, sa, xa, sc, xc, rep = rest[groups + 1 :]
    cols, rows_dev, pitch = cfg["cols"], cfg["rows_dev"], cfg["pitch"]
    n_own, n_halo, n_dep = cfg["n_own"], cfg["n_halo"], cfg["n_dep"]
    rows_in = rows_dev + 2 * EDGE
    rows_mid = rows_dev + 2
    mid = rows_mid * pitch
    half = LANES // 2
    per_dev = nb // groups
    place = lax.axis_index("block")
    left_open, right_open = flags_ref[0:1, :], flags_ref[8:9, :]
    top_open = jnp.where(place > 0, 1.0, 0.0)
    bottom_open = jnp.where(place < groups - 1, 1.0, 0.0)

    sides = earlier_ref.shape[0] // 3
    stacked = 2 * per_dev * groups
    earlier = [earlier_ref[i * sides : i * sides + nb, :stacked] for i in range(3)]

    at = n_own + n_halo
    own_rows = [bufs[s][at : at + n_dep, :].astype(F32) for s in range(groups)]
    halo_rows = [bufs[s][at + n_dep :, :].astype(F32) for s in range(groups)]
    chunks = n_own // LANES
    factors = []
    for k in range(chunks):
        stack = jnp.concatenate([own_rows[s][4 * k : 4 * k + 4] for s in range(groups)], axis=0)
        factors.append(jnp.exp(-dot(earlier[0], stack.astype(BF16))))
    lane = lax.broadcasted_iota(jnp.int32, (nb, LANES), 1)
    side_pitch = (cfg["rows_all"] + 2 * EDGE) * EDGE
    for k in range(cfg["hchunks"]):
        on_left = lane + k * LANES < side_pitch
        stack = jnp.concatenate(
            [halo_rows[s][4 * k : 4 * k + 4] for s in range(groups)], axis=0
        ).astype(BF16)
        from_left = jnp.exp(-dot(earlier[1], stack)) * left_open
        from_right = jnp.exp(-dot(earlier[2], stack)) * right_open
        factors.append(jnp.where(on_left, from_left, from_right))
    used = len(factors) * nb
    factors.append(jnp.zeros((LANES - used, LANES), F32))
    turned = jnp.concatenate(factors, axis=0).T
    high, low = split16(turned)
    high, low = high.astype(BF16), low.astype(BF16)

    def spread(k):
        r = lax.broadcasted_iota(jnp.int32, (LANES, groups * LANES), 0)
        c = lax.broadcasted_iota(jnp.int32, (LANES, groups * LANES), 1)
        block = ((c // LANES) ^ place) * per_dev + (c & (LANES - 1)) // half
        pick = jnp.where(r - k * nb == block, 1.0, 0.0).astype(BF16)
        return dot(high, pick) + dot(low, pick)

    def mix(weights, lo, n):
        acc = None
        for s in range(groups):
            term = weights[:, s * LANES : (s + 1) * LANES] * bufs[s][lo : lo + n, :].astype(F32)
            acc = term if acc is None else acc + term
        return acc + pltpu.roll(acc, half, 1)

    comp[...] = jnp.zeros(comp.shape, F32)
    base = pitch
    per_chunk = LANES // cols
    for k in range(chunks):
        mixed = mix(spread(k), k * LANES, LANES)
        for t in range(per_chunk):
            q = base + (k * per_chunk + t) * pitch + LEAD
            comp[q : q + cols, :] = mixed[t * cols : (t + 1) * cols]
    for k in range(cfg["hchunks"]):
        rep[k * LANES : (k + 1) * LANES, :] = spread(chunks + k)
    size = n_halo // 2
    for i in range(2):
        start = pl.multiple_of(i * side_pitch + place * (rows_dev * EDGE), 8)
        mixed = mix(rep[pl.ds(start, size), :], n_own + i * size, size)
        for r in range(rows_in):
            q = base + r * pitch + LEAD + (cols if i else -EDGE)
            comp[q : q + EDGE, :] = mixed[r * EDGE : (r + 1) * EDGE]

    n_in = rows_in * pitch
    lane = lax.broadcasted_iota(jnp.int32, (n_in, LANES), 1)
    here = jnp.where(lane < half, comp[base - 1 : base - 1 + n_in, :], comp[base : base + n_in, :])
    x0[:, 0:LANES] = here.astype(BF16)
    x0[:, LANES : 2 * LANES] = comp[base + 1 : base + 1 + n_in, :].astype(BF16)

    q = lax.broadcasted_iota(jnp.int32, (mid, 2 * LANES), 0)
    pos = q
    for r in range(1, rows_mid):
        pos = pos - jnp.where(q >= r * pitch, pitch, 0)
    left_open = jnp.concatenate([left_open, left_open], axis=1)
    right_open = jnp.concatenate([right_open, right_open], axis=1)
    mask = jnp.where(pos < LEAD, left_open, jnp.where(pos >= LEAD + cols, right_open, 1.0))
    mask = mask * jnp.where(q < pitch, top_open, jnp.where(q >= mid - pitch, bottom_open, 1.0))

    def convolve(ref, pieces, n, weights):
        made = []
        for h in range(2):
            lhs = jnp.concatenate(
                [ref[r * pitch + h * n // 2 : r * pitch + (h + 1) * n // 2, a:b] for r, a, b in pieces],
                axis=1,
            )
            made.append(dot_t(lhs, weights))
        return jnp.concatenate(made, axis=0)

    wide = 2 * LANES
    value = convolve(x0, [(d, 0, wide) for d in range(3)], mid, w0_ref[...])
    value = jnp.maximum(value, 0.0) * mask

    sa[0:8, :] = jnp.zeros((8, wide), F32)
    sa[8 + mid :, :] = jnp.zeros((8, wide), F32)
    three = 3 * LANES
    xa[0:pitch, :] = jnp.zeros((pitch, 2 * three), BF16)
    xa[pitch + mid :, :] = jnp.zeros((pitch, 2 * three), BF16)

    def lay_out(value):
        sa[8 : 8 + mid, :] = value
        for pr in range(2):
            for d in range(3):
                c = pr * three + d * LANES
                xa[pitch : pitch + mid, c : c + LANES] = sa[
                    7 + d : 7 + d + mid, pr * LANES : (pr + 1) * LANES
                ].astype(BF16)

    lay_out(value)
    value = convolve(
        xa, [(0, three, 2 * three), (1, 0, 2 * three), (2, 0, three)], mid, w1_ref[...]
    )
    value = jnp.maximum(value, 0.0) * mask
    lay_out(value)
    for pr in range(2):
        for pc in range(2):
            where = [(0, 1), (1, 0), (1, 1)] if pr == 0 else [(1, 0), (1, 1), (2, 0)]
            at = [p * three + pc * LANES for _, p in where]
            value = convolve(
                xa, [(d, c, c + wide) for (d, _), c in zip(where, at)], mid, w2_ref[pc]
            )
            value = jnp.maximum(value, 0.0) * mask
            own = sc.at[2 * pr + pc]
            own[8 : 8 + mid, :] = value
            for rr in range(2):
                at = (2 * pr + rr) * 4 * LANES
                tile = value[:, rr * LANES : (rr + 1) * LANES]
                xc[:, at + (1 + pc) * LANES : at + (2 + pc) * LANES] = tile.astype(BF16)
                slot, move = (3, 9) if pc == 0 else (0, 7)
                xc[:, at + slot * LANES : at + (slot + 1) * LANES] = own[
                    move : move + mid, rr * LANES : (rr + 1) * LANES
                ].astype(BF16)
    n_out = rows_dev * pitch
    four = 4 * LANES
    final = convolve(
        xc, [(0, 3 * four, 4 * four), (1, 0, 4 * four), (2, 0, four)], n_out, w3_ref[...]
    )
    final = final + pltpu.roll(final, half, 1)
    rays = jnp.concatenate(
        [final[r * pitch + LEAD : r * pitch + LEAD + cols] for r in range(rows_dev)], axis=0
    )
    turned = rays.T
    stack = jnp.concatenate(
        [
            jnp.concatenate(
                [turned[16 * v : 16 * v + 16, r * cols : (r + 1) * cols] for v in range(4)], axis=1
            )
            for r in range(rows_dev)
        ],
        axis=0,
    )
    r = lax.broadcasted_iota(jnp.int32, (4 * cols, 4 * cols), 0)
    c = lax.broadcasted_iota(jnp.int32, (4 * cols, 4 * cols), 1)
    place_of = (c & 3) * cols + (c >> 2)
    pick = jnp.where(r == place_of, 1.0, 0.0).astype(BF16)
    high, low = split16(stack)
    image = dot(high.astype(BF16), pick) + dot(low.astype(BF16), pick)
    colours = out_ref.shape[0]
    for r in range(rows_dev):
        for u in range(4):
            for p in range(colours):
                at = r * 16 + u * 4 + p
                out_ref[p, 4 * r + u : 4 * r + u + 1, :] = image[at : at + 1, :]


def phase_taps(p, d):
    return [a for a in range(3) if (p + a - 1) // 2 + 1 == d]


def weights_kernel(conv_ref, colour_ref, after_ref, w0_ref, w1_ref, w2_ref, w3_ref):
    feat = conv_ref.shape[1]
    r = lax.broadcasted_iota(jnp.int32, (feat, LANES), 0)
    lane = lax.broadcasted_iota(jnp.int32, (feat, LANES), 1)
    twice = jnp.where((lane == r) | (lane == r + feat), 1.0, 0.0).astype(BF16)
    low = lane < feat
    zero = jnp.zeros((feat, LANES), F32)
    taps = [
        dot(conv_ref[k * 9 * feat : (k + 1) * 9 * feat, :], twice) for k in range(4)
    ]

    def tap(k, a, e):
        at = (a * 3 + e) * feat
        return taps[k][at : at + feat]

    def pair(left, right):
        if left is None and right is None:
            return zero
        if left is right:
            return left
        return jnp.where(low, zero if left is None else left, zero if right is None else right)

    def put(ref, n, j, tile):
        ref[n * feat : (n + 1) * feat, j * LANES : (j + 1) * LANES] = tile.astype(BF16)

    for k in (0, 2):
        sums = {}
        for p in range(2):
            for q in range(2):
                for d in range(3):
                    for f in range(3):
                        parts = [tap(k, a, e) for a in phase_taps(p, d) for e in phase_taps(q, f)]
                        sums[p, q, d, f] = functools.reduce(jnp.add, parts) if parts else None
        for p in range(2):
            for q in range(2):
                n = 2 * p + q
                for d in range(3):
                    row = [sums[p, q, d, f] for f in range(3)]
                    layouts = [[None] + row, row + [None]]
                    refs = [w2_ref.at[0], w2_ref.at[1]] if k == 2 else [None, w0_ref]
                    for ref, blocks in zip(refs, layouts):
                        if ref is not None:
                            put(ref, n, 2 * d, pair(blocks[0], blocks[1]))
                            put(ref, n, 2 * d + 1, pair(blocks[2], blocks[3]))

    def pick(table, a, e):
        return table(a, e) if 0 <= a < 3 and 0 <= e < 3 else None

    for p in range(2):
        for q in range(2):
            for row in range(4):
                for j in range(3):
                    blocks = [
                        pick(lambda a, e: tap(1, a, e), row - p, c - 1 - q)
                        for c in (2 * j, 2 * j + 1)
                    ]
                    put(w1_ref, 2 * p + q, row * 3 + j, pair(*blocks))

    colours = colour_ref.shape[0]
    given = colour_ref[...].astype(F32)
    sub = lax.broadcasted_iota(jnp.int32, (8, feat), 0)
    mixer = jnp.zeros((8, feat), F32)
    for p in range(colours):
        mixer = jnp.where((sub & 3) == p, given[p : p + 1], mixer)
    mixer = mixer.astype(BF16)
    mixed = {
        (a, e): dot(mixer, tap(3, a, e).astype(BF16)) for a in range(3) for e in range(3)
    }
    lane = lax.broadcasted_iota(jnp.int32, (8, LANES), 1) < feat
    upper = lax.broadcasted_iota(jnp.int32, (8, LANES), 0) < 4
    blank = jnp.zeros((8, LANES), F32)

    def choose(mask, x, y):
        if x is None and y is None:
            return None
        return jnp.where(mask, blank if x is None else x, blank if y is None else y)

    for row in range(6):
        for j in range(4):
            pieces = []
            for v in range(4):
                for u in (0, 2):
                    halves = [
                        choose(
                            lane,
                            pick(lambda a, e: mixed[a, e], row - w, 2 * j - 1 - v),
                            pick(lambda a, e: mixed[a, e], row - w, 2 * j - v),
                        )
                        for w in (u, u + 1)
                    ]
                    made = choose(upper, *halves)
                    pieces.append(blank if made is None else made)
            tile = jnp.concatenate(pieces, axis=0)
            high, low16 = split16(tile)
            at = (row * 4 + j) * LANES
            w3_ref[:, at : at + LANES] = jnp.concatenate([high, low16], axis=0).astype(BF16)


def body(samples_in, block_order, seam_link, w_in, w_mid, w_feat, w_density, w_conv, w_color):
    blk_dev, rows_all, cols, width = samples_in.shape
    groups, patches = lax.axis_size("block"), lax.axis_size("patch")
    nb = block_order.shape[1]
    enc = w_in.shape[1]
    feat = w_feat.shape[2]
    rows_dev = rows_all // groups
    count = rows_all * cols
    hrays = (rows_all + 2 * EDGE) * 2 * EDGE
    hchunks = -(-hrays // LANES)
    n_own = (rows_dev + 2 * EDGE) * cols
    n_halo = (rows_dev + 2 * EDGE) * 2 * EDGE
    n_dep = 4 * n_own // LANES
    n_tail = 16
    samples = width // enc
    cfg = dict(
        groups=groups,
        nb=nb,
        patches=patches,
        samples=samples,
        enc=enc,
        repeat=LANES // (samples * blk_dev),
        cols=cols,
        rows_all=rows_all,
        rows_dev=rows_dev,
        n_near=2 * rows_dev - (EDGE if groups == 4 else 2 * EDGE),
        side_pitch=hrays // 2,
        pitch=cols + 16,
        chunk=2,
        n_own=n_own,
        n_halo=n_halo,
        n_dep=n_dep,
        hchunks=hchunks,
    )
    vmem = pl.BlockSpec(memory_space=pltpu.VMEM)
    hbm = pl.BlockSpec(memory_space=pltpu.HBM)
    params = pltpu.CompilerParams(vmem_limit_bytes=16 * 1024 * 1024)

    def far_off(x):
        return pltpu.with_memory_space_constraint(x, pltpu.HBM)


    edges = blk_dev * rows_all * EDGE
    early = [w_in, w_mid, w_density, w_color]
    own, win, wmid, dens, colour, meta_own, near, far = pl.pallas_call(
        functools.partial(edges_kernel, cfg),
        out_shape=[pltpu.VMEM((blk_dev, count, width), BF16)]
        + [pltpu.VMEM(x.shape, BF16) for x in early]
        + [
            pltpu.VMEM((16, width), BF16),
            pltpu.VMEM((edges + 16, width), BF16),
            pltpu.VMEM((edges + 16, width), BF16),
        ],
        in_specs=[hbm] * (3 + len(early)),
        out_specs=[vmem] * (4 + len(early)),
        scratch_shapes=[
            pltpu.VMEM((edges, width), F32),
            pltpu.VMEM((edges, width), F32),
            pltpu.SMEM(block_order.shape, jnp.int32),
            pltpu.SMEM(seam_link.shape, jnp.int32),
            pltpu.SemaphoreType.DMA((3 + len(early),)),
        ],
        compiler_params=params,
        name="edges",
    )(
        far_off(block_order),
        seam_link,
        far_off(samples_in.reshape(blk_dev, count, width)),
        *[far_off(x) for x in early],
    )
    swap_near = [(i, i ^ 1) for i in range(patches) if i ^ 1 < patches]
    swap_far = []
    for i in range(1, patches - 1, 2):
        swap_far += [(i, i + 1), (i + 1, i)]
    far = lax.ppermute(far, "patch", swap_far)
    near = lax.ppermute(near, "patch", swap_near)

    rays_flops = 2 * 2 * blk_dev * samples * w_mid.shape[2] * (3 * w_mid.shape[2])
    far_rays = (rows_all - cfg["n_near"]) * cols
    col_own, dep_own, tiled, whead, spread = pl.pallas_call(
        functools.partial(field_kernel, cfg),
        out_shape=[
            pltpu.VMEM((count + 2 * EDGE * cols, LANES), BF16),
            pltpu.VMEM((8 * (count + 2 * EDGE * cols) // LANES, LANES), F32),
            pltpu.VMEM((blk_dev, width, w_in.shape[2]), BF16),
            pltpu.VMEM((blk_dev, samples, w_feat.shape[1], 2 * LANES), BF16),
            pltpu.VMEM((2 * LANES, samples * LANES), BF16),
        ],
        in_specs=[vmem] * 5,
        out_specs=[vmem] * 5,
        compiler_params=params,
        cost_estimate=pl.CostEstimate(
            flops=far_rays * rays_flops, bytes_accessed=10**6, transcendentals=0
        ),
        name="field",
    )(own, win, wmid, w_feat, dens)

    size = n_own + n_halo + n_dep + n_tail
    shape = pltpu.VMEM((size, LANES), BF16)
    *bufs, col_halo, dep_halo, meta = pl.pallas_call(
        functools.partial(halo_kernel, cfg),
        out_shape=[shape] * (groups - 2)
        + [
            pltpu.VMEM((hrays, LANES), F32),
            pltpu.VMEM((n_tail, LANES), F32),
            pltpu.VMEM((16, LANES), F32),
        ],
        in_specs=[vmem] * 8,
        out_specs=[vmem] * (groups + 1),
        scratch_shapes=[pltpu.VMEM((blk_dev, hrays, width), F32)],
        compiler_params=params,
        name="halo",
    )(near, far, tiled, wmid, whead, spread, col_own, dep_own)
    got = []
    for s in range(2, groups):
        got.append(lax.ppermute(bufs[s - 2], "block", [(i, i ^ s) for i in range(groups)]))

    near_rows = pl.pallas_call(
        functools.partial(near_kernel, cfg),
        out_shape=[shape] * 2
        + [pltpu.VMEM((48, LANES), BF16), pltpu.VMEM((16, LANES), F32)],
        in_specs=[vmem] * 11,
        out_specs=[vmem] * 4,
        scratch_shapes=[
            pltpu.VMEM(col_own.shape, BF16),
            pltpu.VMEM(dep_own.shape, F32),
        ],
        compiler_params=params,
        cost_estimate=pl.CostEstimate(
            flops=cfg["n_near"] * cols * rays_flops, bytes_accessed=10**6, transcendentals=0
        ),
        name="near",
    )
    mine, mate, earlier, flags = near_rows(
        own, tiled, wmid, whead, spread, col_own, dep_own, col_halo, dep_halo, meta, meta_own
    )
    got = [mine, lax.ppermute(mate, "block", [(i, i ^ 1) for i in range(groups)])] + got

    w0, w1, w2, w3 = pl.pallas_call(
        weights_kernel,
        out_shape=[
            pltpu.VMEM((4 * feat, 12 * feat), BF16),
            pltpu.VMEM((4 * feat, 24 * feat), BF16),
            pltpu.VMEM((2, 4 * feat, 12 * feat), BF16),
            pltpu.VMEM((2 * feat, 48 * feat), BF16),
        ],
        in_specs=[vmem, vmem, pl.BlockSpec(memory_space=pl.ANY)],
        out_specs=[vmem] * 4,
        compiler_params=params,
        cost_estimate=pl.CostEstimate(flops=10**8, bytes_accessed=10**6, transcendentals=0),
        name="weights",
    )(w_conv.reshape(-1, feat), colour, mine)
    pitch = cfg["pitch"]
    rows_in, rows_mid = rows_dev + 2 * EDGE, rows_dev + 2
    return pl.pallas_call(
        functools.partial(decoder_kernel, cfg),
        out_shape=jax.ShapeDtypeStruct((w_color.shape[0], 4 * rows_dev, 4 * cols), F32),
        in_specs=[vmem] * (6 + groups),
        out_specs=vmem,
        scratch_shapes=[
            pltpu.VMEM(((rows_in + 2) * pitch, LANES), F32),
            pltpu.VMEM((rows_in * pitch, 2 * LANES), BF16),
            pltpu.VMEM((rows_mid * pitch + 16, 2 * LANES), F32),
            pltpu.VMEM(((rows_mid + 2) * pitch, 6 * LANES), BF16),
            pltpu.VMEM((4, rows_mid * pitch + 16, 2 * LANES), F32),
            pltpu.VMEM((rows_mid * pitch, 16 * LANES), BF16),
            pltpu.VMEM((hchunks * LANES, groups * LANES), F32),
        ],
        compiler_params=params,
        name="decoder",
    )(earlier, flags, w0, w1, w2, w3, *got)


def solution(mesh):
    return jax.shard_map(
        body,
        mesh=mesh,
        in_specs=(
            P("block", None, "patch", None),
            P("patch", None),
            P("patch"),
            P("block", None, None),
            P("block", None, None, None),
            P("block", None, None),
            P("block", None),
            P(),
            P(),
        ),
        out_specs=P(None, "block", "patch"),
        check_vma=False,
    )
```

```python
import functools

import jax
import jax.numpy as jnp
from jax import lax
from jax.experimental import pallas as pl
from jax.experimental.pallas import tpu as pltpu
from jax.sharding import PartitionSpec as P


STEP = 0.03
LANES = 128
EDGE = 2
LEAD = 8
F32 = jnp.float32
BF16 = jnp.bfloat16


def dot(a, b):
    return jnp.dot(a, b, preferred_element_type=F32)


def dot_t(a, b):
    return lax.dot_general(a, b, (((1,), (1,)), ((), ())), preferred_element_type=F32)


def relu16(x):
    return jnp.maximum(x.astype(BF16), jnp.zeros((), BF16))


def softplus(v):
    e = jnp.exp(-jnp.abs(v))
    tail = jnp.where(e < 1e-3, e * (1.0 - e * (0.5 - e * (1.0 / 3.0))), jnp.log(1.0 + e))
    return jnp.maximum(v, 0.0) + tail


def stopped(optical):
    small = optical * (1.0 - optical * (0.5 - optical * (1.0 / 6.0 - optical * (1.0 / 24.0))))
    return jnp.where(optical < 0.0625, small, 1.0 - jnp.exp(-optical))


def split16(x):
    high = x.astype(BF16).astype(F32)
    return high, x - high


def one_hot(shape, test):
    r = lax.broadcasted_iota(jnp.int32, shape, 0)
    c = lax.broadcasted_iota(jnp.int32, shape, 1)
    return jnp.where(test(r, c), 1.0, 0.0).astype(BF16)


def field_heads(xs, tiled, wmid, whead, spread, samples, enc):
    rays = xs[0].shape[0]
    lane = lax.broadcasted_iota(jnp.int32, xs[0].shape, 1)
    heads = [None] * samples
    for b, x in enumerate(xs):
        zero = jnp.zeros_like(x)
        parts = [
            jnp.where((lane >= s * enc) & (lane < (s + 1) * enc), x, zero) for s in range(samples)
        ]
        hidden = relu16(dot(jnp.concatenate(parts, axis=0), tiled[b]))
        hidden = relu16(dot(hidden, wmid[b, 0]))
        hidden = relu16(dot(hidden, wmid[b, 1]))
        for s in range(samples):
            made = dot(hidden[s * rays : (s + 1) * rays], whead[b, s])
            heads[s] = made if b == 0 else heads[s] + made
    return heads


def field_mix(heads, spread):
    samples, rays = len(heads), heads[0].shape[0]
    logit = heads[0][:, LANES:]
    for s in range(1, samples):
        logit = logit + heads[s][:, LANES:]
    optical = STEP * softplus(logit)
    group = LANES // samples
    lane = lax.broadcasted_iota(jnp.int32, (rays, LANES), 1)
    depth, before = optical, jnp.zeros((rays, LANES), F32)
    for s in range(1, samples):
        moved = pltpu.roll(optical, s * group, 1)
        depth = depth + moved
        before = before + jnp.where(lane >= s * group, moved, 0.0)
    weight = jnp.exp(-before) * stopped(optical)
    high, low = split16(weight)
    wide = dot(jnp.concatenate([high.astype(BF16), low.astype(BF16)], axis=1), spread[...])
    colour = None
    for s in range(samples):
        term = wide[:, s * LANES : (s + 1) * LANES] * heads[s][:, :LANES]
        colour = term if colour is None else colour + term
    return colour, depth


def depth_rows(depth, step):
    turned = depth.T
    pair = jnp.concatenate([turned[0:1], turned[step : step + 1]], axis=0)
    high, low = split16(pair)
    return jnp.concatenate([high, low], axis=0)


def edges_kernel(
    cfg, order_hbm, seam_hbm, own_hbm, *rest
):
    n = (len(rest) - 9) // 2
    sources, targets = rest[:n], rest[n + 1 : 2 * n + 1]
    own_ref = rest[n]
    meta_ref, near_ref, far_ref, spread, left, right, order_ref, seam_ref, sems = rest[2 * n + 1 :]
    cols, rows_all = cfg["cols"], cfg["rows_all"]
    blocks = own_ref.shape[0]
    small = [
        pltpu.make_async_copy(order_hbm, order_ref, sems.at[n + 1]),
        pltpu.make_async_copy(seam_hbm, seam_ref, sems.at[n + 2]),
    ]
    for copy in small:
        copy.start()
    load = pltpu.make_async_copy(own_hbm, own_ref, sems.at[0])
    load.start()
    more = [
        pltpu.make_async_copy(source, target, sems.at[1 + i])
        for i, (source, target) in enumerate(zip(sources, targets))
    ]
    for copy in more:
        copy.start()
    nb = cfg["nb"]
    lane = lax.broadcasted_iota(jnp.int32, (16, LANES), 1)
    spread[...] = one_hot(
        spread.shape,
        lambda r, c: (r & (LANES - 1)) == c // (LANES // blocks) * cfg["repeat"],
    )
    for copy in small:
        copy.wait()
    meta = jnp.where(lane == nb, seam_ref[0], 0)
    for k in range(nb):
        meta = jnp.where(lane == k, order_ref[0, k], meta)
    meta = meta.astype(F32).astype(BF16)
    load.wait()
    size = blocks * rows_all * EDGE
    for b in range(blocks):
        for r in range(rows_all):
            q = (b * rows_all + r) * EDGE
            left[q : q + EDGE, :] = own_ref[b, r * cols : r * cols + 16, :].astype(F32)[:EDGE]
            last = own_ref[b, (r + 1) * cols - 16 : (r + 1) * cols, :].astype(F32)
            right[q : q + EDGE, :] = last[16 - EDGE :]
    meta_ref[...] = meta
    odd = (lax.axis_index("patch") & 1) == 1
    near_ref[:size, :] = jnp.where(odd, left[...], right[...]).astype(BF16)
    far_ref[:size, :] = jnp.where(odd, right[...], left[...]).astype(BF16)
    near_ref[size:, :] = meta
    far_ref[size:, :] = meta
    for copy in more:
        copy.wait()


def field_chunks(cfg, own_ref, nets, col_own, dep_own, pieces, extra=None):
    pad = EDGE * cfg["cols"]
    blocks = own_ref.shape[0]

    def start(chunk):
        xs = [
            jnp.concatenate([own_ref[b, pl.ds(at, LANES), :] for at in chunk], axis=0)
            for b in range(blocks)
        ]
        return field_heads(xs, *nets, cfg["samples"], cfg["enc"])

    def finish(chunk, heads):
        colour, depth = field_mix(heads, nets[3])
        for k, at in enumerate(chunk):
            rows = slice(k * LANES, (k + 1) * LANES)
            col_own[pl.ds(pl.multiple_of(at + pad, LANES), LANES), :] = colour[rows].astype(BF16)
            q = pl.multiple_of((at + pad) // LANES * 8, 8)
            dep_own[pl.ds(q, 4), :] = depth_rows(depth[rows], cfg["repeat"])

    waiting = None
    for chunk in pieces:
        heads = start(chunk)
        if waiting is not None:
            finish(*waiting)
        waiting = (chunk, heads)
    made = None if extra is None else field_heads(extra, *nets, cfg["samples"], cfg["enc"])
    finish(*waiting)
    return made


def grouped(items, n):
    return [items[i : i + n] for i in range(0, len(items), n)]


def row_pieces(cfg, place, near):
    per = LANES // cfg["cols"]
    chip = place >> 1
    if cfg["groups"] == 4:
        first = jnp.where(chip == 0, 0, cfg["rows_all"] - cfg["n_near"])
    else:
        first = chip * (2 * cfg["rows_dev"]) + EDGE
    n = cfg["n_near"] if near else cfg["rows_all"] - cfg["n_near"]
    first = first if near else first + cfg["n_near"]
    starts = []
    for k in range(n // per):
        row = lax.rem(first + k * per, cfg["rows_all"])
        starts.append(pl.multiple_of(row * cfg["cols"], LANES))
    return starts


def field_kernel(
    cfg, own_ref, win_ref, wmid_ref, wf_ref, wd_ref, spread, col_own, dep_own, tiled, whead
):
    samples, enc = cfg["samples"], cfg["enc"]
    blocks = own_ref.shape[0]
    pad = EDGE * cfg["cols"]
    count = cfg["rows_all"] * cfg["cols"]
    col_own[0:pad, :] = jnp.zeros((pad, LANES), BF16)
    col_own[pad + count :, :] = jnp.zeros((pad, LANES), BF16)
    ends = 8 * pad // LANES
    dep_own[0:ends, :] = jnp.zeros((ends, LANES), F32)
    dep_own[dep_own.shape[0] - ends :, :] = jnp.zeros((ends, LANES), F32)
    for b in range(blocks):
        for s in range(samples):
            tiled[b, s * enc : (s + 1) * enc, :] = win_ref[b]
    feat, width = wf_ref.shape[2], wf_ref.shape[1]
    repeat = cfg["repeat"]
    dens = wd_ref[...].astype(F32)
    group = lax.broadcasted_iota(jnp.int32, (width, LANES), 1) // repeat
    for b in range(blocks):
        lift = one_hot((feat, LANES), lambda r, c: c - b * feat == r)
        r = lax.broadcasted_iota(jnp.int32, (width, width), 0)
        c = lax.broadcasted_iota(jnp.int32, (width, width), 1)
        diag = jnp.where(r == c, dens[b : b + 1], 0.0).astype(BF16)
        features = dot(wf_ref[b], lift).astype(BF16)
        column = dot(diag, jnp.ones((width, LANES), BF16))
        for s in range(samples):
            whead[b, s, :, :LANES] = features
            whead[b, s, :, LANES:] = jnp.where(group == s * blocks + b, column, 0.0).astype(BF16)
    nets = (tiled, wmid_ref, whead, spread)
    pieces = row_pieces(cfg, lax.axis_index("block"), False)[:-1]
    field_chunks(cfg, own_ref, nets, col_own, dep_own, grouped(pieces, cfg["chunk"]))


def pack(cfg, place, s, out, col_own, dep_own, col_halo, dep_halo):
    n_own, n_halo, n_dep = cfg["n_own"], cfg["n_halo"], cfg["n_dep"]
    cols, rows_dev = cfg["cols"], cfg["rows_dev"]
    half = n_halo // 2
    dest = place ^ s
    start = pl.multiple_of(dest * (rows_dev * cols), LANES)
    out[0:n_own, :] = col_own[pl.ds(start, n_own), :]
    for i in range(2):
        start = pl.multiple_of(i * cfg["side_pitch"] + dest * (rows_dev * EDGE), 8)
        q = n_own + i * half
        out[q : q + half, :] = col_halo[pl.ds(start, half), :].astype(BF16)
    start = pl.multiple_of(dest * (8 * rows_dev * cols // LANES), 8)
    at = n_own + n_halo
    groups = n_dep // 4
    rows = dep_own[pl.ds(start, 8 * groups), :]
    rows = jnp.concatenate([rows[8 * k : 8 * k + 4] for k in range(groups)], axis=0)
    out[at : at + n_dep, :] = rows.astype(BF16)
    out[at + n_dep :, :] = dep_halo[...].astype(BF16)


def halo_kernel(
    cfg, near_ref, far_ref, own_ref, tiled, wmid_ref, whead, spread, col_in, dep_in, *rest
):
    outs = rest[: cfg["groups"] - 2]
    col_halo, dep_halo, meta, col_own, dep_own, halo_ref = rest[cfg["groups"] - 2 :]
    col_own[...] = col_in[...]
    dep_own[...] = dep_in[...]
    rows_all = cfg["rows_all"]
    blocks = halo_ref.shape[0]
    odd = (lax.axis_index("patch") & 1) == 1
    near, far = near_ref[...].astype(F32), far_ref[...].astype(F32)
    sides = [jnp.where(odd, near, far), jnp.where(odd, far, near)]
    side_rays = rows_all * EDGE
    halo_ref[...] = jnp.zeros(halo_ref.shape, F32)
    for b in range(blocks):
        for i, side in enumerate(sides):
            q = i * cfg["side_pitch"] + EDGE * EDGE
            halo_ref[b, q : q + side_rays, :] = side[b * side_rays : (b + 1) * side_rays]
    for i, side in enumerate(sides):
        meta[8 * i : 8 * i + 8, :] = side[blocks * side_rays : blocks * side_rays + 8]
    xs = [halo_ref[b].astype(BF16) for b in range(blocks)]
    nets = (tiled, wmid_ref, whead, spread)
    pieces = row_pieces(cfg, lax.axis_index("block"), False)[-1:]
    heads = field_chunks(cfg, own_ref, nets, col_own, dep_own, [pieces], xs)
    colour, depth = field_mix(heads, spread)
    col_halo[...] = colour
    dep_halo[...] = jnp.zeros(dep_halo.shape, F32)
    hrays = depth.shape[0]
    for k in range(cfg["hchunks"]):
        part = depth[k * LANES : min((k + 1) * LANES, hrays)]
        if part.shape[0] < LANES:
            part = jnp.concatenate([part, jnp.zeros((LANES - part.shape[0], LANES), F32)], axis=0)
        dep_halo[4 * k : 4 * k + 4, :] = depth_rows(part, cfg["repeat"])
    for s in range(2, cfg["groups"]):
        pack(cfg, lax.axis_index("block"), s, outs[s - 2], col_own, dep_own, col_halo, dep_halo)


def earlier_blocks(cfg, place, order, rows):
    groups, nb = cfg["groups"], cfg["nb"]
    per = nb // groups
    sub = lax.broadcasted_iota(jnp.int32, (rows, LANES), 0)
    lane = lax.broadcasted_iota(jnp.int32, (rows, LANES), 1)
    hit = (jnp.broadcast_to(order, (rows, LANES)) == sub.astype(F32)) & (lane < nb)
    rank = jnp.sum(jnp.where(hit, lane.astype(F32), 0.0), axis=1, keepdims=True)
    rank = jnp.broadcast_to(rank, (rows, LANES))
    block = ((lane // (2 * per)) ^ place) * per + lane % per
    other = jnp.sum(jnp.where(sub == block, rank, 0.0), axis=0, keepdims=True)
    return jnp.where(other < rank, 1.0, 0.0)


def near_kernel(
    cfg, own_ref, tiled, wmid_ref, whead, spread, col_in, dep_in, col_halo, dep_halo,
    meta_sides, meta_own, out_own, out_mate, earlier, flags, col_own, dep_own,
):
    nb, patch = cfg["nb"], lax.axis_index("patch")
    mine = meta_own[...].astype(F32)[0:1]
    sides = [mine, meta_sides[0:1, :], meta_sides[8:9, :]]
    rows = earlier.shape[0] // 3
    for i, order in enumerate(sides):
        made = earlier_blocks(cfg, lax.axis_index("block"), order, rows)
        earlier[i * rows : (i + 1) * rows, :] = made.astype(BF16)
    lane = lax.broadcasted_iota(jnp.int32, (1, LANES), 1)
    for i, (order, there) in enumerate([(sides[1], patch > 0), (mine, patch < cfg["patches"] - 1)]):
        seam = jnp.sum(jnp.where(lane == nb, order, 0.0), axis=1, keepdims=True)
        seam = jnp.where(there, seam, 0.0)
        flags[8 * i : 8 * i + 8, :] = jnp.broadcast_to(seam, (8, LANES))
    col_own[...] = col_in[...]
    dep_own[...] = dep_in[...]
    nets = (tiled, wmid_ref, whead, spread)
    pieces = row_pieces(cfg, lax.axis_index("block"), True)
    field_chunks(cfg, own_ref, nets, col_own, dep_own, grouped(pieces, cfg["chunk"]))
    pack(cfg, lax.axis_index("block"), 0, out_own, col_own, dep_own, col_halo, dep_halo)
    pack(cfg, lax.axis_index("block"), 1, out_mate, col_own, dep_own, col_halo, dep_halo)


def decoder_kernel(cfg, earlier_ref, flags_ref, mask_ref, pick_ref, w0_ref, w1_ref, w2_ref, w3_ref, *rest):
    groups, nb = cfg["groups"], cfg["nb"]
    bufs = rest[:groups]
    out_ref = rest[groups]
    comp, x0, sa, xa, sc, xc, rep = rest[groups + 1 :]
    cols, rows_dev, pitch = cfg["cols"], cfg["rows_dev"], cfg["pitch"]
    n_own, n_halo, n_dep = cfg["n_own"], cfg["n_halo"], cfg["n_dep"]
    rows_in = rows_dev + 2 * EDGE
    rows_mid = rows_dev + 2
    mid = rows_mid * pitch
    half = LANES // 2
    per_dev = nb // groups
    place = lax.axis_index("block")
    left_open, right_open = flags_ref[0:1, :], flags_ref[8:9, :]
    sides = earlier_ref.shape[0] // 3
    stacked = 2 * per_dev * groups
    earlier = [earlier_ref[i * sides : i * sides + nb, :stacked] for i in range(3)]

    at = n_own + n_halo
    own_rows = [bufs[s][at : at + n_dep, :].astype(F32) for s in range(groups)]
    halo_rows = [bufs[s][at + n_dep :, :].astype(F32) for s in range(groups)]
    chunks = n_own // LANES
    factors = []
    for k in range(chunks):
        stack = jnp.concatenate([own_rows[s][4 * k : 4 * k + 4] for s in range(groups)], axis=0)
        factors.append(jnp.exp(-dot(earlier[0], stack.astype(BF16))))
    lane = lax.broadcasted_iota(jnp.int32, (nb, LANES), 1)
    side_pitch = (cfg["rows_all"] + 2 * EDGE) * EDGE
    for k in range(cfg["hchunks"]):
        on_left = lane + k * LANES < side_pitch
        stack = jnp.concatenate(
            [halo_rows[s][4 * k : 4 * k + 4] for s in range(groups)], axis=0
        ).astype(BF16)
        from_left = jnp.exp(-dot(earlier[1], stack)) * left_open
        from_right = jnp.exp(-dot(earlier[2], stack)) * right_open
        factors.append(jnp.where(on_left, from_left, from_right))
    steps = len(factors)
    factors.append(jnp.zeros((LANES - steps * nb, LANES), F32))
    turned = jnp.concatenate(factors, axis=0).T
    lhs = []
    for k in range(steps):
        high, low = split16(pltpu.roll(turned, (LANES - k * nb) % LANES, 1) if k else turned)
        lhs.append(jnp.concatenate([high.astype(BF16), low.astype(BF16)], axis=1))
    lane = lax.broadcasted_iota(jnp.int32, (2 * LANES, groups * LANES), 1)
    block = ((lane // LANES) ^ place) * per_dev + (lane & (LANES - 1)) // half
    sub = lax.broadcasted_iota(jnp.int32, (2 * LANES, groups * LANES), 0) & (LANES - 1)
    wide = dot(jnp.concatenate(lhs, axis=0), jnp.where(sub == block, 1.0, 0.0).astype(BF16))

    def spread(k):
        return wide[k * LANES : (k + 1) * LANES]

    def mix(weights, lo, n):
        acc = None
        for s in range(groups):
            term = weights[:, s * LANES : (s + 1) * LANES] * bufs[s][lo : lo + n, :].astype(F32)
            acc = term if acc is None else acc + term
        return acc + pltpu.roll(acc, half, 1)

    comp[...] = jnp.zeros(comp.shape, F32)
    base = pitch
    per_chunk = LANES // cols
    for k in range(chunks):
        mixed = mix(spread(k), k * LANES, LANES)
        for t in range(per_chunk):
            q = base + (k * per_chunk + t) * pitch + LEAD
            comp[q : q + cols, :] = mixed[t * cols : (t + 1) * cols]
    for k in range(cfg["hchunks"]):
        rep[k * LANES : (k + 1) * LANES, :] = spread(chunks + k)
    size = n_halo // 2
    for i in range(2):
        start = pl.multiple_of(i * side_pitch + place * (rows_dev * EDGE), 8)
        mixed = mix(rep[pl.ds(start, size), :], n_own + i * size, size)
        for r in range(rows_in):
            q = base + r * pitch + LEAD + (cols if i else -EDGE)
            comp[q : q + EDGE, :] = mixed[r * EDGE : (r + 1) * EDGE]

    n_in = rows_in * pitch
    lane = lax.broadcasted_iota(jnp.int32, (n_in, LANES), 1)
    here = jnp.where(lane < half, comp[base - 1 : base - 1 + n_in, :], comp[base : base + n_in, :])
    x0[:, 0:LANES] = here.astype(BF16)
    x0[:, LANES : 2 * LANES] = comp[base + 1 : base + 1 + n_in, :].astype(BF16)

    mask = mask_ref[...]

    def convolve(ref, pieces, n, weights):
        made = []
        for h in range(2):
            lhs = jnp.concatenate(
                [ref[r * pitch + h * n // 2 : r * pitch + (h + 1) * n // 2, a:b] for r, a, b in pieces],
                axis=1,
            )
            made.append(dot_t(lhs, weights))
        return jnp.concatenate(made, axis=0)

    wide = 2 * LANES
    value = convolve(x0, [(d, 0, wide) for d in range(3)], mid, w0_ref[...])
    value = jnp.maximum(value, 0.0) * mask

    sa[0:8, :] = jnp.zeros((8, wide), F32)
    sa[8 + mid :, :] = jnp.zeros((8, wide), F32)
    xa[0:pitch, :] = jnp.zeros((pitch, 2 * wide), BF16)
    xa[pitch + mid :, :] = jnp.zeros((pitch, 2 * wide), BF16)
    low = lax.broadcasted_iota(jnp.int32, (mid, LANES), 1) < half

    def beside(after, before):
        return jnp.where(low, after, before).astype(BF16)

    def lay_out(value):
        sa[8 : 8 + mid, :] = value
        for pr in range(2):
            own = slice(pr * LANES, (pr + 1) * LANES)
            xa[pitch : pitch + mid, pr * wide : pr * wide + LANES] = value[:, own].astype(BF16)
            xa[pitch : pitch + mid, pr * wide + LANES : (pr + 1) * wide] = beside(
                sa[9 : 9 + mid, own], sa[7 : 7 + mid, own]
            )

    lay_out(value)
    value = convolve(
        xa, [(0, wide, 2 * wide), (1, 0, 2 * wide), (2, 0, wide)], mid, w1_ref[...]
    )
    value = jnp.maximum(value, 0.0) * mask
    lay_out(value)
    three = 3 * LANES
    for pr in range(2):
        pieces = [(0, wide, 2 * wide), (1, 0, 2 * wide)] if pr == 0 else [(1, 0, 2 * wide), (2, 0, wide)]
        both = convolve(xa, pieces, mid, w2_ref[...])
        for pc in range(2):
            value = jnp.maximum(both[:, pc * wide : (pc + 1) * wide], 0.0) * mask
            sc[2 * pr + pc, 8 : 8 + mid, :] = value
            for rr in range(2):
                at = (2 * pr + rr) * three + pc * LANES
                xc[:, at : at + LANES] = value[:, rr * LANES : (rr + 1) * LANES].astype(BF16)
        for rr in range(2):
            own = slice(rr * LANES, (rr + 1) * LANES)
            at = (2 * pr + rr) * three + 2 * LANES
            xc[:, at : at + LANES] = beside(
                sc[2 * pr, 9 : 9 + mid, own], sc[2 * pr + 1, 7 : 7 + mid, own]
            )
    n_out = rows_dev * pitch
    final = convolve(
        xc, [(0, 3 * three, 4 * three), (1, 0, 4 * three), (2, 0, three)], n_out, w3_ref[...]
    )
    final = final + pltpu.roll(final, half, 1)
    rays = jnp.concatenate(
        [final[r * pitch + LEAD : r * pitch + LEAD + cols] for r in range(rows_dev)], axis=0
    )
    turned = rays.T
    stack = jnp.concatenate(
        [
            jnp.concatenate(
                [turned[16 * v : 16 * v + 16, r * cols : (r + 1) * cols] for v in range(4)], axis=1
            )
            for r in range(rows_dev)
        ],
        axis=0,
    )
    pick = pick_ref[...]
    high, low = split16(stack)
    image = dot(high.astype(BF16), pick) + dot(low.astype(BF16), pick)
    colours = out_ref.shape[0]
    for r in range(rows_dev):
        for u in range(4):
            for p in range(colours):
                at = r * 16 + u * 4 + p
                out_ref[p, 4 * r + u : 4 * r + u + 1, :] = image[at : at + 1, :]


def phase_taps(p, d):
    return [a for a in range(3) if (p + a - 1) // 2 + 1 == d]


def weights_kernel(
    cfg, conv_ref, colour_ref, flags_ref, w0_ref, w1_ref, w2_ref, w3_ref, mask_ref, pick_ref
):
    feat = conv_ref.shape[1]
    r = lax.broadcasted_iota(jnp.int32, (feat, LANES), 0)
    lane = lax.broadcasted_iota(jnp.int32, (feat, LANES), 1)
    twice = jnp.where((lane == r) | (lane == r + feat), 1.0, 0.0).astype(BF16)
    low = lane < feat
    zero = jnp.zeros((feat, LANES), F32)
    taps = [
        dot(conv_ref[k * 9 * feat : (k + 1) * 9 * feat, :], twice) for k in range(4)
    ]

    def tap(k, a, e):
        at = (a * 3 + e) * feat
        return taps[k][at : at + feat]

    def pair(left, right):
        if left is None and right is None:
            return zero
        if left is right:
            return left
        return jnp.where(low, zero if left is None else left, zero if right is None else right)

    def put(ref, n, j, tile):
        ref[n * feat : (n + 1) * feat, j * LANES : (j + 1) * LANES] = tile.astype(BF16)

    for k in (0, 2):
        sums = {}
        for p in range(2):
            for q in range(2):
                for d in range(3):
                    for f in range(3):
                        parts = [tap(k, a, e) for a in phase_taps(p, d) for e in phase_taps(q, f)]
                        sums[p, q, d, f] = functools.reduce(jnp.add, parts) if parts else None
        for p in range(2):
            for q in range(2):
                n = 2 * p + q
                for d in range(3):
                    row = [sums[p, q, d, f] for f in range(3)]
                    if k == 0:
                        makes = [(w0_ref, n, row + [None])]
                    else:
                        makes = [
                            (w2_ref, n, [row[1], row[2], None, row[0]]),
                            (w2_ref, 4 + n, row + [None]),
                        ]
                    for ref, at, blocks in makes:
                        put(ref, at, 2 * d, pair(blocks[0], blocks[1]))
                        put(ref, at, 2 * d + 1, pair(blocks[2], blocks[3]))

    def pick(table, a, e):
        return table(a, e) if 0 <= a < 3 and 0 <= e < 3 else None

    for p in range(2):
        for q in range(2):
            for row in range(4):
                for j, at in enumerate([(2, 3), (4, 1)]):
                    blocks = [
                        pick(lambda a, e: tap(1, a, e), row - p, c - 1 - q) for c in at
                    ]
                    put(w1_ref, 2 * p + q, row * 2 + j, pair(*blocks))

    colours = colour_ref.shape[0]
    given = colour_ref[...].astype(F32)
    sub = lax.broadcasted_iota(jnp.int32, (8, feat), 0)
    mixer = jnp.zeros((8, feat), F32)
    for p in range(colours):
        mixer = jnp.where((sub & 3) == p, given[p : p + 1], mixer)
    mixer = mixer.astype(BF16)
    mixed = {
        (a, e): dot(mixer, tap(3, a, e).astype(BF16)) for a in range(3) for e in range(3)
    }
    lane = lax.broadcasted_iota(jnp.int32, (8, LANES), 1) < feat
    upper = lax.broadcasted_iota(jnp.int32, (8, LANES), 0) < 4
    blank = jnp.zeros((8, LANES), F32)

    def choose(mask, x, y):
        if x is None and y is None:
            return None
        return jnp.where(mask, blank if x is None else x, blank if y is None else y)

    for row in range(6):
        for j, (c_left, c_right) in enumerate([(2, 3), (4, 5), (6, 1)]):
            pieces = []
            for v in range(4):
                for u in (0, 2):
                    halves = [
                        choose(
                            lane,
                            pick(lambda a, e: mixed[a, e], row - w, c_left - 1 - v),
                            pick(lambda a, e: mixed[a, e], row - w, c_right - 1 - v),
                        )
                        for w in (u, u + 1)
                    ]
                    made = choose(upper, *halves)
                    pieces.append(blank if made is None else made)
            tile = jnp.concatenate(pieces, axis=0)
            high, low16 = split16(tile)
            at = (row * 3 + j) * LANES
            w3_ref[:, at : at + LANES] = jnp.concatenate([high, low16], axis=0).astype(BF16)

    cols, pitch, rows_mid = cfg["cols"], cfg["pitch"], cfg["rows_dev"] + 2
    place, mid = lax.axis_index("block"), rows_mid * pitch
    left_open, right_open = flags_ref[0:1, :], flags_ref[8:9, :]
    top_open = jnp.where(place > 0, 1.0, 0.0)
    bottom_open = jnp.where(place < cfg["groups"] - 1, 1.0, 0.0)
    q = lax.broadcasted_iota(jnp.int32, (mid, 2 * LANES), 0)
    pos = q
    for r in range(1, rows_mid):
        pos = pos - jnp.where(q >= r * pitch, pitch, 0)
    left_open = jnp.concatenate([left_open, left_open], axis=1)
    right_open = jnp.concatenate([right_open, right_open], axis=1)
    mask = jnp.where(pos < LEAD, left_open, jnp.where(pos >= LEAD + cols, right_open, 1.0))
    mask = mask * jnp.where(q < pitch, top_open, jnp.where(q >= mid - pitch, bottom_open, 1.0))
    mask_ref[...] = mask
    r = lax.broadcasted_iota(jnp.int32, (4 * cols, 4 * cols), 0)
    c = lax.broadcasted_iota(jnp.int32, (4 * cols, 4 * cols), 1)
    place_of = (c & 3) * cols + (c >> 2)
    pick = jnp.where(r == place_of, 1.0, 0.0).astype(BF16)
    pick_ref[...] = pick


def body(samples_in, block_order, seam_link, w_in, w_mid, w_feat, w_density, w_conv, w_color):
    blk_dev, rows_all, cols, width = samples_in.shape
    groups, patches = lax.axis_size("block"), lax.axis_size("patch")
    nb = block_order.shape[1]
    enc = w_in.shape[1]
    feat = w_feat.shape[2]
    rows_dev = rows_all // groups
    count = rows_all * cols
    hrays = (rows_all + 2 * EDGE) * 2 * EDGE
    hchunks = -(-hrays // LANES)
    n_own = (rows_dev + 2 * EDGE) * cols
    n_halo = (rows_dev + 2 * EDGE) * 2 * EDGE
    n_dep = 4 * n_own // LANES
    n_tail = 16
    samples = width // enc
    cfg = dict(
        groups=groups,
        nb=nb,
        patches=patches,
        samples=samples,
        enc=enc,
        repeat=LANES // (samples * blk_dev),
        cols=cols,
        rows_all=rows_all,
        rows_dev=rows_dev,
        n_near=2 * rows_dev - (EDGE if groups == 4 else 2 * EDGE),
        side_pitch=hrays // 2,
        pitch=cols + 16,
        chunk=2,
        n_own=n_own,
        n_halo=n_halo,
        n_dep=n_dep,
        hchunks=hchunks,
    )
    vmem = pl.BlockSpec(memory_space=pltpu.VMEM)
    hbm = pl.BlockSpec(memory_space=pltpu.HBM)
    params = pltpu.CompilerParams(vmem_limit_bytes=16 * 1024 * 1024)

    def far_off(x):
        return pltpu.with_memory_space_constraint(x, pltpu.HBM)


    edges = blk_dev * rows_all * EDGE
    early = [w_in, w_mid, w_density, w_color]
    own, win, wmid, dens, colour, meta_own, near, far, spread = pl.pallas_call(
        functools.partial(edges_kernel, cfg),
        out_shape=[pltpu.VMEM((blk_dev, count, width), BF16)]
        + [pltpu.VMEM(x.shape, BF16) for x in early]
        + [
            pltpu.VMEM((16, width), BF16),
            pltpu.VMEM((edges + 16, width), BF16),
            pltpu.VMEM((edges + 16, width), BF16),
            pltpu.VMEM((2 * LANES, samples * LANES), BF16),
        ],
        in_specs=[hbm] * (3 + len(early)),
        out_specs=[vmem] * (5 + len(early)),
        scratch_shapes=[
            pltpu.VMEM((edges, width), F32),
            pltpu.VMEM((edges, width), F32),
            pltpu.SMEM(block_order.shape, jnp.int32),
            pltpu.SMEM(seam_link.shape, jnp.int32),
            pltpu.SemaphoreType.DMA((3 + len(early),)),
        ],
        compiler_params=params,
        name="edges",
    )(
        far_off(block_order),
        seam_link,
        far_off(samples_in.reshape(blk_dev, count, width)),
        *[far_off(x) for x in early],
    )
    swap_near = [(i, i ^ 1) for i in range(patches) if i ^ 1 < patches]
    swap_far = []
    for i in range(1, patches - 1, 2):
        swap_far += [(i, i + 1), (i + 1, i)]
    far = lax.ppermute(far, "patch", swap_far)
    near = lax.ppermute(near, "patch", swap_near)

    rays_flops = 2 * 2 * blk_dev * samples * w_mid.shape[2] * (3 * w_mid.shape[2])
    far_rays = (rows_all - cfg["n_near"]) * cols
    col_own, dep_own, tiled, whead = pl.pallas_call(
        functools.partial(field_kernel, cfg),
        out_shape=[
            pltpu.VMEM((count + 2 * EDGE * cols, LANES), BF16),
            pltpu.VMEM((8 * (count + 2 * EDGE * cols) // LANES, LANES), F32),
            pltpu.VMEM((blk_dev, width, w_in.shape[2]), BF16),
            pltpu.VMEM((blk_dev, samples, w_feat.shape[1], 2 * LANES), BF16),
        ],
        in_specs=[vmem] * 6,
        out_specs=[vmem] * 4,
        compiler_params=params,
        cost_estimate=pl.CostEstimate(
            flops=far_rays * rays_flops, bytes_accessed=10**6, transcendentals=0
        ),
        name="field",
    )(own, win, wmid, w_feat, dens, spread)

    size = n_own + n_halo + n_dep + n_tail
    shape = pltpu.VMEM((size, LANES), BF16)
    *bufs, col_halo, dep_halo, meta, col_own, dep_own = pl.pallas_call(
        functools.partial(halo_kernel, cfg),
        out_shape=[shape] * (groups - 2)
        + [
            pltpu.VMEM((hrays, LANES), F32),
            pltpu.VMEM((n_tail, LANES), F32),
            pltpu.VMEM((16, LANES), F32),
            pltpu.VMEM(col_own.shape, BF16),
            pltpu.VMEM(dep_own.shape, F32),
        ],
        in_specs=[vmem] * 9,
        out_specs=[vmem] * (groups + 3),
        scratch_shapes=[pltpu.VMEM((blk_dev, hrays, width), F32)],
        compiler_params=params,
        name="halo",
    )(near, far, own, tiled, wmid, whead, spread, col_own, dep_own)
    got = []
    for s in range(2, groups):
        got.append(lax.ppermute(bufs[s - 2], "block", [(i, i ^ s) for i in range(groups)]))

    near_rows = pl.pallas_call(
        functools.partial(near_kernel, cfg),
        out_shape=[shape] * 2
        + [pltpu.VMEM((48, LANES), BF16), pltpu.VMEM((16, LANES), F32)],
        in_specs=[vmem] * 11,
        out_specs=[vmem] * 4,
        scratch_shapes=[
            pltpu.VMEM(col_own.shape, BF16),
            pltpu.VMEM(dep_own.shape, F32),
        ],
        compiler_params=params,
        cost_estimate=pl.CostEstimate(
            flops=cfg["n_near"] * cols * rays_flops, bytes_accessed=10**6, transcendentals=0
        ),
        name="near",
    )
    mine, mate, earlier, flags = near_rows(
        own, tiled, wmid, whead, spread, col_own, dep_own, col_halo, dep_halo, meta, meta_own
    )
    got = [mine, lax.ppermute(mate, "block", [(i, i ^ 1) for i in range(groups)])] + got

    pitch = cfg["pitch"]
    rows_in, rows_mid = rows_dev + 2 * EDGE, rows_dev + 2
    w0, w1, w2, w3, mask, pick = pl.pallas_call(
        functools.partial(weights_kernel, cfg),
        out_shape=[
            pltpu.VMEM((4 * feat, 12 * feat), BF16),
            pltpu.VMEM((4 * feat, 16 * feat), BF16),
            pltpu.VMEM((8 * feat, 12 * feat), BF16),
            pltpu.VMEM((2 * feat, 36 * feat), BF16),
            pltpu.VMEM((rows_mid * pitch, 2 * LANES), F32),
            pltpu.VMEM((4 * cols, 4 * cols), BF16),
        ],
        in_specs=[vmem] * 3,
        out_specs=[vmem] * 6,
        compiler_params=params,
        cost_estimate=pl.CostEstimate(flops=10**8, bytes_accessed=10**6, transcendentals=0),
        name="weights",
    )(w_conv.reshape(-1, feat), colour, flags)
    return pl.pallas_call(
        functools.partial(decoder_kernel, cfg),
        out_shape=jax.ShapeDtypeStruct((w_color.shape[0], 4 * rows_dev, 4 * cols), F32),
        in_specs=[vmem] * (8 + groups),
        out_specs=vmem,
        scratch_shapes=[
            pltpu.VMEM(((rows_in + 2) * pitch, LANES), F32),
            pltpu.VMEM((rows_in * pitch, 2 * LANES), BF16),
            pltpu.VMEM((rows_mid * pitch + 16, 2 * LANES), F32),
            pltpu.VMEM(((rows_mid + 2) * pitch, 4 * LANES), BF16),
            pltpu.VMEM((4, rows_mid * pitch + 16, 2 * LANES), F32),
            pltpu.VMEM((rows_mid * pitch, 12 * LANES), BF16),
            pltpu.VMEM((hchunks * LANES, groups * LANES), F32),
        ],
        compiler_params=params,
        name="decoder",
    )(earlier, flags, mask, pick, w0, w1, w2, w3, *got)


def solution(mesh):
    return jax.shard_map(
        body,
        mesh=mesh,
        in_specs=(
            P("block", None, "patch", None),
            P("patch", None),
            P("patch"),
            P("block", None, None),
            P("block", None, None, None),
            P("block", None, None),
            P("block", None),
            P(),
            P(),
        ),
        out_specs=P(None, "block", "patch"),
        check_vma=False,
    )
```

```python
import functools

import jax
import jax.numpy as jnp
from jax import lax
from jax.experimental import pallas as pl
from jax.experimental.pallas import tpu as pltpu
from jax.sharding import PartitionSpec as P


STEP = 0.03
LANES = 128
EDGE = 2
LEAD = 8
F32 = jnp.float32
BF16 = jnp.bfloat16


def dot(a, b):
    return jnp.dot(a, b, preferred_element_type=F32)


def dot_t(a, b):
    return lax.dot_general(a, b, (((1,), (1,)), ((), ())), preferred_element_type=F32)


def relu16(x):
    return jnp.maximum(x.astype(BF16), jnp.zeros((), BF16))


def softplus(v):
    e = jnp.exp(-jnp.abs(v))
    tail = jnp.where(e < 1e-3, e * (1.0 - e * (0.5 - e * (1.0 / 3.0))), jnp.log(1.0 + e))
    return jnp.maximum(v, 0.0) + tail


def stopped(optical):
    small = optical * (1.0 - optical * (0.5 - optical * (1.0 / 6.0 - optical * (1.0 / 24.0))))
    return jnp.where(optical < 0.0625, small, 1.0 - jnp.exp(-optical))


def split16(x):
    high = x.astype(BF16).astype(F32)
    return high, x - high


def one_hot(shape, test):
    r = lax.broadcasted_iota(jnp.int32, shape, 0)
    c = lax.broadcasted_iota(jnp.int32, shape, 1)
    return jnp.where(test(r, c), 1.0, 0.0).astype(BF16)


def field_heads(xs, tiled, wmid, whead, spread, samples, enc):
    rays = xs[0].shape[0]
    lane = lax.broadcasted_iota(jnp.int32, xs[0].shape, 1)
    heads = [None] * samples
    for b, x in enumerate(xs):
        zero = jnp.zeros_like(x)
        parts = [
            jnp.where((lane >= s * enc) & (lane < (s + 1) * enc), x, zero) for s in range(samples)
        ]
        hidden = relu16(dot(jnp.concatenate(parts, axis=0), tiled[b]))
        hidden = relu16(dot(hidden, wmid[b, 0]))
        hidden = relu16(dot(hidden, wmid[b, 1]))
        for s in range(samples):
            made = dot(hidden[s * rays : (s + 1) * rays], whead[b, s])
            heads[s] = made if b == 0 else heads[s] + made
    return heads


def field_mix(heads, spread):
    samples, rays = len(heads), heads[0].shape[0]
    logit = heads[0][:, LANES:]
    for s in range(1, samples):
        logit = logit + heads[s][:, LANES:]
    optical = STEP * softplus(logit)
    group = LANES // samples
    lane = lax.broadcasted_iota(jnp.int32, (rays, LANES), 1)
    depth, before = optical, jnp.zeros((rays, LANES), F32)
    for s in range(1, samples):
        moved = pltpu.roll(optical, s * group, 1)
        depth = depth + moved
        before = before + jnp.where(lane >= s * group, moved, 0.0)
    weight = jnp.exp(-before) * stopped(optical)
    high, low = split16(weight)
    wide = dot(jnp.concatenate([high.astype(BF16), low.astype(BF16)], axis=1), spread[...])
    colour = None
    for s in range(samples):
        term = wide[:, s * LANES : (s + 1) * LANES] * heads[s][:, :LANES]
        colour = term if colour is None else colour + term
    return colour, depth


def depth_rows(depth, step):
    turned = depth.T
    pair = jnp.concatenate([turned[0:1], turned[step : step + 1]], axis=0)
    high, low = split16(pair)
    return jnp.concatenate([high, low], axis=0)


def edges_kernel(
    cfg, order_hbm, seam_hbm, own_hbm, *rest
):
    n = (len(rest) - 10) // 2
    sources, targets = rest[:n], rest[n : 2 * n]
    meta_ref, near_ref, far_ref, spread, ends, left, right, order_ref, seam_ref, sems = rest[2 * n :]
    cols, rows_all = cfg["cols"], cfg["rows_all"]
    blocks = own_hbm.shape[0]
    small = [
        pltpu.make_async_copy(order_hbm, order_ref, sems.at[n + 1]),
        pltpu.make_async_copy(seam_hbm, seam_ref, sems.at[n + 2]),
    ]
    for copy in small:
        copy.start()
    loads = [
        pltpu.make_async_copy(own_hbm.at[:, :, pl.ds(at, 8), :], ends.at[i], sems.at[n + 3 + i])
        for i, at in enumerate((0, cols - 8))
    ]
    for copy in loads:
        copy.start()
    more = [
        pltpu.make_async_copy(source, target, sems.at[i])
        for i, (source, target) in enumerate(zip(sources, targets))
    ]
    for copy in more:
        copy.start()
    nb = cfg["nb"]
    lane = lax.broadcasted_iota(jnp.int32, (16, LANES), 1)
    spread[...] = one_hot(
        spread.shape,
        lambda r, c: (r & (LANES - 1)) == c // (LANES // blocks) * cfg["repeat"],
    )
    for copy in small:
        copy.wait()
    meta = jnp.where(lane == nb, seam_ref[0], 0)
    for k in range(nb):
        meta = jnp.where(lane == k, order_ref[0, k], meta)
    meta = meta.astype(F32).astype(BF16)
    for copy in loads:
        copy.wait()
    size = blocks * rows_all * EDGE
    for b in range(blocks):
        for r in range(rows_all):
            q = (b * rows_all + r) * EDGE
            left[q : q + EDGE, :] = ends[0, b, r].astype(F32)[:EDGE]
            right[q : q + EDGE, :] = ends[1, b, r].astype(F32)[8 - EDGE :]
    meta_ref[...] = meta
    odd = (lax.axis_index("patch") & 1) == 1
    near_ref[:size, :] = jnp.where(odd, left[...], right[...]).astype(BF16)
    far_ref[:size, :] = jnp.where(odd, right[...], left[...]).astype(BF16)
    near_ref[size:, :] = meta
    far_ref[size:, :] = meta
    for copy in more:
        copy.wait()


def field_chunks(cfg, own_ref, nets, col_own, dep_own, pieces, extra=None):
    pad = EDGE * cfg["cols"]
    blocks = own_ref.shape[0]

    def start(chunk):
        xs = [
            jnp.concatenate([own_ref[b, pl.ds(at, LANES), :] for at in chunk], axis=0)
            for b in range(blocks)
        ]
        return field_heads(xs, *nets, cfg["samples"], cfg["enc"])

    def finish(chunk, heads):
        colour, depth = field_mix(heads, nets[3])
        for k, at in enumerate(chunk):
            rows = slice(k * LANES, (k + 1) * LANES)
            col_own[pl.ds(pl.multiple_of(at + pad, LANES), LANES), :] = colour[rows].astype(BF16)
            q = pl.multiple_of((at + pad) // LANES * 8, 8)
            dep_own[pl.ds(q, 4), :] = depth_rows(depth[rows], cfg["repeat"])

    waiting = None
    for chunk in pieces:
        heads = start(chunk)
        if waiting is not None:
            finish(*waiting)
        waiting = (chunk, heads)
    made = None if extra is None else field_heads(extra, *nets, cfg["samples"], cfg["enc"])
    finish(*waiting)
    return made


def grouped(items, n):
    return [items[i : i + n] for i in range(0, len(items), n)]


def row_pieces(cfg, place, near):
    per = LANES // cfg["cols"]
    chip = place >> 1
    if cfg["groups"] == 4:
        first = jnp.where(chip == 0, 0, cfg["rows_all"] - cfg["n_near"])
    else:
        first = chip * (2 * cfg["rows_dev"]) + EDGE
    n = cfg["n_near"] if near else cfg["rows_all"] - cfg["n_near"]
    first = first if near else first + cfg["n_near"]
    starts = []
    for k in range(n // per):
        row = lax.rem(first + k * per, cfg["rows_all"])
        starts.append(pl.multiple_of(row * cfg["cols"], LANES))
    return starts


def field_kernel(
    cfg, own_ref, win_ref, wmid_ref, wf_ref, wd_ref, spread, col_own, dep_own, tiled, whead
):
    samples, enc = cfg["samples"], cfg["enc"]
    blocks = own_ref.shape[0]
    pad = EDGE * cfg["cols"]
    count = cfg["rows_all"] * cfg["cols"]
    col_own[0:pad, :] = jnp.zeros((pad, LANES), BF16)
    col_own[pad + count :, :] = jnp.zeros((pad, LANES), BF16)
    ends = 8 * pad // LANES
    dep_own[0:ends, :] = jnp.zeros((ends, LANES), F32)
    dep_own[dep_own.shape[0] - ends :, :] = jnp.zeros((ends, LANES), F32)
    for b in range(blocks):
        for s in range(samples):
            tiled[b, s * enc : (s + 1) * enc, :] = win_ref[b]
    feat, width = wf_ref.shape[2], wf_ref.shape[1]
    repeat = cfg["repeat"]
    dens = wd_ref[...].astype(F32)
    group = lax.broadcasted_iota(jnp.int32, (width, LANES), 1) // repeat
    for b in range(blocks):
        lift = one_hot((feat, LANES), lambda r, c: c - b * feat == r)
        r = lax.broadcasted_iota(jnp.int32, (width, width), 0)
        c = lax.broadcasted_iota(jnp.int32, (width, width), 1)
        diag = jnp.where(r == c, dens[b : b + 1], 0.0).astype(BF16)
        features = dot(wf_ref[b], lift).astype(BF16)
        column = dot(diag, jnp.ones((width, LANES), BF16))
        for s in range(samples):
            whead[b, s, :, :LANES] = features
            whead[b, s, :, LANES:] = jnp.where(group == s * blocks + b, column, 0.0).astype(BF16)
    nets = (tiled, wmid_ref, whead, spread)
    pieces = row_pieces(cfg, lax.axis_index("block"), False)[:-1]
    field_chunks(cfg, own_ref, nets, col_own, dep_own, grouped(pieces, cfg["chunk"]))


def pack(cfg, place, s, out, col_own, dep_own, col_halo, dep_halo):
    n_own, n_halo, n_dep = cfg["n_own"], cfg["n_halo"], cfg["n_dep"]
    cols, rows_dev = cfg["cols"], cfg["rows_dev"]
    half = n_halo // 2
    dest = place ^ s
    start = pl.multiple_of(dest * (rows_dev * cols), LANES)
    out[0:n_own, :] = col_own[pl.ds(start, n_own), :]
    for i in range(2):
        start = pl.multiple_of(i * cfg["side_pitch"] + dest * (rows_dev * EDGE), 8)
        q = n_own + i * half
        out[q : q + half, :] = col_halo[pl.ds(start, half), :].astype(BF16)
    start = pl.multiple_of(dest * (8 * rows_dev * cols // LANES), 8)
    at = n_own + n_halo
    groups = n_dep // 4
    rows = dep_own[pl.ds(start, 8 * groups), :]
    rows = jnp.concatenate([rows[8 * k : 8 * k + 4] for k in range(groups)], axis=0)
    out[at : at + n_dep, :] = rows.astype(BF16)
    out[at + n_dep :, :] = dep_halo[...].astype(BF16)


def halo_kernel(
    cfg, near_ref, far_ref, own_ref, tiled, wmid_ref, whead, spread, col_in, dep_in, *rest
):
    outs = rest[: cfg["groups"] - 2]
    col_halo, dep_halo, meta, col_own, dep_own, halo_ref = rest[cfg["groups"] - 2 :]
    col_own[...] = col_in[...]
    dep_own[...] = dep_in[...]
    rows_all = cfg["rows_all"]
    blocks = halo_ref.shape[0]
    odd = (lax.axis_index("patch") & 1) == 1
    near, far = near_ref[...].astype(F32), far_ref[...].astype(F32)
    sides = [jnp.where(odd, near, far), jnp.where(odd, far, near)]
    side_rays = rows_all * EDGE
    halo_ref[...] = jnp.zeros(halo_ref.shape, F32)
    for b in range(blocks):
        for i, side in enumerate(sides):
            q = i * cfg["side_pitch"] + EDGE * EDGE
            halo_ref[b, q : q + side_rays, :] = side[b * side_rays : (b + 1) * side_rays]
    for i, side in enumerate(sides):
        meta[8 * i : 8 * i + 8, :] = side[blocks * side_rays : blocks * side_rays + 8]
    xs = [halo_ref[b].astype(BF16) for b in range(blocks)]
    nets = (tiled, wmid_ref, whead, spread)
    pieces = row_pieces(cfg, lax.axis_index("block"), False)[-1:]
    heads = field_chunks(cfg, own_ref, nets, col_own, dep_own, [pieces], xs)
    colour, depth = field_mix(heads, spread)
    col_halo[...] = colour
    dep_halo[...] = jnp.zeros(dep_halo.shape, F32)
    hrays = depth.shape[0]
    for k in range(cfg["hchunks"]):
        part = depth[k * LANES : min((k + 1) * LANES, hrays)]
        if part.shape[0] < LANES:
            part = jnp.concatenate([part, jnp.zeros((LANES - part.shape[0], LANES), F32)], axis=0)
        dep_halo[4 * k : 4 * k + 4, :] = depth_rows(part, cfg["repeat"])
    for s in range(2, cfg["groups"]):
        pack(cfg, lax.axis_index("block"), s, outs[s - 2], col_own, dep_own, col_halo, dep_halo)


def earlier_blocks(cfg, place, order, rows):
    groups, nb = cfg["groups"], cfg["nb"]
    per = nb // groups
    sub = lax.broadcasted_iota(jnp.int32, (rows, LANES), 0)
    lane = lax.broadcasted_iota(jnp.int32, (rows, LANES), 1)
    hit = (jnp.broadcast_to(order, (rows, LANES)) == sub.astype(F32)) & (lane < nb)
    rank = jnp.sum(jnp.where(hit, lane.astype(F32), 0.0), axis=1, keepdims=True)
    rank = jnp.broadcast_to(rank, (rows, LANES))
    block = ((lane // (2 * per)) ^ place) * per + lane % per
    other = jnp.sum(jnp.where(sub == block, rank, 0.0), axis=0, keepdims=True)
    return jnp.where(other < rank, 1.0, 0.0)


def near_kernel(
    cfg, own_ref, tiled, wmid_ref, whead, spread, col_in, dep_in, col_halo, dep_halo,
    meta_sides, meta_own, out_own, out_mate, earlier, flags, col_own, dep_own,
):
    nb, patch = cfg["nb"], lax.axis_index("patch")
    mine = meta_own[...].astype(F32)[0:1]
    sides = [mine, meta_sides[0:1, :], meta_sides[8:9, :]]
    rows = earlier.shape[0] // 3
    for i, order in enumerate(sides):
        made = earlier_blocks(cfg, lax.axis_index("block"), order, rows)
        earlier[i * rows : (i + 1) * rows, :] = made.astype(BF16)
    lane = lax.broadcasted_iota(jnp.int32, (1, LANES), 1)
    for i, (order, there) in enumerate([(sides[1], patch > 0), (mine, patch < cfg["patches"] - 1)]):
        seam = jnp.sum(jnp.where(lane == nb, order, 0.0), axis=1, keepdims=True)
        seam = jnp.where(there, seam, 0.0)
        flags[8 * i : 8 * i + 8, :] = jnp.broadcast_to(seam, (8, LANES))
    col_own[...] = col_in[...]
    dep_own[...] = dep_in[...]
    nets = (tiled, wmid_ref, whead, spread)
    pieces = row_pieces(cfg, lax.axis_index("block"), True)
    field_chunks(cfg, own_ref, nets, col_own, dep_own, grouped(pieces, cfg["chunk"]))
    pack(cfg, lax.axis_index("block"), 0, out_own, col_own, dep_own, col_halo, dep_halo)
    pack(cfg, lax.axis_index("block"), 1, out_mate, col_own, dep_own, col_halo, dep_halo)


def decoder_kernel(cfg, earlier_ref, flags_ref, mask_ref, pick_ref, w0_ref, w1_ref, w2_ref, w3_ref, *rest):
    groups, nb = cfg["groups"], cfg["nb"]
    bufs = rest[:groups]
    out_ref = rest[groups]
    comp, x0, sa, xa, sc, xc, rep = rest[groups + 1 :]
    cols, rows_dev, pitch = cfg["cols"], cfg["rows_dev"], cfg["pitch"]
    n_own, n_halo, n_dep = cfg["n_own"], cfg["n_halo"], cfg["n_dep"]
    rows_in = rows_dev + 2 * EDGE
    rows_mid = rows_dev + 2
    mid = rows_mid * pitch
    half = LANES // 2
    per_dev = nb // groups
    place = lax.axis_index("block")
    left_open, right_open = flags_ref[0:1, :], flags_ref[8:9, :]
    sides = earlier_ref.shape[0] // 3
    stacked = 2 * per_dev * groups
    earlier = [earlier_ref[i * sides : i * sides + nb, :stacked] for i in range(3)]

    at = n_own + n_halo
    own_rows = [bufs[s][at : at + n_dep, :].astype(F32) for s in range(groups)]
    halo_rows = [bufs[s][at + n_dep :, :].astype(F32) for s in range(groups)]
    chunks = n_own // LANES
    factors = []
    for k in range(chunks):
        stack = jnp.concatenate([own_rows[s][4 * k : 4 * k + 4] for s in range(groups)], axis=0)
        factors.append(jnp.exp(-dot(earlier[0], stack.astype(BF16))))
    lane = lax.broadcasted_iota(jnp.int32, (nb, LANES), 1)
    side_pitch = (cfg["rows_all"] + 2 * EDGE) * EDGE
    for k in range(cfg["hchunks"]):
        on_left = lane + k * LANES < side_pitch
        stack = jnp.concatenate(
            [halo_rows[s][4 * k : 4 * k + 4] for s in range(groups)], axis=0
        ).astype(BF16)
        from_left = jnp.exp(-dot(earlier[1], stack)) * left_open
        from_right = jnp.exp(-dot(earlier[2], stack)) * right_open
        factors.append(jnp.where(on_left, from_left, from_right))
    steps = len(factors)
    factors.append(jnp.zeros((LANES - steps * nb, LANES), F32))
    turned = jnp.concatenate(factors, axis=0).T
    lhs = []
    for k in range(steps):
        high, low = split16(pltpu.roll(turned, (LANES - k * nb) % LANES, 1) if k else turned)
        lhs.append(jnp.concatenate([high.astype(BF16), low.astype(BF16)], axis=1))
    lane = lax.broadcasted_iota(jnp.int32, (2 * LANES, groups * LANES), 1)
    block = ((lane // LANES) ^ place) * per_dev + (lane & (LANES - 1)) // half
    sub = lax.broadcasted_iota(jnp.int32, (2 * LANES, groups * LANES), 0) & (LANES - 1)
    wide = dot(jnp.concatenate(lhs, axis=0), jnp.where(sub == block, 1.0, 0.0).astype(BF16))

    def spread(k):
        return wide[k * LANES : (k + 1) * LANES]

    def mix(weights, lo, n):
        acc = None
        for s in range(groups):
            term = weights[:, s * LANES : (s + 1) * LANES] * bufs[s][lo : lo + n, :].astype(F32)
            acc = term if acc is None else acc + term
        return acc + pltpu.roll(acc, half, 1)

    comp[...] = jnp.zeros(comp.shape, F32)
    base = pitch
    per_chunk = LANES // cols
    for k in range(chunks):
        mixed = mix(spread(k), k * LANES, LANES)
        for t in range(per_chunk):
            q = base + (k * per_chunk + t) * pitch + LEAD
            comp[q : q + cols, :] = mixed[t * cols : (t + 1) * cols]
    for k in range(cfg["hchunks"]):
        rep[k * LANES : (k + 1) * LANES, :] = spread(chunks + k)
    size = n_halo // 2
    for i in range(2):
        start = pl.multiple_of(i * side_pitch + place * (rows_dev * EDGE), 8)
        mixed = mix(rep[pl.ds(start, size), :], n_own + i * size, size)
        for r in range(rows_in):
            q = base + r * pitch + LEAD + (cols if i else -EDGE)
            comp[q : q + EDGE, :] = mixed[r * EDGE : (r + 1) * EDGE]

    n_in = rows_in * pitch
    lane = lax.broadcasted_iota(jnp.int32, (n_in, LANES), 1)
    here = jnp.where(lane < half, comp[base - 1 : base - 1 + n_in, :], comp[base : base + n_in, :])
    x0[:, 0:LANES] = here.astype(BF16)
    x0[:, LANES : 2 * LANES] = comp[base + 1 : base + 1 + n_in, :].astype(BF16)

    mask = mask_ref[...]

    def convolve(ref, pieces, n, weights):
        made = []
        for h in range(2):
            lhs = jnp.concatenate(
                [ref[r * pitch + h * n // 2 : r * pitch + (h + 1) * n // 2, a:b] for r, a, b in pieces],
                axis=1,
            )
            made.append(dot_t(lhs, weights))
        return jnp.concatenate(made, axis=0)

    wide = 2 * LANES
    value = convolve(x0, [(d, 0, wide) for d in range(3)], mid, w0_ref[...])
    value = jnp.maximum(value, 0.0) * mask

    sa[0:8, :] = jnp.zeros((8, wide), F32)
    sa[8 + mid :, :] = jnp.zeros((8, wide), F32)
    xa[0:pitch, :] = jnp.zeros((pitch, 2 * wide), BF16)
    xa[pitch + mid :, :] = jnp.zeros((pitch, 2 * wide), BF16)
    low = lax.broadcasted_iota(jnp.int32, (mid, LANES), 1) < half

    def beside(after, before):
        return jnp.where(low, after, before).astype(BF16)

    def lay_out(value):
        sa[8 : 8 + mid, :] = value
        for pr in range(2):
            own = slice(pr * LANES, (pr + 1) * LANES)
            xa[pitch : pitch + mid, pr * wide : pr * wide + LANES] = value[:, own].astype(BF16)
            xa[pitch : pitch + mid, pr * wide + LANES : (pr + 1) * wide] = beside(
                sa[9 : 9 + mid, own], sa[7 : 7 + mid, own]
            )

    lay_out(value)
    value = convolve(
        xa, [(0, wide, 2 * wide), (1, 0, 2 * wide), (2, 0, wide)], mid, w1_ref[...]
    )
    value = jnp.maximum(value, 0.0) * mask
    lay_out(value)
    three = 3 * LANES
    for pr in range(2):
        pieces = [(0, wide, 2 * wide), (1, 0, 2 * wide)] if pr == 0 else [(1, 0, 2 * wide), (2, 0, wide)]
        both = convolve(xa, pieces, mid, w2_ref[...])
        for pc in range(2):
            value = jnp.maximum(both[:, pc * wide : (pc + 1) * wide], 0.0) * mask
            sc[2 * pr + pc, 8 : 8 + mid, :] = value
            for rr in range(2):
                at = (2 * pr + rr) * three + pc * LANES
                xc[:, at : at + LANES] = value[:, rr * LANES : (rr + 1) * LANES].astype(BF16)
        for rr in range(2):
            own = slice(rr * LANES, (rr + 1) * LANES)
            at = (2 * pr + rr) * three + 2 * LANES
            xc[:, at : at + LANES] = beside(
                sc[2 * pr, 9 : 9 + mid, own], sc[2 * pr + 1, 7 : 7 + mid, own]
            )
    n_out = rows_dev * pitch
    final = convolve(
        xc, [(0, 3 * three, 4 * three), (1, 0, 4 * three), (2, 0, three)], n_out, w3_ref[...]
    )
    final = final + pltpu.roll(final, half, 1)
    rays = jnp.concatenate(
        [final[r * pitch + LEAD : r * pitch + LEAD + cols] for r in range(rows_dev)], axis=0
    )
    turned = rays.T
    stack = jnp.concatenate(
        [
            jnp.concatenate(
                [turned[16 * v : 16 * v + 16, r * cols : (r + 1) * cols] for v in range(4)], axis=1
            )
            for r in range(rows_dev)
        ],
        axis=0,
    )
    pick = pick_ref[...]
    high, low = split16(stack)
    image = dot(high.astype(BF16), pick) + dot(low.astype(BF16), pick)
    colours = out_ref.shape[0]
    for r in range(rows_dev):
        for u in range(4):
            for p in range(colours):
                at = r * 16 + u * 4 + p
                out_ref[p, 4 * r + u : 4 * r + u + 1, :] = image[at : at + 1, :]


def phase_taps(p, d):
    return [a for a in range(3) if (p + a - 1) // 2 + 1 == d]


def weights_kernel(
    cfg, conv_ref, colour_ref, flags_ref, w0_ref, w1_ref, w2_ref, w3_ref, mask_ref, pick_ref
):
    feat = conv_ref.shape[1]
    r = lax.broadcasted_iota(jnp.int32, (feat, LANES), 0)
    lane = lax.broadcasted_iota(jnp.int32, (feat, LANES), 1)
    twice = jnp.where((lane == r) | (lane == r + feat), 1.0, 0.0).astype(BF16)
    low = lane < feat
    zero = jnp.zeros((feat, LANES), F32)
    taps = [
        dot(conv_ref[k * 9 * feat : (k + 1) * 9 * feat, :], twice) for k in range(4)
    ]

    def tap(k, a, e):
        at = (a * 3 + e) * feat
        return taps[k][at : at + feat]

    def pair(left, right):
        if left is None and right is None:
            return zero
        if left is right:
            return left
        return jnp.where(low, zero if left is None else left, zero if right is None else right)

    def put(ref, n, j, tile):
        ref[n * feat : (n + 1) * feat, j * LANES : (j + 1) * LANES] = tile.astype(BF16)

    for k in (0, 2):
        sums = {}
        for p in range(2):
            for q in range(2):
                for d in range(3):
                    for f in range(3):
                        parts = [tap(k, a, e) for a in phase_taps(p, d) for e in phase_taps(q, f)]
                        sums[p, q, d, f] = functools.reduce(jnp.add, parts) if parts else None
        for p in range(2):
            for q in range(2):
                n = 2 * p + q
                for d in range(3):
                    row = [sums[p, q, d, f] for f in range(3)]
                    if k == 0:
                        makes = [(w0_ref, n, row + [None])]
                    else:
                        makes = [
                            (w2_ref, n, [row[1], row[2], None, row[0]]),
                            (w2_ref, 4 + n, row + [None]),
                        ]
                    for ref, at, blocks in makes:
                        put(ref, at, 2 * d, pair(blocks[0], blocks[1]))
                        put(ref, at, 2 * d + 1, pair(blocks[2], blocks[3]))

    def pick(table, a, e):
        return table(a, e) if 0 <= a < 3 and 0 <= e < 3 else None

    for p in range(2):
        for q in range(2):
            for row in range(4):
                for j, at in enumerate([(2, 3), (4, 1)]):
                    blocks = [
                        pick(lambda a, e: tap(1, a, e), row - p, c - 1 - q) for c in at
                    ]
                    put(w1_ref, 2 * p + q, row * 2 + j, pair(*blocks))

    colours = colour_ref.shape[0]
    given = colour_ref[...].astype(F32)
    sub = lax.broadcasted_iota(jnp.int32, (8, feat), 0)
    mixer = jnp.zeros((8, feat), F32)
    for p in range(colours):
        mixer = jnp.where((sub & 3) == p, given[p : p + 1], mixer)
    mixer = mixer.astype(BF16)
    mixed = {
        (a, e): dot(mixer, tap(3, a, e).astype(BF16)) for a in range(3) for e in range(3)
    }
    lane = lax.broadcasted_iota(jnp.int32, (8, LANES), 1) < feat
    upper = lax.broadcasted_iota(jnp.int32, (8, LANES), 0) < 4
    blank = jnp.zeros((8, LANES), F32)

    def choose(mask, x, y):
        if x is None and y is None:
            return None
        return jnp.where(mask, blank if x is None else x, blank if y is None else y)

    for row in range(6):
        for j, (c_left, c_right) in enumerate([(2, 3), (4, 5), (6, 1)]):
            pieces = []
            for v in range(4):
                for u in (0, 2):
                    halves = [
                        choose(
                            lane,
                            pick(lambda a, e: mixed[a, e], row - w, c_left - 1 - v),
                            pick(lambda a, e: mixed[a, e], row - w, c_right - 1 - v),
                        )
                        for w in (u, u + 1)
                    ]
                    made = choose(upper, *halves)
                    pieces.append(blank if made is None else made)
            tile = jnp.concatenate(pieces, axis=0)
            high, low16 = split16(tile)
            at = (row * 3 + j) * LANES
            w3_ref[:, at : at + LANES] = jnp.concatenate([high, low16], axis=0).astype(BF16)

    cols, pitch, rows_mid = cfg["cols"], cfg["pitch"], cfg["rows_dev"] + 2
    place, mid = lax.axis_index("block"), rows_mid * pitch
    left_open, right_open = flags_ref[0:1, :], flags_ref[8:9, :]
    top_open = jnp.where(place > 0, 1.0, 0.0)
    bottom_open = jnp.where(place < cfg["groups"] - 1, 1.0, 0.0)
    q = lax.broadcasted_iota(jnp.int32, (mid, 2 * LANES), 0)
    pos = q
    for r in range(1, rows_mid):
        pos = pos - jnp.where(q >= r * pitch, pitch, 0)
    left_open = jnp.concatenate([left_open, left_open], axis=1)
    right_open = jnp.concatenate([right_open, right_open], axis=1)
    mask = jnp.where(pos < LEAD, left_open, jnp.where(pos >= LEAD + cols, right_open, 1.0))
    mask = mask * jnp.where(q < pitch, top_open, jnp.where(q >= mid - pitch, bottom_open, 1.0))
    mask_ref[...] = mask
    r = lax.broadcasted_iota(jnp.int32, (4 * cols, 4 * cols), 0)
    c = lax.broadcasted_iota(jnp.int32, (4 * cols, 4 * cols), 1)
    place_of = (c & 3) * cols + (c >> 2)
    pick = jnp.where(r == place_of, 1.0, 0.0).astype(BF16)
    pick_ref[...] = pick


def body(samples_in, block_order, seam_link, w_in, w_mid, w_feat, w_density, w_conv, w_color):
    blk_dev, rows_all, cols, width = samples_in.shape
    groups, patches = lax.axis_size("block"), lax.axis_size("patch")
    nb = block_order.shape[1]
    enc = w_in.shape[1]
    feat = w_feat.shape[2]
    rows_dev = rows_all // groups
    count = rows_all * cols
    hrays = (rows_all + 2 * EDGE) * 2 * EDGE
    hchunks = -(-hrays // LANES)
    n_own = (rows_dev + 2 * EDGE) * cols
    n_halo = (rows_dev + 2 * EDGE) * 2 * EDGE
    n_dep = 4 * n_own // LANES
    n_tail = 16
    samples = width // enc
    cfg = dict(
        groups=groups,
        nb=nb,
        patches=patches,
        samples=samples,
        enc=enc,
        repeat=LANES // (samples * blk_dev),
        cols=cols,
        rows_all=rows_all,
        rows_dev=rows_dev,
        n_near=2 * rows_dev - (EDGE if groups == 4 else 2 * EDGE),
        side_pitch=hrays // 2,
        pitch=cols + 16,
        chunk=2,
        n_own=n_own,
        n_halo=n_halo,
        n_dep=n_dep,
        hchunks=hchunks,
    )
    vmem = pl.BlockSpec(memory_space=pltpu.VMEM)
    hbm = pl.BlockSpec(memory_space=pltpu.HBM)
    params = pltpu.CompilerParams(vmem_limit_bytes=16 * 1024 * 1024)

    def far_off(x):
        return pltpu.with_memory_space_constraint(x, pltpu.HBM)


    edges = blk_dev * rows_all * EDGE
    early = [w_in, w_density, w_color]
    win, dens, colour, meta_own, near, far, spread = pl.pallas_call(
        functools.partial(edges_kernel, cfg),
        out_shape=[pltpu.VMEM(x.shape, BF16) for x in early]
        + [
            pltpu.VMEM((16, width), BF16),
            pltpu.VMEM((edges + 16, width), BF16),
            pltpu.VMEM((edges + 16, width), BF16),
            pltpu.VMEM((2 * LANES, samples * LANES), BF16),
        ],
        in_specs=[hbm] * (3 + len(early)),
        out_specs=[vmem] * (4 + len(early)),
        scratch_shapes=[
            pltpu.VMEM((2, blk_dev, rows_all, 8, width), BF16),
            pltpu.VMEM((edges, width), F32),
            pltpu.VMEM((edges, width), F32),
            pltpu.SMEM(block_order.shape, jnp.int32),
            pltpu.SMEM(seam_link.shape, jnp.int32),
            pltpu.SemaphoreType.DMA((5 + len(early),)),
        ],
        compiler_params=params,
        cost_estimate=pl.CostEstimate(flops=4 * 10**9, bytes_accessed=10**6, transcendentals=0),
        name="edges",
    )(
        far_off(block_order),
        seam_link,
        far_off(samples_in),
        *[far_off(x) for x in early],
    )
    own, wmid = samples_in.reshape(blk_dev, count, width), w_mid
    swap_near = [(i, i ^ 1) for i in range(patches) if i ^ 1 < patches]
    swap_far = []
    for i in range(1, patches - 1, 2):
        swap_far += [(i, i + 1), (i + 1, i)]
    far = lax.ppermute(far, "patch", swap_far)
    near = lax.ppermute(near, "patch", swap_near)

    rays_flops = 2 * 2 * blk_dev * samples * w_mid.shape[2] * (3 * w_mid.shape[2])
    far_rays = (rows_all - cfg["n_near"]) * cols
    col_own, dep_own, tiled, whead = pl.pallas_call(
        functools.partial(field_kernel, cfg),
        out_shape=[
            pltpu.VMEM((count + 2 * EDGE * cols, LANES), BF16),
            pltpu.VMEM((8 * (count + 2 * EDGE * cols) // LANES, LANES), F32),
            pltpu.VMEM((blk_dev, width, w_in.shape[2]), BF16),
            pltpu.VMEM((blk_dev, samples, w_feat.shape[1], 2 * LANES), BF16),
        ],
        in_specs=[vmem] * 6,
        out_specs=[vmem] * 4,
        compiler_params=params,
        cost_estimate=pl.CostEstimate(
            flops=far_rays * rays_flops, bytes_accessed=10**6, transcendentals=0
        ),
        name="field",
    )(own, win, wmid, w_feat, dens, spread)

    size = n_own + n_halo + n_dep + n_tail
    shape = pltpu.VMEM((size, LANES), BF16)
    *bufs, col_halo, dep_halo, meta, col_own, dep_own = pl.pallas_call(
        functools.partial(halo_kernel, cfg),
        out_shape=[shape] * (groups - 2)
        + [
            pltpu.VMEM((hrays, LANES), F32),
            pltpu.VMEM((n_tail, LANES), F32),
            pltpu.VMEM((16, LANES), F32),
            pltpu.VMEM(col_own.shape, BF16),
            pltpu.VMEM(dep_own.shape, F32),
        ],
        in_specs=[vmem] * 9,
        out_specs=[vmem] * (groups + 3),
        scratch_shapes=[pltpu.VMEM((blk_dev, hrays, width), F32)],
        compiler_params=params,
        name="halo",
    )(near, far, own, tiled, wmid, whead, spread, col_own, dep_own)
    got = []
    for s in range(2, groups):
        got.append(lax.ppermute(bufs[s - 2], "block", [(i, i ^ s) for i in range(groups)]))

    near_rows = pl.pallas_call(
        functools.partial(near_kernel, cfg),
        out_shape=[shape] * 2
        + [pltpu.VMEM((48, LANES), BF16), pltpu.VMEM((16, LANES), F32)],
        in_specs=[vmem] * 11,
        out_specs=[vmem] * 4,
        scratch_shapes=[
            pltpu.VMEM(col_own.shape, BF16),
            pltpu.VMEM(dep_own.shape, F32),
        ],
        compiler_params=params,
        cost_estimate=pl.CostEstimate(
            flops=cfg["n_near"] * cols * rays_flops, bytes_accessed=10**6, transcendentals=0
        ),
        name="near",
    )
    mine, mate, earlier, flags = near_rows(
        own, tiled, wmid, whead, spread, col_own, dep_own, col_halo, dep_halo, meta, meta_own
    )
    got = [mine, lax.ppermute(mate, "block", [(i, i ^ 1) for i in range(groups)])] + got

    pitch = cfg["pitch"]
    rows_in, rows_mid = rows_dev + 2 * EDGE, rows_dev + 2
    w0, w1, w2, w3, mask, pick = pl.pallas_call(
        functools.partial(weights_kernel, cfg),
        out_shape=[
            pltpu.VMEM((4 * feat, 12 * feat), BF16),
            pltpu.VMEM((4 * feat, 16 * feat), BF16),
            pltpu.VMEM((8 * feat, 12 * feat), BF16),
            pltpu.VMEM((2 * feat, 36 * feat), BF16),
            pltpu.VMEM((rows_mid * pitch, 2 * LANES), F32),
            pltpu.VMEM((4 * cols, 4 * cols), BF16),
        ],
        in_specs=[vmem] * 3,
        out_specs=[vmem] * 6,
        compiler_params=params,
        cost_estimate=pl.CostEstimate(flops=10**8, bytes_accessed=10**6, transcendentals=0),
        name="weights",
    )(w_conv.reshape(-1, feat), colour, flags)
    return pl.pallas_call(
        functools.partial(decoder_kernel, cfg),
        out_shape=jax.ShapeDtypeStruct((w_color.shape[0], 4 * rows_dev, 4 * cols), F32),
        in_specs=[vmem] * (8 + groups),
        out_specs=vmem,
        scratch_shapes=[
            pltpu.VMEM(((rows_in + 2) * pitch, LANES), F32),
            pltpu.VMEM((rows_in * pitch, 2 * LANES), BF16),
            pltpu.VMEM((rows_mid * pitch + 16, 2 * LANES), F32),
            pltpu.VMEM(((rows_mid + 2) * pitch, 4 * LANES), BF16),
            pltpu.VMEM((4, rows_mid * pitch + 16, 2 * LANES), F32),
            pltpu.VMEM((rows_mid * pitch, 12 * LANES), BF16),
            pltpu.VMEM((hchunks * LANES, groups * LANES), F32),
        ],
        compiler_params=params,
        name="decoder",
    )(earlier, flags, mask, pick, w0, w1, w2, w3, *got)


def solution(mesh):
    return jax.shard_map(
        body,
        mesh=mesh,
        in_specs=(
            P("block", None, "patch", None),
            P("patch", None),
            P("patch"),
            P("block", None, None),
            P("block", None, None, None),
            P("block", None, None),
            P("block", None),
            P(),
            P(),
        ),
        out_specs=P(None, "block", "patch"),
        check_vma=False,
    )
```
